32 devices in a mesh: row: 8 (over y, x, core), col: 4 (over z).
Axes of the slice: x: 2, y: 2, z: 4, core: 2. Of those that a mesh axis runs over, the one named last changes fastest.
Arguments:
- sources: float32 [3, 1024, 4096], P(None, 'row', 'col'), may hold values from -32 to 32
- labels: int32 [1024, 4096], P('row', 'col'), may hold values from 0 to 2
Outputs:
- blended: float32 [1024, 4096], P('row', 'col')
- overview_fine: float32 [512, 2048], P('row', 'col')
- overview_mid: float32 [256, 1024], P(None, 'col')
- overview_coarse: float32 [128, 512], P(None, 'col')
The draws below stay inside these ranges and needn't reach their ends.
All inputs are finite; a program needn't handle non-finite values.
Results may differ from the reference program's by a relative error of at most 0.0001.
Values sent between devices are 32-bit elements; how exact they have to be, the bound alone decides.
A program may use at most 64 MiB of HBM per device.

```python
import jax
import jax.numpy as jnp

K = 3
ITERS = 3
H = 1024
W = 4096


def draw_sources(key, part):
    row_frac = jnp.arange(H, dtype=jnp.float32) / H
    col_frac = jnp.arange(W, dtype=jnp.float32) / W
    amplitude = (1.0 + 2.0 * row_frac)[:, None] * (1.0 + 2.0 * col_frac)[None, :] / 3.0
    noise_draw = jnp.clip(jax.random.normal(key, (K, H, W), jnp.float32), -6.0, 6.0)
    return noise_draw * amplitude


def touch_ends(entries, own_key, smallest, top_value):
    place = [jax.random.randint(jax.random.fold_in(own_key, axis), (), 0, length) for axis, length in enumerate(entries.shape)]
    main_axis = entries.shape.index(max(entries.shape))
    neighbour = place[:main_axis] + [(place[main_axis] + 1) % entries.shape[main_axis]] + place[main_axis + 1:]
    return entries.at[tuple(place)].set(smallest).at[tuple(neighbour)].set(top_value)


def setup_inputs(seed: int = 0) -> dict:
    key_of = jax.random.split(jax.random.key(seed), 3)
    return {
        "sources": draw_sources(jax.random.fold_in(key_of[2], 71), 0),
        "labels": touch_ends(jax.random.randint(key_of[1], (H, W), 0, K), jax.random.fold_in(key_of[1], 1), 0, K - 1).astype(jnp.int32),
    }


def apply_stencil(values):
    padded = jnp.pad(values, 1)
    beside = padded[2:, 1:-1] + padded[:-2, 1:-1]
    beside = beside + padded[1:-1, 2:] + padded[1:-1, :-2]
    return 4.0 * values - beside


def average_pool(values):
    return 0.25 * (values[0::2, 0::2] + values[1::2, 0::2] + values[0::2, 1::2] + values[1::2, 1::2])


def reference(sources, labels):
    right_side = jnp.zeros(labels.shape, jnp.float32)
    for channel in range(K):
        right_side = right_side + jnp.where(labels == channel, apply_stencil(sources[channel]), jnp.float32(0.0))
    blended = jnp.zeros(labels.shape, jnp.float32)
    residual = right_side
    direction = right_side
    norm_now = jnp.sum(residual * residual)
    for iteration in range(ITERS):
        applied = apply_stencil(direction)
        step_size = norm_now / jnp.sum(direction * applied)
        blended = blended + step_size * direction
        residual = residual - step_size * applied
        norm_next = jnp.sum(residual * residual)
        direction = residual + (norm_next / norm_now) * direction
        norm_now = norm_next
    overview_fine = average_pool(blended)
    overview_mid = average_pool(overview_fine)
    overview_coarse = average_pool(overview_mid)
    return (blended, overview_fine, overview_mid, overview_coarse)
```

```python
import functools

import jax
import jax.numpy as jnp
from jax import lax
from jax.experimental import pallas as pl
from jax.experimental.pallas import tpu as pltpu
from jax.sharding import PartitionSpec as P

ITERS = 3
MESH = pl.DeviceIdType.MESH
HALO = 4
TOP = 8
LANES = 128
SIDES = ((-1, -1), (-1, 1), (1, -1), (1, 1), (-1, 0), (1, 0), (0, -1), (0, 1))


def lane_of(shape):
    return lax.broadcasted_iota(jnp.int32, shape, len(shape) - 1)


def line_of(shape):
    return lax.broadcasted_iota(jnp.int32, shape, len(shape) - 2)


def lines(ref, index, start):
    return ref[index + (pl.ds(start, 8), slice(None))]


def beside_ring(mid):
    tiles = mid.shape[0]
    lane = lane_of(mid.shape)
    left = pltpu.roll(mid, 1, axis=2)
    right = pltpu.roll(mid, LANES - 1, axis=2)
    from_left = jnp.concatenate([left[tiles - 1:], left[:tiles - 1]], axis=0)
    from_right = jnp.concatenate([right[1:], right[:1]], axis=0)
    return jnp.where(lane == 0, from_left, left) + jnp.where(lane == LANES - 1, from_right, right)


def beside_tile(mid):
    return pltpu.roll(mid, 1, axis=1) + pltpu.roll(mid, LANES - 1, axis=1)


def neighbour_sum(ref, index, start, mid, beside):
    return (lines(ref, index, start - 1) + lines(ref, index, start + 1)) + beside(mid)


def right_side(src, lab, tile, start, beside):
    here = lines(lab, (tile,), start)
    total = None
    for k in reversed(range(src.shape[0])):
        mid = lines(src, (k, tile), start)
        term = 4.0 * mid - neighbour_sum(src, (k, tile), start, mid, beside)
        total = term if total is None else jnp.where(here == k, term, total)
    return total


def quadratic(left, right, moments, shift):
    total = None
    for i, a in enumerate(left):
        for j, b in enumerate(right):
            term = a * b * moments[i + j + shift]
            total = term if total is None else total + term
    return total


def padded_sum(a, b):
    if len(a) < len(b):
        a, b = b, a
    return [x + b[i] if i < len(b) else x for i, x in enumerate(a)]


def coefficients(moments):
    residual = [jnp.ones_like(moments[0])]
    direction = residual
    solution_coords = [jnp.zeros_like(moments[0])]
    norm_now = moments[0]
    for iteration in range(ITERS):
        applied_dot = 4.0 * (
            quadratic(direction, direction, moments, 0)
            - quadratic(direction, direction, moments, 1)
        )
        step = norm_now / applied_dot
        solution_coords = padded_sum(solution_coords, [step * d for d in direction])
        if iteration + 1 < ITERS:
            moved = [-4.0 * step * d for d in direction]
            residual = padded_sum(residual, moved)
            residual = padded_sum(residual, [jnp.zeros_like(step)] + [-m for m in moved])
            norm_next = quadratic(residual, residual, moments, 0)
            ratio = norm_next / norm_now
            direction = padded_sum(residual, [ratio * d for d in direction])
            norm_now = norm_next
    return solution_coords


def split_dot(values, pool):
    total = None
    for _ in range(3):
        piece = values.astype(jnp.bfloat16)
        values = values - piece.astype(jnp.float32)
        part = jnp.dot(piece, pool, preferred_element_type=jnp.float32)
        total = part if total is None else total + part
    return total


def pooled(load, stride, pool):
    parts = []
    for tile in range(stride):
        part = load(tile, 0)
        for line in range(1, stride):
            part = part + load(tile, line)
        parts.append(part)
    return split_dot(jnp.concatenate(parts, axis=1), pool)


def pool_matrix(stride):
    shape = (LANES * stride, LANES)
    source, target = (lax.broadcasted_iota(jnp.int32, shape, d) for d in range(2))
    return jnp.where(source // stride == target, 1.0 / (stride * stride), 0.0).astype(jnp.bfloat16)


def gather_kernel(
    n_row, n_col, rows, cols, kinds,
    src_hbm, lab_hbm, vec, fines, mids, coord_ref,
    src, lab, edge, edge_lab, pack_r, pack_c, got_r, got_c, got_d, part, moment,
    load_sem, send_sem, recv_sem, mom_send, mom_recv, mid_send, mid_recv, fwd_send, fwd_recv,
):
    tiles = cols // LANES
    side_tile = tiles
    main = slice(0, tiles)
    body_rows = pl.ds(TOP, rows)
    n = n_row * n_col
    row, col = lax.axis_index("row"), lax.axis_index("col")
    me = row * n_col + col
    f32 = jnp.float32

    def plane_load(k, t):
        lanes = pl.ds(t * LANES, LANES)
        if k < kinds:
            return pltpu.make_async_copy(
                src_hbm.at[k, :, lanes], src.at[k, t, body_rows], load_sem.at[k, t])
        return pltpu.make_async_copy(lab_hbm.at[:, lanes], lab.at[t, body_rows], load_sem.at[k, t])

    def edge_load(k, side):
        here = pl.ds(0 if side == 0 else rows - 8, 8)
        if k < kinds:
            return pltpu.make_async_copy(
                src_hbm.at[k, here], edge.at[k, side], load_sem.at[k, tiles + side])
        return pltpu.make_async_copy(lab_hbm.at[here], edge_lab.at[side], load_sem.at[k, tiles + side])

    first_loads = [plane_load(k, t) for k in range(kinds + 1) for t in (0, tiles - 1)]
    first_loads += [edge_load(k, side) for k in range(kinds + 1) for side in range(2)]
    later_loads = [plane_load(k, t) for t in range(1, tiles - 1) for k in range(kinds + 1)]
    for load in first_loads:
        load.start()

    barrier = pltpu.get_barrier_semaphore()

    columns = [col]
    for _ in range(n_col - 1):
        columns.append(jnp.where(columns[-1] + 1 == n_col, 0, columns[-1] + 1))

    def for_all_others(act):
        for c in columns[1:]:
            act(row, c)

        def body(step, _):
            r = row + step
            r = jnp.where(r >= n_row, r - n_row, r)
            for c in columns:
                act(r, c)
            return 0

        lax.fori_loop(1, n_row, body, 0)

    for_all_others(lambda r, c: pl.semaphore_signal(
        barrier, inc=1, device_id=(r, c), device_id_type=MESH))
    for load in later_loads:
        load.start()

    first_row, last_row = row == 0, row == n_row - 1
    first_col, last_col = col == 0, col == n_col - 1
    pad = jnp.zeros((tiles + 1, 8, LANES), f32)
    for start in (0, TOP + rows):
        for k in range(kinds):
            src[k, :, pl.ds(start, 8), :] = pad
        lab[:, pl.ds(start, 8), :] = pad.astype(jnp.int32)
        for w in range(ITERS):
            vec[w, :, pl.ds(start, 8), :] = pad

    n_pack = HALO * (kinds + 1)
    with jax.named_scope("wait_first"):
        for load in first_loads:
            load.wait()
    with jax.named_scope("pack"):
        for k in range(kinds + 1):
            at = pl.ds(HALO * k, HALO)
            for side in range(2):
                lines_here = pl.ds(0 if side == 0 else 8 - HALO, HALO)
                for t in range(tiles):
                    lanes = pl.ds(t * LANES, LANES)
                    if k < kinds:
                        value = edge[k, side, lines_here, lanes]
                    else:
                        value = edge_lab[side, lines_here, lanes].astype(f32)
                    pack_r[side, t, at, :] = value
        wide_lane = lane_of((rows, LANES))
        for k in range(kinds + 1):
            if k < kinds:
                first, last = src[k, 0, body_rows], src[k, tiles - 1, body_rows]
            else:
                first, last = lab[0, body_rows].astype(f32), lab[tiles - 1, body_rows].astype(f32)
            both = jnp.where(wide_lane < LANES // 2, first, last)
            turned = jnp.transpose(both)
            at = pl.ds(HALO * k, HALO)
            pack_c[0, at, :] = turned[0:HALO]
            pack_c[1, at, :] = turned[LANES - HALO:LANES]

    with jax.named_scope("barrier"):
        pl.semaphore_wait(barrier, n - 1)

    sends = []
    for i, (dr, dc) in enumerate(SIDES):
        mine_r, mine_c = (0 if dr < 0 else 1), (0 if dc < 0 else 1)
        if dc == 0:
            source, target, here = pack_r.at[mine_r], got_r.at[1 - mine_r], got_r.at[mine_r]
        elif dr == 0:
            source, target, here = pack_c.at[mine_c], got_c.at[1 - mine_c], got_c.at[mine_c]
        else:
            source = pack_r.at[mine_r, 0 if dc < 0 else tiles - 1]
            target, here = got_d.at[1 - mine_r, 1 - mine_c], got_d.at[mine_r, mine_c]
        there = jnp.logical_and(
            jnp.logical_and(row + dr >= 0, row + dr < n_row),
            jnp.logical_and(col + dc >= 0, col + dc < n_col),
        )
        opposite = SIDES.index((-dr, -dc))
        device = (
            jnp.clip(row + dr, 0, n_row - 1),
            jnp.clip(col + dc, 0, n_col - 1),
        )
        copy = pltpu.make_async_remote_copy(
            src_ref=source, dst_ref=target, send_sem=send_sem.at[i],
            recv_sem=recv_sem.at[opposite], device_id=device, device_id_type=MESH,
        )
        back = pltpu.make_async_remote_copy(
            src_ref=source, dst_ref=here, send_sem=send_sem.at[i],
            recv_sem=recv_sem.at[i], device_id=device, device_id_type=MESH,
        )
        sends.append((there, copy, back))
        pl.when(there)(copy.start)

    with jax.named_scope("wait_later"):
        for load in later_loads:
            load.wait()
    groups = rows // 8
    lane_r = lane_of((tiles, 8, LANES))
    lane_t = lane_of((8, LANES))
    line_t = line_of((8, LANES))

    def whole_loop(count, act):
        def body(i, _):
            act(i)
            return 0

        lax.fori_loop(0, count, body, 0, unroll=count)

    def save(which, tile, start, value):
        vec[which, tile, pl.ds(start, 8), :] = value

    def applied(which, tile, start, beside):
        mid = lines(vec, (which, tile), start)
        return neighbour_sum(vec, (which, tile), start, mid, beside)

    with jax.named_scope("main_b"):
        whole_loop(groups, lambda i: save(
            0, main, TOP + 8 * i, right_side(src, lab, main, TOP + 8 * i, beside_ring)))
    with jax.named_scope("main_v"):
        for which in range(1, ITERS):
            whole_loop(groups, lambda i: save(
                which, main, TOP + 8 * i, applied(which - 1, main, TOP + 8 * i, beside_ring)))

    def products(tile, start, beside, keep):
        powers = [lines(vec, (w, tile), start) for w in range(ITERS)]
        powers.append(neighbour_sum(vec, (ITERS - 1, tile), start, powers[-1], beside))
        kept = [keep(p) for p in powers[:ITERS]]
        return [kept[i // 2] * powers[(i + 1) // 2] for i in range(2 * ITERS)]

    def keep_main(p):
        edge_lane = lane_of((1, 8, LANES))
        return jnp.concatenate([
            jnp.where(edge_lane < HALO, 0.0, p[0:1]), p[1:tiles - 1],
            jnp.where(edge_lane >= LANES - HALO, 0.0, p[tiles - 1:]),
        ], axis=0)

    def fold(value):
        if len(value.shape) == 2:
            return value
        total = value[0]
        for t in range(1, value.shape[0]):
            total = total + value[t]
        return total

    with jax.named_scope("main_m"):
        def main_body(i, sums):
            new = products(main, TOP + HALO + 8 * i, beside_ring, keep_main)
            return tuple(s + fold(p) for s, p in zip(sums, new))

        zero8 = jnp.zeros((8, LANES), f32)
        sums = lax.fori_loop(
            0, groups - 1, main_body, tuple(zero8 for _ in range(2 * ITERS)), unroll=groups - 1)
        for i, s in enumerate(sums):
            part[i] = s
    with jax.named_scope("side_fill"):
        for k in range(kinds + 1):
            if k < kinds:
                first, last = src[k, 0, body_rows], src[k, tiles - 1, body_rows]
                src[k, side_tile, body_rows, :] = jnp.where(
                    wide_lane < LANES // 2, pltpu.roll(first, 2 * HALO, axis=1), last)
            else:
                first, last = lab[0, body_rows], lab[tiles - 1, body_rows]
                lab[side_tile, body_rows, :] = jnp.where(
                    wide_lane < LANES // 2, pltpu.roll(first, 2 * HALO, axis=1), last)

    with jax.named_scope("wait_halo"):
        for there, copy, back in sends:
            pl.when(there)(back.wait_recv)

    with jax.named_scope("unpack"):
        for k in range(kinds + 1):
            at = pl.ds(HALO * k, HALO)
            right = jnp.where(last_col, 0.0, got_c[1, at, :])
            left = jnp.where(first_col, 0.0, got_c[0, at, :])
            turned = jnp.transpose(jnp.concatenate([right, left], axis=0))
            if k < kinds:
                src[k, side_tile, body_rows, 0:2 * HALO] = turned
            else:
                lab[side_tile, body_rows, 0:2 * HALO] = turned.astype(jnp.int32)
        corner_lane = lane_of((HALO, LANES))
        for side in range(2):
            missing = first_row if side == 0 else last_row
            base = TOP - HALO if side == 0 else TOP + rows
            for k in range(kinds + 1):
                at = pl.ds(HALO * k, HALO)
                wide = [jnp.where(missing, 0.0, got_r[side, t, at, :]) for t in range(tiles)]
                right = jnp.where(missing | last_col, 0.0, got_d[side, 1, at, :])
                left = jnp.where(missing | first_col, 0.0, got_d[side, 0, at, :])
                moved = pltpu.roll(
                    jnp.where(corner_lane >= LANES - HALO, left, wide[0]), 2 * HALO, axis=1)
                own = jnp.where(corner_lane < LANES // 2, moved, wide[-1])
                wide.append(jnp.where(corner_lane < HALO, right, own))
                for t, value in enumerate(wide):
                    if k < kinds:
                        src[k, t, pl.ds(base, HALO), :] = value
                    else:
                        lab[t, pl.ds(base, HALO), :] = value.astype(jnp.int32)

    off_lane = ((lane_t < HALO) & last_col) | ((lane_t >= HALO) & (lane_t < 2 * HALO) & first_col)
    off_top = (line_t < HALO) & first_row
    off_bottom = (line_t >= HALO) & last_row
    ends = ((TOP - HALO, off_top), (TOP + rows - HALO, off_bottom))

    def frame(which):
        def value(tile, start, beside):
            if which == 0:
                return right_side(src, lab, tile, start, beside)
            return applied(which - 1, tile, start, beside)

        def side_group(start, off):
            save(which, side_tile, start, jnp.where(off, 0.0, value(side_tile, start, beside_tile)))

        side_group(ends[0][0], off_top | off_lane)
        whole_loop(groups - 1, lambda i: side_group(TOP + HALO + 8 * i, off_lane))
        side_group(ends[1][0], off_bottom | off_lane)
        for start, off in ends:
            save(which, main, start, jnp.where(off[None], 0.0, value(main, start, beside_ring)))

    with jax.named_scope("frames"):
        for which in range(ITERS):
            frame(which)

    with jax.named_scope("moments"):
        sums = [part[i] for i in range(2 * ITERS)]
        on_side = ((lane_t >= 2 * HALO) & (lane_t < 3 * HALO)) | (lane_t >= LANES - HALO)

        def side_body(i, sums):
            new = products(
                side_tile, TOP + 8 * i, beside_tile, lambda p: jnp.where(on_side, p, 0.0))
            return tuple(s + p for s, p in zip(sums, new))

        sums = lax.fori_loop(0, groups, side_body, tuple(sums), unroll=groups)
        for (start, _), on in zip(ends, (line_t >= HALO, line_t < HALO)):
            new = products(main, start, beside_ring, lambda p: jnp.where(on[None], keep_main(p), 0.0))
            sums = [s + fold(p) for s, p in zip(sums, new)]
        lane1 = lane_of((1, LANES))
        mine = jnp.zeros((1, LANES), f32)
        for i, s in enumerate(sums):
            mine = jnp.where(lane1 == i, jnp.sum(s, keepdims=True), mine)
        moment[me] = mine

    with jax.named_scope("send_moments"):
        for_all_others(lambda r, c: pltpu.make_async_remote_copy(
            src_ref=moment.at[me], dst_ref=moment.at[me], send_sem=mom_send, recv_sem=mom_recv,
            device_id=(r, c), device_id_type=MESH).start())

    chips = n_row // 2
    partner = row + 1 - 2 * lax.rem(row, 2)
    quad = rows // 4
    pool4, pool2 = pool_matrix(4), pool_matrix(2)

    def block(w, owner):
        return mids.at[w, :, pl.ds(pl.multiple_of(owner * quad, 8), quad)]

    def peer(step):
        other = row + 2 * step
        return jnp.where(other >= n_row, other - n_row, other)

    def hand(w, owner, target, send, recv):
        return pltpu.make_async_remote_copy(
            src_ref=block(w, owner), dst_ref=block(w, owner), send_sem=send, recv_sem=recv,
            device_id=(target, col), device_id_type=MESH)

    hops = []
    with jax.named_scope("mids"):
        for w in range(ITERS):
            side = vec[w, side_tile, body_rows]
            vec[w, 0, body_rows, :] = jnp.where(
                wide_lane < HALO, pltpu.roll(side, LANES - 2 * HALO, axis=1), vec[w, 0, body_rows])
            vec[w, tiles - 1, body_rows, :] = jnp.where(
                wide_lane >= LANES - HALO, side, vec[w, tiles - 1, body_rows])
            for q in range(tiles // 4):
                mids[w, q, pl.ds(pl.multiple_of(row * quad, 8), quad), :] = pooled(
                    lambda tile, line: vec[w, 4 * q + tile, pl.ds(TOP + line, quad, stride=4), :],
                    4, pool4)
            here = [
                hand(w, row, peer(step), mid_send.at[w, step], mid_recv.at[w, step])
                for step in range(1, chips)
            ]
            here.append(hand(w, row, partner, mid_send.at[w, 0], mid_recv.at[w, 0]))
            for hop in here:
                hop.start()
            hops += here
    with jax.named_scope("fines"):
        for w in range(ITERS):
            for q in range(tiles // 2):
                fines[w, q] = pooled(
                    lambda tile, line: vec[
                        w, 2 * q + tile, pl.ds(TOP + line, rows // 2, stride=2), :],
                    2, pool2)

    with jax.named_scope("wait_moments"):
        everyone = moment.at[pl.ds(0, n - 1)]
        pltpu.make_async_copy(everyone, everyone, mom_recv).wait()
    with jax.named_scope("coefs"):
        total = jnp.sum(moment[...], axis=0)
        moments = [
            0.25 ** i * jnp.sum(jnp.where(lane1 == i, total, 0.0), axis=1, keepdims=True)
            for i in range(2 * ITERS)
        ]
        for w, c in enumerate(coefficients(moments)):
            coord_ref[w] = jnp.broadcast_to(0.25 ** w * c, (8, LANES))

    def source_of(step):
        other = row - 2 * step
        return jnp.where(other < 0, other + n_row, other)

    def other_core(owner):
        return owner + 1 - 2 * lax.rem(owner, 2)

    with jax.named_scope("forwards"):
        forwards = []
        for w in range(ITERS):
            for step in range(1, chips):
                owner = source_of(step)
                hand(w, owner, partner, mid_send.at[w, step], mid_recv.at[w, step]).wait_recv()
                forward = hand(w, owner, partner, fwd_send.at[w, step], fwd_recv.at[w, step])
                forward.start()
                forwards.append(forward)
    with jax.named_scope("wait_forwards"):
        for w in range(ITERS):
            hand(w, partner, partner, mid_send.at[w, 0], mid_recv.at[w, 0]).wait_recv()
            for step in range(1, chips):
                hand(w, other_core(source_of(step)), partner,
                     fwd_send.at[w, step], fwd_recv.at[w, step]).wait_recv()
    with jax.named_scope("wait_sends"):
        for hop in hops:
            hop.wait_send()
        for forward in forwards:
            forward.wait_send()
        for there, copy, back in sends:
            pl.when(there)(copy.wait_send)
        pltpu.make_async_copy(everyone, everyone, mom_send).wait()


def finish_kernel(
    rows, cols, vec, fines, mids, coord_ref, blend_out, fine_out, mid_out, coarse_out,
    blend, fine, mid, coarse, out_sem,
):
    tiles = cols // LANES
    started = []

    def leave(source, target):
        copy = pltpu.make_async_copy(source, target, out_sem.at[len(started)])
        copy.start()
        started.append(copy)

    def combine(load, target, height):
        coords = [coord_ref[w] for w in range(ITERS)]

        def body(g, _):
            start = pl.multiple_of(g * 8, 8)
            strip = None
            for w in range(ITERS):
                term = coords[w] * load(w, start)
                strip = term if strip is None else strip + term
            target[pl.ds(start, 8), :] = strip
            return 0

        lax.fori_loop(0, height // 8, body, 0, unroll=height // 8)

    with jax.named_scope("blend"):
        for t in range(tiles):
            combine(lambda w, start: vec[w, t, pl.ds(start + TOP, 8), :], blend.at[t], rows)
            leave(blend.at[t], blend_out.at[:, pl.ds(t * LANES, LANES)])
    tall = mid.shape[1]
    with jax.named_scope("mid"):
        for q in range(mid.shape[0]):
            combine(lambda w, start: mids[w, q, pl.ds(start, 8), :], mid.at[q], tall)
            leave(mid.at[q], mid_out.at[:, pl.ds(q * LANES, LANES)])
    with jax.named_scope("coarse"):
        pool2 = pool_matrix(2)
        for q in range(coarse.shape[0]):
            coarse[q] = pooled(
                lambda tile, line: mid[2 * q + tile, pl.ds(line, tall // 2, stride=2), :], 2, pool2)
            leave(coarse.at[q], coarse_out.at[:, pl.ds(q * LANES, LANES)])
    with jax.named_scope("fine"):
        for q in range(tiles // 2):
            combine(lambda w, start: fines[w, q, pl.ds(start, 8), :], fine.at[q], rows // 2)
            leave(fine.at[q], fine_out.at[:, pl.ds(q * LANES, LANES)])
    with jax.named_scope("wait_out"):
        for copy in started:
            copy.wait()


def per_device(n_row, n_col, sources, labels):
    kinds, rows, cols = sources.shape
    n = n_row * n_col
    tiles = cols // LANES
    tall = rows + 2 * TOP
    n_pack = HALO * (kinds + 1)
    f32 = jnp.float32
    vmem = pl.BlockSpec(memory_space=pltpu.VMEM)
    hbm = pl.BlockSpec(memory_space=pltpu.HBM)
    mid_rows, coarse_rows = n_row * rows // 4, n_row * rows // 8
    chips = n_row // 2
    dma = pltpu.SemaphoreType.DMA
    vec, fines, mids, coords = pl.pallas_call(
        functools.partial(gather_kernel, n_row, n_col, rows, cols, kinds),
        out_shape=(
            jax.ShapeDtypeStruct((ITERS, tiles + 1, tall, LANES), f32),
            jax.ShapeDtypeStruct((ITERS, tiles // 2, rows // 2, LANES), f32),
            jax.ShapeDtypeStruct((ITERS, tiles // 4, mid_rows, LANES), f32),
            jax.ShapeDtypeStruct((ITERS, 8, LANES), f32),
        ),
        in_specs=[hbm] * 2,
        out_specs=(vmem,) * 4,
        scratch_shapes=[
            pltpu.VMEM((kinds, tiles + 1, tall, LANES), f32),
            pltpu.VMEM((tiles + 1, tall, LANES), jnp.int32),
            pltpu.VMEM((kinds, 2, 8, cols), f32),
            pltpu.VMEM((2, 8, cols), jnp.int32),
            pltpu.VMEM((2, tiles, n_pack, LANES), f32),
            pltpu.VMEM((2, n_pack, rows), f32),
            pltpu.VMEM((2, tiles, n_pack, LANES), f32),
            pltpu.VMEM((2, n_pack, rows), f32),
            pltpu.VMEM((2, 2, n_pack, LANES), f32),
            pltpu.VMEM((2 * ITERS, 8, LANES), f32),
            pltpu.VMEM((n, 1, LANES), f32),
            dma((kinds + 1, tiles + 2)),
            dma((8,)),
            dma((8,)),
            dma,
            dma,
            dma((ITERS, chips)),
            dma((ITERS, chips)),
            dma((ITERS, chips)),
            dma((ITERS, chips)),
        ],
        compiler_params=pltpu.CompilerParams(
            collective_id=0, has_side_effects=True, vmem_limit_bytes=24 * 2**20),
    )(
        pltpu.with_memory_space_constraint(sources, pltpu.HBM),
        pltpu.with_memory_space_constraint(labels, pltpu.HBM),
    )
    return pl.pallas_call(
        functools.partial(finish_kernel, rows, cols),
        out_shape=(
            jax.ShapeDtypeStruct((rows, cols), f32),
            jax.ShapeDtypeStruct((rows // 2, cols // 2), f32),
            jax.ShapeDtypeStruct((mid_rows, cols // 4), f32),
            jax.ShapeDtypeStruct((coarse_rows, cols // 8), f32),
        ),
        in_specs=[vmem] * 4,
        out_specs=(hbm,) * 4,
        scratch_shapes=[
            pltpu.VMEM((tiles, rows, LANES), f32),
            pltpu.VMEM((tiles // 2, rows // 2, LANES), f32),
            pltpu.VMEM((tiles // 4, mid_rows, LANES), f32),
            pltpu.VMEM((tiles // 8, coarse_rows, LANES), f32),
            dma((tiles + tiles // 2 + tiles // 4 + tiles // 8,)),
        ],
        compiler_params=pltpu.CompilerParams(vmem_limit_bytes=24 * 2**20),
    )(vec, fines, mids, coords)


def solution(mesh):
    sizes = dict(mesh.shape)
    return jax.shard_map(
        functools.partial(per_device, sizes["row"], sizes["col"]),
        mesh=mesh,
        in_specs=(P(None, "row", "col"), P("row", "col")),
        out_specs=(P("row", "col"), P("row", "col"), P(None, "col"), P(None, "col")),
        check_vma=False,
    )
```

```python
import functools

import jax
import jax.numpy as jnp
from jax import lax
from jax.experimental import pallas as pl
from jax.experimental.pallas import tpu as pltpu
from jax.sharding import PartitionSpec as P

ITERS = 3
MESH = pl.DeviceIdType.MESH
HALO = 4
TOP = 8
LANES = 128
SIDES = ((-1, -1), (-1, 1), (1, -1), (1, 1), (-1, 0), (1, 0), (0, -1), (0, 1))


def lane_of(shape):
    return lax.broadcasted_iota(jnp.int32, shape, len(shape) - 1)


def line_of(shape):
    return lax.broadcasted_iota(jnp.int32, shape, len(shape) - 2)


def lines(ref, index, start):
    return ref[index + (pl.ds(start, 8), slice(None))]


def beside_ring(mid):
    tiles = mid.shape[0]
    lane = lane_of(mid.shape)
    left = pltpu.roll(mid, 1, axis=2)
    right = pltpu.roll(mid, LANES - 1, axis=2)
    from_left = jnp.concatenate([left[tiles - 1:], left[:tiles - 1]], axis=0)
    from_right = jnp.concatenate([right[1:], right[:1]], axis=0)
    return jnp.where(lane == 0, from_left, left) + jnp.where(lane == LANES - 1, from_right, right)


def beside_tile(mid):
    return pltpu.roll(mid, 1, axis=1) + pltpu.roll(mid, LANES - 1, axis=1)


def neighbour_sum(ref, index, start, mid, beside):
    return (lines(ref, index, start - 1) + lines(ref, index, start + 1)) + beside(mid)


def right_side(src, lab, tile, start, beside):
    here = lines(lab, (tile,), start)
    total = None
    for k in reversed(range(src.shape[0])):
        mid = lines(src, (k, tile), start)
        term = 4.0 * mid - neighbour_sum(src, (k, tile), start, mid, beside)
        total = term if total is None else jnp.where(here == k, term, total)
    return total


def quadratic(left, right, moments, shift):
    total = None
    for i, a in enumerate(left):
        for j, b in enumerate(right):
            term = a * b * moments[i + j + shift]
            total = term if total is None else total + term
    return total


def padded_sum(a, b):
    if len(a) < len(b):
        a, b = b, a
    return [x + b[i] if i < len(b) else x for i, x in enumerate(a)]


def coefficients(moments):
    residual = [jnp.ones_like(moments[0])]
    direction = residual
    solution_coords = [jnp.zeros_like(moments[0])]
    norm_now = moments[0]
    for iteration in range(ITERS):
        applied_dot = 4.0 * (
            quadratic(direction, direction, moments, 0)
            - quadratic(direction, direction, moments, 1)
        )
        step = norm_now / applied_dot
        solution_coords = padded_sum(solution_coords, [step * d for d in direction])
        if iteration + 1 < ITERS:
            moved = [-4.0 * step * d for d in direction]
            residual = padded_sum(residual, moved)
            residual = padded_sum(residual, [jnp.zeros_like(step)] + [-m for m in moved])
            norm_next = quadratic(residual, residual, moments, 0)
            ratio = norm_next / norm_now
            direction = padded_sum(residual, [ratio * d for d in direction])
            norm_now = norm_next
    return solution_coords


def split_dot(values, pool):
    pieces = []
    for _ in range(3):
        pieces.append(values.astype(jnp.bfloat16))
        values = values - pieces[-1].astype(jnp.float32)
    parts = jnp.dot(jnp.concatenate(pieces, axis=0), pool, preferred_element_type=jnp.float32)
    size = values.shape[0]
    return (parts[0:size] + parts[size:2 * size]) + parts[2 * size:]


def pooled(load, stride, pool):
    parts = []
    for tile in range(stride):
        part = load(tile, 0)
        for line in range(1, stride):
            part = part + load(tile, line)
        parts.append(part)
    return split_dot(jnp.concatenate(parts, axis=1), pool)


def pool_matrix(stride):
    shape = (LANES * stride, LANES)
    source, target = (lax.broadcasted_iota(jnp.int32, shape, d) for d in range(2))
    return jnp.where(source // stride == target, 1.0 / (stride * stride), 0.0).astype(jnp.bfloat16)


def gather_kernel(
    n_row, n_col, rows, cols, kinds,
    src_hbm, lab_hbm, vec, fines, mids, coord_ref,
    src, lab, edge, edge_lab, pack_r, pack_c, got_r, got_c, got_d, part, moment,
    band, patch, load_sem, send_sem, recv_sem, chain, mom_send, mom_recv, mid_send, near_recv, far_recv,
    fwd_send, fwd_recv, patch_send, patch_recv,
):
    tiles = cols // LANES
    side_tile = tiles
    main = slice(0, tiles)
    body_rows = pl.ds(TOP, rows)
    n = n_row * n_col
    row, col = lax.axis_index("row"), lax.axis_index("col")
    me = row * n_col + col
    f32 = jnp.float32

    first_row, last_row = row == 0, row == n_row - 1
    first_col, last_col = col == 0, col == n_col - 1
    there = {
        (dr, dc): functools.reduce(jnp.logical_and, [
            jnp.logical_not(edge) for step, edge in (
                (dr < 0, first_row), (dr > 0, last_row), (dc < 0, first_col), (dc > 0, last_col))
            if step])
        for dr, dc in SIDES
    }

    def other_row(step):
        return jnp.where(step >= row, step + 1, step)

    def for_other_rows(act):
        def body(step, _):
            act(other_row(step))
            return 0

        lax.fori_loop(0, n_row - 1, body, 0)

    barrier = pltpu.get_barrier_semaphore()

    def greet(r, c):
        pl.semaphore_signal(barrier, inc=1, device_id=(r, c), device_id_type=MESH)

    greeters = n_row - 1
    for dr, dc in SIDES:
        if dc:
            pl.when(there[dr, dc])(functools.partial(
                greet, jnp.clip(row + dr, 0, n_row - 1), jnp.clip(col + dc, 0, n_col - 1)))
            greeters = greeters + jnp.where(there[dr, dc], 1, 0)
    def plane_load(k, t, wave):
        lanes = pl.ds(t * LANES, LANES)
        if k < kinds:
            return pltpu.make_async_copy(
                src_hbm.at[k, :, lanes], src.at[k, t, body_rows], load_sem.at[2 * wave])
        return pltpu.make_async_copy(
            lab_hbm.at[:, lanes], lab.at[t, body_rows], load_sem.at[2 * wave + 1])

    def edge_load(k, side):
        here = pl.ds(0 if side == 0 else rows - 8, 8)
        if k < kinds:
            return pltpu.make_async_copy(src_hbm.at[k, here], edge.at[k, side], load_sem.at[4])
        return pltpu.make_async_copy(lab_hbm.at[here], edge_lab.at[side], load_sem.at[5])

    def wait_bytes(ref, sem):
        pltpu.make_async_copy(ref, ref, sem).wait()

    for k in range(kinds + 1):
        for side in range(2):
            edge_load(k, side).start()
    for k in range(kinds + 1):
        for t in (0, tiles - 1):
            plane_load(k, t, 0).start()
    for_other_rows(lambda r: greet(r, col))
    for t in range(1, tiles - 1):
        for k in range(kinds + 1):
            plane_load(k, t, 1).start()

    pad = jnp.zeros((tiles + 1, 8, LANES), f32)
    for start in (0, TOP + rows):
        for k in range(kinds):
            src[k, :, pl.ds(start, 8), :] = pad
        lab[:, pl.ds(start, 8), :] = pad.astype(jnp.int32)
        for w in range(ITERS):
            vec[w, :, pl.ds(start, 8), :] = pad

    n_pack = HALO * (kinds + 1)
    with jax.named_scope("wait_first"):
        wait_bytes(edge, load_sem.at[4])
        wait_bytes(edge_lab, load_sem.at[5])
        wait_bytes(src.at[:, pl.ds(0, 2), body_rows], load_sem.at[0])
        wait_bytes(lab.at[pl.ds(0, 2), body_rows], load_sem.at[1])
    with jax.named_scope("pack"):
        for k in range(kinds + 1):
            at = pl.ds(HALO * k, HALO)
            for side in range(2):
                lines_here = pl.ds(0 if side == 0 else 8 - HALO, HALO)
                for t in range(tiles):
                    lanes = pl.ds(t * LANES, LANES)
                    if k < kinds:
                        value = edge[k, side, lines_here, lanes]
                    else:
                        value = edge_lab[side, lines_here, lanes].astype(f32)
                    pack_r[side, t, at, :] = value
        wide_lane = lane_of((rows, LANES))
        for k in range(kinds + 1):
            if k < kinds:
                first, last = src[k, 0, body_rows], src[k, tiles - 1, body_rows]
            else:
                first, last = lab[0, body_rows].astype(f32), lab[tiles - 1, body_rows].astype(f32)
            both = jnp.where(wide_lane < LANES // 2, first, last)
            turned = jnp.transpose(both)
            at = pl.ds(HALO * k, HALO)
            pack_c[0, at, :] = turned[0:HALO]
            pack_c[1, at, :] = turned[LANES - HALO:LANES]

    with jax.named_scope("barrier"):
        pl.semaphore_wait(barrier, greeters)

    sends = []
    for i, (dr, dc) in enumerate(SIDES):
        mine_r, mine_c = (0 if dr < 0 else 1), (0 if dc < 0 else 1)
        if dc == 0:
            source, target, here = pack_r.at[mine_r], got_r.at[1 - mine_r], got_r.at[mine_r]
        elif dr == 0:
            source, target, here = pack_c.at[mine_c], got_c.at[1 - mine_c], got_c.at[mine_c]
        else:
            source = pack_r.at[mine_r, 0 if dc < 0 else tiles - 1]
            target, here = got_d.at[1 - mine_r, 1 - mine_c], got_d.at[mine_r, mine_c]
        opposite = SIDES.index((-dr, -dc))
        device = (
            jnp.clip(row + dr, 0, n_row - 1),
            jnp.clip(col + dc, 0, n_col - 1),
        )
        copy = pltpu.make_async_remote_copy(
            src_ref=source, dst_ref=target, send_sem=send_sem.at[i],
            recv_sem=recv_sem.at[opposite], device_id=device, device_id_type=MESH,
        )
        back = pltpu.make_async_remote_copy(
            src_ref=source, dst_ref=here, send_sem=send_sem.at[i],
            recv_sem=recv_sem.at[i], device_id=device, device_id_type=MESH,
        )
        sends.append((there[dr, dc], copy, back))
        pl.when(there[dr, dc])(copy.start)

    def pass_on(dc):
        pl.semaphore_signal(
            chain.at[0 if dc > 0 else 1], inc=1,
            device_id=(row, jnp.clip(col + dc, 0, n_col - 1)), device_id_type=MESH)

    def hear(dc):
        pl.semaphore_wait(chain.at[0 if dc > 0 else 1], 1)

    def relay(dc):
        hear(dc)
        pass_on(dc)

    inner_col = jnp.logical_and(there[0, 1], there[0, -1])
    upper_half = 2 * col >= n_col
    pl.when(jnp.logical_and(first_col, there[0, 1]))(lambda: pass_on(1))
    pl.when(jnp.logical_and(last_col, there[0, -1]))(lambda: pass_on(-1))

    with jax.named_scope("wait_later"):
        wait_bytes(src.at[:, pl.ds(1, tiles - 2), body_rows], load_sem.at[2])
        wait_bytes(lab.at[pl.ds(1, tiles - 2), body_rows], load_sem.at[3])
    groups = rows // 8
    lane_r = lane_of((tiles, 8, LANES))
    lane_t = lane_of((8, LANES))
    line_t = line_of((8, LANES))

    def whole_loop(count, act):
        def body(i, _):
            act(i)
            return 0

        lax.fori_loop(0, count, body, 0, unroll=count)

    def save(which, tile, start, value):
        vec[which, tile, pl.ds(start, 8), :] = value

    def applied(which, tile, start, beside):
        mid = lines(vec, (which, tile), start)
        return neighbour_sum(vec, (which, tile), start, mid, beside)

    with jax.named_scope("main_b"):
        whole_loop(groups, lambda i: save(
            0, main, TOP + 8 * i, right_side(src, lab, main, TOP + 8 * i, beside_ring)))
    with jax.named_scope("main_v"):
        for which in range(1, ITERS):
            whole_loop(groups, lambda i: save(
                which, main, TOP + 8 * i, applied(which - 1, main, TOP + 8 * i, beside_ring)))

    chips = n_row // 2
    core = lax.rem(row, 2)
    chip = lax.div(row, 2)
    partner = row + 1 - 2 * core
    quad = rows // 4
    pool4, pool2 = pool_matrix(4), pool_matrix(2)

    def some(w, count):
        return mids.at[w, :, pl.ds(0, count * quad)]

    def hand(w, owner, target, send, recv):
        block = mids.at[w, :, pl.ds(pl.multiple_of(owner * quad, 8), quad)]
        pltpu.make_async_remote_copy(
            src_ref=block, dst_ref=block, send_sem=send, recv_sem=recv,
            device_id=(target, col), device_id_type=MESH).start()

    def same_core(q):
        return 2 * q + core

    def to_partner(w, owner):
        hand(w, owner, partner, fwd_send, fwd_recv)

    if chips == 4:
        beside = [chip + 1 - 2 * lax.rem(chip, 2), chip + 2 - 4 * lax.div(chip, 2)]
        across = 3 - chip
        via = same_core(jnp.where(core == 0, beside[0], beside[1]))
        onward = same_core(jnp.where(core == 0, beside[1], beside[0]))
        near = [same_core(q) for q in beside]
    else:
        near = []
        for step in range(1, chips):
            q = chip + step
            near.append(same_core(jnp.where(q >= chips, q - chips, q)))

    with jax.named_scope("early"):
        for w in range(ITERS):
            own = pooled(
                lambda tile, line: jnp.concatenate([
                    vec[w, 4 * q + tile, pl.ds(TOP + line, quad, stride=4), :]
                    for q in range(tiles // 4)], axis=0),
                4, pool4)
            for q in range(tiles // 4):
                mids[w, q, pl.ds(pl.multiple_of(row * quad, 8), quad), :] = own[
                    q * quad:(q + 1) * quad]
            for target in near:
                hand(w, row, target, mid_send, near_recv.at[w])
            to_partner(w, row)

    def products(tile, start, beside, keep):
        powers = [lines(vec, (w, tile), start) for w in range(ITERS)]
        powers.append(neighbour_sum(vec, (ITERS - 1, tile), start, powers[-1], beside))
        kept = [keep(p) for p in powers[:ITERS]]
        return [kept[i // 2] * powers[(i + 1) // 2] for i in range(2 * ITERS)]

    def keep_main(p):
        edge_lane = lane_of((1, 8, LANES))
        return jnp.concatenate([
            jnp.where(edge_lane < HALO, 0.0, p[0:1]), p[1:tiles - 1],
            jnp.where(edge_lane >= LANES - HALO, 0.0, p[tiles - 1:]),
        ], axis=0)

    def fold(value):
        if len(value.shape) == 2:
            return value
        total = value[0]
        for t in range(1, value.shape[0]):
            total = total + value[t]
        return total

    with jax.named_scope("main_m"):
        def main_body(i, sums):
            new = products(main, TOP + HALO + 8 * i, beside_ring, keep_main)
            return tuple(s + fold(p) for s, p in zip(sums, new))

        zero8 = jnp.zeros((8, LANES), f32)
        sums = lax.fori_loop(
            0, groups - 1, main_body, tuple(zero8 for _ in range(2 * ITERS)), unroll=groups - 1)
        for i, s in enumerate(sums):
            part[i] = s
    with jax.named_scope("side_fill"):
        for k in range(kinds + 1):
            if k < kinds:
                first, last = src[k, 0, body_rows], src[k, tiles - 1, body_rows]
                src[k, side_tile, body_rows, :] = jnp.where(
                    wide_lane < LANES // 2, pltpu.roll(first, 2 * HALO, axis=1), last)
            else:
                first, last = lab[0, body_rows], lab[tiles - 1, body_rows]
                lab[side_tile, body_rows, :] = jnp.where(
                    wide_lane < LANES // 2, pltpu.roll(first, 2 * HALO, axis=1), last)

    with jax.named_scope("relay"):
        pl.when(inner_col)(lambda: relay(1))
        pl.when(jnp.logical_and(inner_col, upper_half))(lambda: relay(-1))

    with jax.named_scope("wait_halo"):
        for exists, copy, back in sends:
            pl.when(exists)(back.wait_recv)

    with jax.named_scope("unpack"):
        for k in range(kinds + 1):
            at = pl.ds(HALO * k, HALO)
            right = jnp.where(last_col, 0.0, got_c[1, at, :])
            left = jnp.where(first_col, 0.0, got_c[0, at, :])
            turned = jnp.transpose(jnp.concatenate([right, left], axis=0))
            if k < kinds:
                src[k, side_tile, body_rows, 0:2 * HALO] = turned
            else:
                lab[side_tile, body_rows, 0:2 * HALO] = turned.astype(jnp.int32)
        corner_lane = lane_of((HALO, LANES))
        for side in range(2):
            missing = first_row if side == 0 else last_row
            base = TOP - HALO if side == 0 else TOP + rows
            for k in range(kinds + 1):
                at = pl.ds(HALO * k, HALO)
                wide = [jnp.where(missing, 0.0, got_r[side, t, at, :]) for t in range(tiles)]
                right = jnp.where(missing | last_col, 0.0, got_d[side, 1, at, :])
                left = jnp.where(missing | first_col, 0.0, got_d[side, 0, at, :])
                moved = pltpu.roll(
                    jnp.where(corner_lane >= LANES - HALO, left, wide[0]), 2 * HALO, axis=1)
                own = jnp.where(corner_lane < LANES // 2, moved, wide[-1])
                wide.append(jnp.where(corner_lane < HALO, right, own))
                for t, value in enumerate(wide):
                    if k < kinds:
                        src[k, t, pl.ds(base, HALO), :] = value
                    else:
                        lab[t, pl.ds(base, HALO), :] = value.astype(jnp.int32)

    off_lane = ((lane_t < HALO) & last_col) | ((lane_t >= HALO) & (lane_t < 2 * HALO) & first_col)
    off_top = (line_t < HALO) & first_row
    off_bottom = (line_t >= HALO) & last_row
    ends = ((TOP - HALO, off_top), (TOP + rows - HALO, off_bottom))

    def frame(which):
        def value(tile, start, beside):
            if which == 0:
                return right_side(src, lab, tile, start, beside)
            return applied(which - 1, tile, start, beside)

        def side_group(start, off):
            save(which, side_tile, start, jnp.where(off, 0.0, value(side_tile, start, beside_tile)))

        side_group(ends[0][0], off_top | off_lane)
        whole_loop(groups - 1, lambda i: side_group(TOP + HALO + 8 * i, off_lane))
        side_group(ends[1][0], off_bottom | off_lane)
        for start, off in ends:
            save(which, main, start, jnp.where(off[None], 0.0, value(main, start, beside_ring)))

    with jax.named_scope("frames"):
        for which in range(ITERS):
            frame(which)

    with jax.named_scope("moments"):
        sums = [part[i] for i in range(2 * ITERS)]
        on_side = ((lane_t >= 2 * HALO) & (lane_t < 3 * HALO)) | (lane_t >= LANES - HALO)

        def side_body(i, sums):
            new = products(
                side_tile, TOP + 8 * i, beside_tile, lambda p: jnp.where(on_side, p, 0.0))
            return tuple(s + p for s, p in zip(sums, new))

        sums = lax.fori_loop(0, groups, side_body, tuple(sums), unroll=groups)
        for (start, _), on in zip(ends, (line_t >= HALO, line_t < HALO)):
            new = products(main, start, beside_ring, lambda p: jnp.where(on[None], keep_main(p), 0.0))
            sums = [s + fold(p) for s, p in zip(sums, new)]
        lane1 = lane_of((1, LANES))
        mine = jnp.zeros((1, LANES), f32)
        for i, s in enumerate(sums):
            mine = jnp.where(lane1 == i, jnp.sum(s, keepdims=True), mine)
        moment[me] = mine

    with jax.named_scope("send_moments"):
        pl.when(jnp.logical_and(last_col, there[0, -1]))(lambda: hear(1))

        def tell(r, c):
            pltpu.make_async_remote_copy(
                src_ref=moment.at[me], dst_ref=moment.at[me], send_sem=mom_send, recv_sem=mom_recv,
                device_id=(r, c), device_id_type=MESH).start()

        def tell_block(c):
            def body(r, _):
                tell(r, c)
                return 0

            lax.fori_loop(0, n_row, body, 0)

        for c in range(n_col - 1):
            pl.when(c < col)(functools.partial(tell_block, c))
        for_other_rows(lambda r: tell(r, col))
        pl.when(jnp.logical_and(inner_col, jnp.logical_not(upper_half)))(lambda: relay(-1))

    def tell_rest():
        pl.when(first_col)(lambda: hear(-1))
        for c in range(1, n_col):
            pl.when(c > col)(functools.partial(tell_block, c))

    with jax.named_scope("tell_inner"):
        pl.when(inner_col)(tell_rest)

    ends_of = ((0, TOP), (quad - 1, TOP + rows - 4))
    lines_of = [(w, e, q) for w in range(ITERS) for e in range(2) for q in range(tiles // 4)]
    with jax.named_scope("patch"):
        for at, (w, e, q) in enumerate(lines_of):
            for i in range(4):
                four = vec[w, 4 * q + i, pl.ds(ends_of[e][1], 4), :]
                band[i, at:at + 1, :] = jnp.sum(four, axis=0, keepdims=True)
        wide = jnp.concatenate([band[i] for i in range(4)], axis=1)
        patch[row, 0:wide.shape[0], :] = split_dot(wide, pool4)
        odd = lax.rem(row, 2) == 1
        row_lane = lane_of((1, rows))
        for w in range(ITERS):
            flat = vec[w, side_tile, pl.ds(TOP, quad, stride=4), :]
            for line in range(1, 4):
                flat = flat + vec[w, side_tile, pl.ds(TOP + line, quad, stride=4), :]
            even_part, odd_part = jnp.where(odd, 0.0, flat), jnp.where(odd, flat, 0.0)
            turned = jnp.transpose(jnp.concatenate([even_part, odd_part] * 2, axis=0))
            left = jnp.sum(turned[2 * HALO:3 * HALO], axis=0, keepdims=True)
            right = jnp.sum(turned[LANES - HALO:], axis=0, keepdims=True)
            at = len(lines_of) + w
            patch[row, at:at + 1, :] = jnp.where(row_lane < 2 * quad, left, right) * (1.0 / 16)
        for_other_rows(lambda r: pltpu.make_async_remote_copy(
            src_ref=patch.at[row], dst_ref=patch.at[row], send_sem=patch_send,
            recv_sem=patch_recv, device_id=(r, col), device_id_type=MESH).start())

    with jax.named_scope("near"):
        for w in range(ITERS):
            wait_bytes(some(w, len(near)), near_recv.at[w])
            if chips == 4:
                hand(w, via, onward, mid_send, far_recv.at[w])
            for owner in near:
                to_partner(w, owner)
    with jax.named_scope("merge"):
        for w in range(ITERS):
            side = vec[w, side_tile, body_rows]
            vec[w, 0, body_rows, :] = jnp.where(
                wide_lane < HALO, pltpu.roll(side, LANES - 2 * HALO, axis=1), vec[w, 0, body_rows])
            vec[w, tiles - 1, body_rows, :] = jnp.where(
                wide_lane >= LANES - HALO, side, vec[w, tiles - 1, body_rows])

    with jax.named_scope("fines"):
        half = rows // 2
        for w in range(ITERS):
            own = pooled(
                lambda tile, line: jnp.concatenate([
                    vec[w, 2 * q + tile, pl.ds(TOP + line, half, stride=2), :]
                    for q in range(tiles // 2)], axis=0),
                2, pool2)
            for q in range(tiles // 2):
                fines[w, q] = own[q * half:(q + 1) * half]

    if chips == 4:
        with jax.named_scope("far"):
            for w in range(ITERS):
                wait_bytes(some(w, 1), far_recv.at[w])
                to_partner(w, same_core(across))

    with jax.named_scope("tell_first"):
        pl.when(jnp.logical_and(first_col, there[0, 1]))(tell_rest)

    every_core = mids.at[:, :, pl.ds(0, chips * quad)]
    with jax.named_scope("wait_forwards"):
        wait_bytes(mids.at[:, :, pl.ds(0, (chips - 1) * quad)], mid_send)
        wait_bytes(every_core, fwd_send)
        wait_bytes(every_core, fwd_recv)
    with jax.named_scope("wait_patch"):
        patches = patch.at[pl.ds(0, n_row - 1)]
        wait_bytes(patches, patch_recv)
    with jax.named_scope("apply"):
        for owner in range(n_row):
            for at, (w, e, q) in enumerate(lines_of):
                mids[w, q, pl.ds(owner * quad + ends_of[e][0], 1), :] = patch[
                    owner, at:at + 1, :]
        tall_lane = lane_of((2 * quad, LANES))
        for pair in range(n_row // 2):
            there_rows = pl.ds(2 * pair * quad, 2 * quad)
            for w in range(ITERS):
                at = len(lines_of) + w
                both = patch[2 * pair, at:at + 1, :] + patch[2 * pair + 1, at:at + 1, :]
                turned = jnp.transpose(jnp.broadcast_to(both, (8, LANES)))
                for q, lane, lines_here in (
                        (0, 0, turned[0:2 * quad]),
                        (tiles // 4 - 1, LANES - 1, turned[2 * quad:])):
                    value = jnp.broadcast_to(lines_here[:, 0:1], (2 * quad, LANES))
                    mids[w, q, there_rows, :] = jnp.where(
                        tall_lane == lane, value, mids[w, q, there_rows, :])

    with jax.named_scope("wait_moments"):
        everyone = moment.at[pl.ds(0, n - 1)]
        wait_bytes(everyone, mom_recv)
    with jax.named_scope("coefs"):
        total = jnp.sum(moment[...], axis=0)
        moments = [
            0.25 ** i * jnp.sum(jnp.where(lane1 == i, total, 0.0), axis=1, keepdims=True)
            for i in range(2 * ITERS)
        ]
        for w, c in enumerate(coefficients(moments)):
            coord_ref[w] = jnp.broadcast_to(0.25 ** w * c, (8, LANES))

    with jax.named_scope("wait_sends"):
        for exists, copy, back in sends:
            pl.when(exists)(copy.wait_send)
        wait_bytes(everyone, mom_send)
        wait_bytes(patches, patch_send)


def finish_kernel(
    rows, cols, vec, fines, mids, coord_ref, blend_out, fine_out, mid_out, coarse_out,
    blend, fine, mid, coarse, out_sem,
):
    tiles = cols // LANES

    def leave(which, source, target, q):
        pltpu.make_async_copy(
            source.at[q], target.at[:, pl.ds(q * LANES, LANES)], out_sem.at[which]).start()

    def combine(load, target, height):
        coords = [coord_ref[w] for w in range(ITERS)]

        def body(g, _):
            start = pl.multiple_of(g * 8, 8)
            strip = None
            for w in range(ITERS):
                term = coords[w] * load(w, start)
                strip = term if strip is None else strip + term
            target[pl.ds(start, 8), :] = strip
            return 0

        lax.fori_loop(0, height // 8, body, 0, unroll=height // 8)

    tall = mid.shape[1]
    with jax.named_scope("mid"):
        for q in range(mid.shape[0]):
            combine(lambda w, start: mids[w, q, pl.ds(start, 8), :], mid.at[q], tall)
            leave(1, mid, mid_out, q)
    with jax.named_scope("blend"):
        for t in range(tiles):
            combine(lambda w, start: vec[w, t, pl.ds(start + TOP, 8), :], blend.at[t], rows)
            leave(0, blend, blend_out, t)
    with jax.named_scope("fine"):
        for q in range(tiles // 2):
            combine(lambda w, start: fines[w, q, pl.ds(start, 8), :], fine.at[q], rows // 2)
            leave(2, fine, fine_out, q)
    with jax.named_scope("coarse"):
        pool2 = pool_matrix(2)
        for q in range(coarse.shape[0]):
            coarse[q] = pooled(
                lambda tile, line: mid[2 * q + tile, pl.ds(line, tall // 2, stride=2), :], 2, pool2)
            leave(3, coarse, coarse_out, q)
    with jax.named_scope("wait_out"):
        for which, ref in enumerate((blend, mid, fine, coarse)):
            pltpu.make_async_copy(ref, ref, out_sem.at[which]).wait()


def per_device(n_row, n_col, sources, labels):
    kinds, rows, cols = sources.shape
    n = n_row * n_col
    tiles = cols // LANES
    tall = rows + 2 * TOP
    n_pack = HALO * (kinds + 1)
    f32 = jnp.float32
    vmem = pl.BlockSpec(memory_space=pltpu.VMEM)
    hbm = pl.BlockSpec(memory_space=pltpu.HBM)
    mid_rows, coarse_rows = n_row * rows // 4, n_row * rows // 8
    chips = n_row // 2
    dma = pltpu.SemaphoreType.DMA
    vec, fines, mids, coords = pl.pallas_call(
        functools.partial(gather_kernel, n_row, n_col, rows, cols, kinds),
        out_shape=(
            jax.ShapeDtypeStruct((ITERS, tiles + 1, tall, LANES), f32),
            jax.ShapeDtypeStruct((ITERS, tiles // 2, rows // 2, LANES), f32),
            jax.ShapeDtypeStruct((ITERS, tiles // 4, mid_rows, LANES), f32),
            jax.ShapeDtypeStruct((ITERS, 8, LANES), f32),
        ),
        in_specs=[hbm] * 2,
        out_specs=(vmem,) * 4,
        scratch_shapes=[
            pltpu.VMEM((kinds, tiles + 1, tall, LANES), f32),
            pltpu.VMEM((tiles + 1, tall, LANES), jnp.int32),
            pltpu.VMEM((kinds, 2, 8, cols), f32),
            pltpu.VMEM((2, 8, cols), jnp.int32),
            pltpu.VMEM((2, tiles, n_pack, LANES), f32),
            pltpu.VMEM((2, n_pack, rows), f32),
            pltpu.VMEM((2, tiles, n_pack, LANES), f32),
            pltpu.VMEM((2, n_pack, rows), f32),
            pltpu.VMEM((2, 2, n_pack, LANES), f32),
            pltpu.VMEM((2 * ITERS, 8, LANES), f32),
            pltpu.VMEM((n, 1, LANES), f32),
            pltpu.VMEM((4, ITERS * (tiles // 2), LANES), f32),
            pltpu.VMEM((n_row, ITERS * (tiles // 2) + 4, LANES), f32),
            dma((6,)),
            dma((8,)),
            dma((8,)),
            pltpu.SemaphoreType.REGULAR((2,)),
            dma,
            dma,
            dma,
            dma((ITERS,)),
            dma((ITERS,)),
            dma,
            dma,
            dma,
            dma,
        ],
        compiler_params=pltpu.CompilerParams(
            collective_id=0, has_side_effects=True, vmem_limit_bytes=24 * 2**20),
    )(
        pltpu.with_memory_space_constraint(sources, pltpu.HBM),
        pltpu.with_memory_space_constraint(labels, pltpu.HBM),
    )
    return pl.pallas_call(
        functools.partial(finish_kernel, rows, cols),
        out_shape=(
            jax.ShapeDtypeStruct((rows, cols), f32),
            jax.ShapeDtypeStruct((rows // 2, cols // 2), f32),
            jax.ShapeDtypeStruct((mid_rows, cols // 4), f32),
            jax.ShapeDtypeStruct((coarse_rows, cols // 8), f32),
        ),
        in_specs=[vmem] * 4,
        out_specs=(hbm,) * 4,
        scratch_shapes=[
            pltpu.VMEM((tiles, rows, LANES), f32),
            pltpu.VMEM((tiles // 2, rows // 2, LANES), f32),
            pltpu.VMEM((tiles // 4, mid_rows, LANES), f32),
            pltpu.VMEM((tiles // 8, coarse_rows, LANES), f32),
            dma((4,)),
        ],
        compiler_params=pltpu.CompilerParams(vmem_limit_bytes=24 * 2**20),
    )(vec, fines, mids, coords)


def solution(mesh):
    sizes = dict(mesh.shape)
    return jax.shard_map(
        functools.partial(per_device, sizes["row"], sizes["col"]),
        mesh=mesh,
        in_specs=(P(None, "row", "col"), P("row", "col")),
        out_specs=(P("row", "col"), P("row", "col"), P(None, "col"), P(None, "col")),
        check_vma=False,
    )
```

```python
import functools

import jax
import jax.numpy as jnp
from jax import lax
from jax.experimental import pallas as pl
from jax.experimental.pallas import tpu as pltpu
from jax.sharding import PartitionSpec as P

ITERS = 3
DIRECT = 3
MESH = pl.DeviceIdType.MESH
HALO = 4
TOP = 8
LANES = 128
SIDES = ((-1, -1), (-1, 1), (1, -1), (1, 1), (-1, 0), (1, 0), (0, -1), (0, 1))


def lane_of(shape):
    return lax.broadcasted_iota(jnp.int32, shape, len(shape) - 1)


def line_of(shape):
    return lax.broadcasted_iota(jnp.int32, shape, len(shape) - 2)


def lines(ref, index, start):
    return ref[index + (pl.ds(start, 8), slice(None))]


def beside_ring(mid):
    tiles = mid.shape[0]
    lane = lane_of(mid.shape)
    left = pltpu.roll(mid, 1, axis=2)
    right = pltpu.roll(mid, LANES - 1, axis=2)
    from_left = jnp.concatenate([left[tiles - 1:], left[:tiles - 1]], axis=0)
    from_right = jnp.concatenate([right[1:], right[:1]], axis=0)
    return jnp.where(lane == 0, from_left, left) + jnp.where(lane == LANES - 1, from_right, right)


def beside_tile(mid):
    return pltpu.roll(mid, 1, axis=1) + pltpu.roll(mid, LANES - 1, axis=1)


def neighbour_sum(ref, index, start, mid, beside):
    return (lines(ref, index, start - 1) + lines(ref, index, start + 1)) + beside(mid)


def right_side(src, lab, tile, start, beside):
    here = lines(lab, (tile,), start)
    total = None
    for k in reversed(range(src.shape[0])):
        mid = lines(src, (k, tile), start)
        term = 4.0 * mid - neighbour_sum(src, (k, tile), start, mid, beside)
        total = term if total is None else jnp.where(here == k, term, total)
    return total


def from_left(values):
    lane = lane_of(values.shape)
    moved = pltpu.roll(values, 1, axis=2)
    return jnp.where(lane == 0, jnp.concatenate([moved[-1:], moved[:-1]], axis=0), moved)


def from_right(values):
    lane = lane_of(values.shape)
    moved = pltpu.roll(values, LANES - 1, axis=2)
    return jnp.where(lane == LANES - 1, jnp.concatenate([moved[1:], moved[:1]], axis=0), moved)


def chosen(here, values):
    total = values[-1]
    for k in reversed(range(len(values) - 1)):
        total = jnp.where(here == k, values[k], total)
    return total


def beside_chosen(src, lab, tile, start):
    here = lines(lab, (tile,), start)
    mids = [lines(src, (k, tile), start) for k in range(src.shape[0])]
    return chosen(from_right(here), mids), chosen(from_left(here), mids)


def right_side_ring(src, lab, tile, start, left, right):
    here = lines(lab, (tile,), start)
    crosses = [
        4.0 * lines(src, (k, tile), start)
        - (lines(src, (k, tile), start - 1) + lines(src, (k, tile), start + 1))
        for k in range(src.shape[0])
    ]
    return chosen(here, crosses) - (from_left(left) + from_right(right))


def quadratic(left, right, moments, shift):
    total = None
    for i, a in enumerate(left):
        for j, b in enumerate(right):
            term = a * b * moments[i + j + shift]
            total = term if total is None else total + term
    return total


def padded_sum(a, b):
    if len(a) < len(b):
        a, b = b, a
    return [x + b[i] if i < len(b) else x for i, x in enumerate(a)]


def coefficients(moments):
    residual = [jnp.ones_like(moments[0])]
    direction = residual
    solution_coords = [jnp.zeros_like(moments[0])]
    norm_now = moments[0]
    for iteration in range(ITERS):
        applied_dot = 4.0 * (
            quadratic(direction, direction, moments, 0)
            - quadratic(direction, direction, moments, 1)
        )
        step = norm_now / applied_dot
        solution_coords = padded_sum(solution_coords, [step * d for d in direction])
        if iteration + 1 < ITERS:
            moved = [-4.0 * step * d for d in direction]
            residual = padded_sum(residual, moved)
            residual = padded_sum(residual, [jnp.zeros_like(step)] + [-m for m in moved])
            norm_next = quadratic(residual, residual, moments, 0)
            ratio = norm_next / norm_now
            direction = padded_sum(residual, [ratio * d for d in direction])
            norm_now = norm_next
    return solution_coords


def split_dot(values, pool):
    pieces = []
    for _ in range(3):
        pieces.append(values.astype(jnp.bfloat16))
        values = values - pieces[-1].astype(jnp.float32)
    parts = jnp.dot(jnp.concatenate(pieces, axis=0), pool, preferred_element_type=jnp.float32)
    size = values.shape[0]
    return (parts[0:size] + parts[size:2 * size]) + parts[2 * size:]


def pooled(load, stride, pool):
    parts = []
    for tile in range(stride):
        part = load(tile, 0)
        for line in range(1, stride):
            part = part + load(tile, line)
        parts.append(part)
    return split_dot(jnp.concatenate(parts, axis=1), pool)


def pool_matrix(stride):
    shape = (LANES * stride, LANES)
    source, target = (lax.broadcasted_iota(jnp.int32, shape, d) for d in range(2))
    return jnp.where(source // stride == target, 1.0 / (stride * stride), 0.0).astype(jnp.bfloat16)


def gather_kernel(
    n_row, n_col, rows, cols, kinds,
    src_hbm, lab_hbm, vec, fines, mids, coord_ref,
    src, lab, edge, edge_lab, pack_up, pack_down, pack_c, pack_d, got_up, got_down, got_c, got_d,
    part, moment, band, patch, sides, load_sem, send_sem, recv_sem, chain, mom_send, mom_recv, mid_send, near_recv, far_recv,
    fwd_send, fwd_recv, patch_send, patch_recv,
):
    tiles = cols // LANES
    side_tile = tiles
    main = slice(0, tiles)
    body_rows = pl.ds(TOP, rows)
    n = n_row * n_col
    row, col = lax.axis_index("row"), lax.axis_index("col")
    me = row * n_col + col
    f32 = jnp.float32

    first_row, last_row = row == 0, row == n_row - 1
    first_col, last_col = col == 0, col == n_col - 1
    there = {
        (dr, dc): functools.reduce(jnp.logical_and, [
            jnp.logical_not(edge) for step, edge in (
                (dr < 0, first_row), (dr > 0, last_row), (dc < 0, first_col), (dc > 0, last_col))
            if step])
        for dr, dc in SIDES
    }

    def other_row(step):
        return jnp.where(step >= row, step + 1, step)

    def for_other_rows(act):
        def body(step, _):
            act(other_row(step))
            return 0

        lax.fori_loop(0, n_row - 1, body, 0)

    barrier = pltpu.get_barrier_semaphore()

    def greet(r, c):
        pl.semaphore_signal(barrier, inc=1, device_id=(r, c), device_id_type=MESH)

    greeters = n_row - 1
    for dr, dc in SIDES:
        if dc:
            pl.when(there[dr, dc])(functools.partial(
                greet, jnp.clip(row + dr, 0, n_row - 1), jnp.clip(col + dc, 0, n_col - 1)))
            greeters = greeters + jnp.where(there[dr, dc], 1, 0)
    def plane_load(k, t, wave):
        lanes = pl.ds(t * LANES, LANES)
        if k < kinds:
            return pltpu.make_async_copy(
                src_hbm.at[k, :, lanes], src.at[k, t, body_rows], load_sem.at[2 * wave])
        return pltpu.make_async_copy(
            lab_hbm.at[:, lanes], lab.at[t, body_rows], load_sem.at[2 * wave + 1])

    def edge_load(k, side):
        here = pl.ds(0 if side == 0 else rows - 8, 8)
        if k < kinds:
            return pltpu.make_async_copy(src_hbm.at[k, here], edge.at[k, side], load_sem.at[4])
        return pltpu.make_async_copy(lab_hbm.at[here], edge_lab.at[side], load_sem.at[5])

    def wait_bytes(ref, sem):
        pltpu.make_async_copy(ref, ref, sem).wait()

    for k in range(kinds + 1):
        for side in range(2):
            edge_load(k, side).start()
    for k in range(kinds + 1):
        for t in (0, tiles - 1):
            plane_load(k, t, 0).start()
    for_other_rows(lambda r: greet(r, col))
    for t in range(1, tiles - 1):
        for k in range(kinds + 1):
            plane_load(k, t, 1).start()

    pad = jnp.zeros((tiles + 1, 8, LANES), f32)
    for start in (0, TOP + rows):
        for k in range(kinds):
            src[k, :, pl.ds(start, 8), :] = pad
        lab[:, pl.ds(start, 8), :] = pad.astype(jnp.int32)
        for w in range(ITERS):
            vec[w, :, pl.ds(start, 8), :] = pad

    def row_part(side, k, t):
        depth = HALO - side
        each = kinds * depth + depth - 1
        return (depth if k < kinds else depth - 1), t * each + k * depth

    n_pack = HALO * (kinds + 1)
    with jax.named_scope("wait_first"):
        wait_bytes(edge, load_sem.at[4])
        wait_bytes(edge_lab, load_sem.at[5])
        wait_bytes(src.at[:, pl.ds(0, 2), body_rows], load_sem.at[0])
        wait_bytes(lab.at[pl.ds(0, 2), body_rows], load_sem.at[1])
    with jax.named_scope("pack"):
        for side in range(2):
            for k in range(kinds + 1):
                for t in range(tiles):
                    lanes = pl.ds(t * LANES, LANES)
                    depth, at = row_part(side, k, t)
                    lines_here = pl.ds(0 if side == 0 else 8 - depth, depth)
                    if k < kinds:
                        value = edge[k, side, lines_here, lanes]
                    else:
                        value = edge_lab[side, lines_here, lanes].astype(f32)
                    (pack_up if side == 0 else pack_down)[pl.ds(at, depth), :] = value
                for end, t in enumerate((0, tiles - 1)):
                    lanes = pl.ds(t * LANES, LANES)
                    lines_here = pl.ds(0 if side == 0 else 8 - HALO, HALO)
                    if k < kinds:
                        value = edge[k, side, lines_here, lanes]
                    else:
                        value = edge_lab[side, lines_here, lanes].astype(f32)
                    pack_d[side, end, pl.ds(HALO * k, HALO), :] = value
        wide_lane = lane_of((rows, LANES))
        for k in range(kinds + 1):
            if k < kinds:
                first, last = src[k, 0, body_rows], src[k, tiles - 1, body_rows]
            else:
                first, last = lab[0, body_rows].astype(f32), lab[tiles - 1, body_rows].astype(f32)
            both = jnp.where(wide_lane < LANES // 2, first, last)
            turned = jnp.transpose(both)
            at = pl.ds(HALO * k, HALO)
            pack_c[0, at, :] = turned[0:HALO]
            pack_c[1, at, :] = turned[LANES - HALO:LANES]

    with jax.named_scope("barrier"):
        pl.semaphore_wait(barrier, greeters)

    sends = []
    for i, (dr, dc) in enumerate(SIDES):
        mine_r, mine_c = (0 if dr < 0 else 1), (0 if dc < 0 else 1)
        if dc == 0:
            source, target, here = (
                (pack_up, got_up, got_down) if dr < 0 else (pack_down, got_down, got_up))
        elif dr == 0:
            source, target, here = pack_c.at[mine_c], got_c.at[1 - mine_c], got_c.at[mine_c]
        else:
            source = pack_d.at[mine_r, mine_c]
            target, here = got_d.at[1 - mine_r, 1 - mine_c], got_d.at[mine_r, mine_c]
        opposite = SIDES.index((-dr, -dc))
        device = (
            jnp.clip(row + dr, 0, n_row - 1),
            jnp.clip(col + dc, 0, n_col - 1),
        )
        copy = pltpu.make_async_remote_copy(
            src_ref=source, dst_ref=target, send_sem=send_sem.at[i],
            recv_sem=recv_sem.at[opposite], device_id=device, device_id_type=MESH,
        )
        back = pltpu.make_async_remote_copy(
            src_ref=source, dst_ref=here, send_sem=send_sem.at[i],
            recv_sem=recv_sem.at[i], device_id=device, device_id_type=MESH,
        )
        sends.append((there[dr, dc], copy, back))
        pl.when(there[dr, dc])(copy.start)

    def pass_on(dc):
        pl.semaphore_signal(
            chain.at[0 if dc > 0 else 1], inc=1,
            device_id=(row, jnp.clip(col + dc, 0, n_col - 1)), device_id_type=MESH)

    def hear(dc):
        pl.semaphore_wait(chain.at[0 if dc > 0 else 1], 1)

    def relay(dc):
        hear(dc)
        pass_on(dc)

    inner_col = jnp.logical_and(there[0, 1], there[0, -1])
    upper_half = 2 * col >= n_col
    pl.when(jnp.logical_and(first_col, there[0, 1]))(lambda: pass_on(1))
    pl.when(jnp.logical_and(last_col, there[0, -1]))(lambda: pass_on(-1))

    with jax.named_scope("wait_later"):
        wait_bytes(src.at[:, pl.ds(1, tiles - 2), body_rows], load_sem.at[2])
        wait_bytes(lab.at[pl.ds(1, tiles - 2), body_rows], load_sem.at[3])
    groups = rows // 8
    lane_r = lane_of((tiles, 8, LANES))
    lane_t = lane_of((8, LANES))
    line_t = line_of((8, LANES))

    def whole_loop(count, act):
        def body(i, _):
            act(i)
            return 0

        lax.fori_loop(0, count, body, 0, unroll=count)

    def save(which, tile, start, value):
        vec[which, tile, pl.ds(start, 8), :] = value

    def applied(which, tile, start, beside):
        mid = lines(vec, (which, tile), start)
        return neighbour_sum(vec, (which, tile), start, mid, beside)

    with jax.named_scope("main_b"):
        def choose(i):
            start = TOP + 8 * i
            left, right = beside_chosen(src, lab, main, start)
            save(1, main, start, left)
            save(2, main, start, right)

        whole_loop(groups, choose)
        whole_loop(groups, lambda i: save(0, main, TOP + 8 * i, right_side_ring(
            src, lab, main, TOP + 8 * i,
            lines(vec, (1, main), TOP + 8 * i), lines(vec, (2, main), TOP + 8 * i))))

    def inner(which):
        whole_loop(groups, lambda i: save(
            which, main, TOP + 8 * i, applied(which - 1, main, TOP + 8 * i, beside_ring)))


    chips = n_row // 2
    core = lax.rem(row, 2)
    chip = lax.div(row, 2)
    partner = row + 1 - 2 * core
    quad = rows // 4
    pool4, pool2 = pool_matrix(4), pool_matrix(2)

    def some(w, count):
        return mids.at[w, :, pl.ds(0, count * quad)]

    def hand(w, owner, target, send, recv):
        block = mids.at[w, :, pl.ds(pl.multiple_of(owner * quad, 8), quad)]
        pltpu.make_async_remote_copy(
            src_ref=block, dst_ref=block, send_sem=send, recv_sem=recv,
            device_id=(target, col), device_id_type=MESH).start()

    def same_core(q):
        return 2 * q + core

    def to_partner(w, owner):
        hand(w, owner, partner, fwd_send, fwd_recv)

    if chips == 4:
        beside = [chip + 1 - 2 * lax.rem(chip, 2), chip + 2 - 4 * lax.div(chip, 2)]
        across = 3 - chip
        via = same_core(jnp.where(core == 0, beside[0], beside[1]))
        onward = same_core(jnp.where(core == 0, beside[1], beside[0]))
        near = [same_core(q) for q in beside]
    else:
        near = []
        for step in range(1, chips):
            q = chip + step
            near.append(same_core(jnp.where(q >= chips, q - chips, q)))

    def send_early(w):
        own = pooled(
            lambda tile, line: jnp.concatenate([
                vec[w, 4 * q + tile, pl.ds(TOP + line, quad, stride=4), :]
                for q in range(tiles // 4)], axis=0),
            4, pool4)
        for q in range(tiles // 4):
            mids[w, q, pl.ds(pl.multiple_of(row * quad, 8), quad), :] = own[
                q * quad:(q + 1) * quad]
        for target in near:
            hand(w, row, target, mid_send, near_recv.at[w])
        if chips == 4 and w < DIRECT:
            hand(w, row, same_core(across), mid_send, far_recv.at[w])
        to_partner(w, row)

    with jax.named_scope("main_v"):
        for w in range(1, ITERS):
            inner(w)
            send_early(w - 1)
        send_early(ITERS - 1)

    def products(tile, start, right_of, keep):
        powers = [lines(vec, (w, tile), start) for w in range(ITERS)]
        powers.append(lines(vec, (ITERS - 1, tile), start + 1) + right_of(powers[-1]))
        kept = [keep(p) for p in powers[:ITERS]]
        return [kept[i // 2] * powers[(i + 1) // 2] for i in range(2 * ITERS)]

    def right_ring(mid):
        right = pltpu.roll(mid, LANES - 1, axis=2)
        return jnp.where(
            lane_r == LANES - 1, jnp.concatenate([right[1:], right[:1]], axis=0), right)

    def right_tile(mid):
        return pltpu.roll(mid, LANES - 1, axis=1)

    def keep_main(p):
        edge_lane = lane_of((1, 8, LANES))
        return jnp.concatenate([
            jnp.where(edge_lane < HALO, 0.0, p[0:1]), p[1:tiles - 1],
            jnp.where(edge_lane >= LANES - HALO, 0.0, p[tiles - 1:]),
        ], axis=0)

    def fold(value):
        if len(value.shape) == 2:
            return value
        total = value[0]
        for t in range(1, value.shape[0]):
            total = total + value[t]
        return total

    with jax.named_scope("main_m"):
        def main_body(i, sums):
            new = products(main, TOP + HALO + 8 * i, right_ring, keep_main)
            return tuple(s + fold(p) for s, p in zip(sums, new))

        zero8 = jnp.zeros((8, LANES), f32)
        sums = lax.fori_loop(
            0, groups - 1, main_body, tuple(zero8 for _ in range(2 * ITERS)), unroll=groups - 1)
        for i, s in enumerate(sums):
            part[i] = s
    with jax.named_scope("side_fill"):
        for k in range(kinds + 1):
            if k < kinds:
                first, last = src[k, 0, body_rows], src[k, tiles - 1, body_rows]
                src[k, side_tile, body_rows, :] = jnp.where(
                    wide_lane < LANES // 2, pltpu.roll(first, 2 * HALO, axis=1), last)
            else:
                first, last = lab[0, body_rows], lab[tiles - 1, body_rows]
                lab[side_tile, body_rows, :] = jnp.where(
                    wide_lane < LANES // 2, pltpu.roll(first, 2 * HALO, axis=1), last)

    with jax.named_scope("relay"):
        pl.when(inner_col)(lambda: relay(1))
        pl.when(jnp.logical_and(inner_col, upper_half))(lambda: relay(-1))

    with jax.named_scope("wait_halo"):
        for exists, copy, back in sends:
            pl.when(exists)(back.wait_recv)

    with jax.named_scope("unpack"):
        for k in range(kinds + 1):
            at = pl.ds(HALO * k, HALO)
            right = jnp.where(last_col, 0.0, got_c[1, at, :])
            left = jnp.where(first_col, 0.0, got_c[0, at, :])
            turned = jnp.transpose(jnp.concatenate([right, left], axis=0))
            if k < kinds:
                src[k, side_tile, body_rows, 0:2 * HALO] = turned
            else:
                lab[side_tile, body_rows, 0:2 * HALO] = turned.astype(jnp.int32)
        corner_lane = lane_of((HALO, LANES))
        for side in range(2):
            missing = first_row if side == 0 else last_row
            got = got_down if side == 0 else got_up
            for k in range(kinds + 1):
                wide = []
                for t in range(tiles):
                    depth, at = row_part(1 - side, k, t)
                    wide.append(jnp.where(missing, 0.0, got[pl.ds(at, depth), :]))
                shift = HALO - depth if side == 0 else 0
                near_lines = slice(shift, shift + depth)
                at = pl.ds(HALO * k, HALO)
                right = jnp.where(missing | last_col, 0.0, got_d[side, 1, at, :])[near_lines]
                left = jnp.where(missing | first_col, 0.0, got_d[side, 0, at, :])[near_lines]
                corner_lane = lane_of((depth, LANES))
                moved = pltpu.roll(
                    jnp.where(corner_lane >= LANES - HALO, left, wide[0]), 2 * HALO, axis=1)
                own = jnp.where(corner_lane < LANES // 2, moved, wide[-1])
                wide.append(jnp.where(corner_lane < HALO, right, own))
                base = TOP - depth if side == 0 else TOP + rows
                for t, value in enumerate(wide):
                    if k < kinds:
                        src[k, t, pl.ds(base, depth), :] = value
                    else:
                        lab[t, pl.ds(base, depth), :] = value.astype(jnp.int32)

    off_lane = ((lane_t < HALO) & last_col) | ((lane_t >= HALO) & (lane_t < 2 * HALO) & first_col)
    off_top = (line_t < HALO) & first_row
    off_bottom = (line_t >= HALO) & last_row
    ends = ((TOP - HALO, off_top), (TOP + rows - HALO, off_bottom))

    def frame(which):
        def value(tile, start, beside):
            if which == 0:
                return right_side(src, lab, tile, start, beside)
            return applied(which - 1, tile, start, beside)

        def side_group(start, off):
            save(which, side_tile, start, jnp.where(off, 0.0, value(side_tile, start, beside_tile)))

        side_group(ends[0][0], off_top | off_lane)
        whole_loop(groups - 1, lambda i: side_group(TOP + HALO + 8 * i, off_lane))
        side_group(ends[1][0], off_bottom | off_lane)
        for start, off in ends:
            save(which, main, start, jnp.where(off[None], 0.0, value(main, start, beside_ring)))

    with jax.named_scope("frames"):
        for which in range(ITERS):
            frame(which)

    with jax.named_scope("moments"):
        sums = [part[i] for i in range(2 * ITERS)]
        on_side = ((lane_t >= 2 * HALO) & (lane_t < 3 * HALO)) | (lane_t >= LANES - HALO)

        def side_body(i, sums):
            new = products(
                side_tile, TOP + 8 * i, right_tile, lambda p: jnp.where(on_side, p, 0.0))
            return tuple(s + p for s, p in zip(sums, new))

        sums = lax.fori_loop(0, groups, side_body, tuple(sums), unroll=groups)
        for (start, _), on in zip(ends, (line_t >= HALO, line_t < HALO)):
            new = products(main, start, right_ring, lambda p: jnp.where(on[None], keep_main(p), 0.0))
            sums = [s + fold(p) for s, p in zip(sums, new)]
        lane1 = lane_of((1, LANES))
        mine = jnp.zeros((1, LANES), f32)
        for i, s in enumerate(sums):
            mine = jnp.where(lane1 == i, jnp.sum(s, keepdims=True), mine)
        moment[me] = mine

    with jax.named_scope("send_moments"):
        pl.when(jnp.logical_and(last_col, there[0, -1]))(lambda: hear(1))

        def tell(r, c):
            pltpu.make_async_remote_copy(
                src_ref=moment.at[me], dst_ref=moment.at[me], send_sem=mom_send, recv_sem=mom_recv,
                device_id=(r, c), device_id_type=MESH).start()

        def tell_block(c):
            def body(r, _):
                tell(r, c)
                return 0

            lax.fori_loop(0, n_row, body, 0)

        for c in range(n_col - 1):
            pl.when(c < col)(functools.partial(tell_block, c))
        for_other_rows(lambda r: tell(r, col))
        pl.when(jnp.logical_and(inner_col, jnp.logical_not(upper_half)))(lambda: relay(-1))

    def tell_rest():
        pl.when(first_col)(lambda: hear(-1))
        for c in range(1, n_col):
            pl.when(c > col)(functools.partial(tell_block, c))

    with jax.named_scope("tell_inner"):
        pl.when(inner_col)(tell_rest)

    ends_of = ((0, TOP), (quad - 1, TOP + rows - 4))
    lines_of = [(w, e, q) for w in range(ITERS) for e in range(2) for q in range(tiles // 4)]
    with jax.named_scope("patch"):
        for at, (w, e, q) in enumerate(lines_of):
            for i in range(4):
                four = vec[w, 4 * q + i, pl.ds(ends_of[e][1], 4), :]
                band[i, at:at + 1, :] = jnp.sum(four, axis=0, keepdims=True)
        wide = jnp.concatenate([band[i] for i in range(4)], axis=1)
        patch[row, 0:wide.shape[0], :] = split_dot(wide, pool4)
        odd = lax.rem(row, 2) == 1
        row_lane = lane_of((1, rows))
        for w in range(ITERS):
            flat = vec[w, side_tile, pl.ds(TOP, quad, stride=4), :]
            for line in range(1, 4):
                flat = flat + vec[w, side_tile, pl.ds(TOP + line, quad, stride=4), :]
            even_part, odd_part = jnp.where(odd, 0.0, flat), jnp.where(odd, flat, 0.0)
            turned = jnp.transpose(jnp.concatenate([even_part, odd_part] * 2, axis=0))
            left = jnp.sum(turned[2 * HALO:3 * HALO], axis=0, keepdims=True)
            right = jnp.sum(turned[LANES - HALO:], axis=0, keepdims=True)
            at = len(lines_of) + w
            patch[row, at:at + 1, :] = jnp.where(row_lane < 2 * quad, left, right) * (1.0 / 16)
        for_other_rows(lambda r: pltpu.make_async_remote_copy(
            src_ref=patch.at[row], dst_ref=patch.at[row], send_sem=patch_send,
            recv_sem=patch_recv, device_id=(r, col), device_id_type=MESH).start())

    with jax.named_scope("near"):
        for w in range(ITERS):
            wait_bytes(some(w, len(near)), near_recv.at[w])
            if chips == 4 and w >= DIRECT:
                hand(w, via, onward, mid_send, far_recv.at[w])
            for owner in near:
                to_partner(w, owner)
    with jax.named_scope("merge"):
        for w in range(ITERS):
            side = vec[w, side_tile, body_rows]
            vec[w, 0, body_rows, :] = jnp.where(
                wide_lane < HALO, pltpu.roll(side, LANES - 2 * HALO, axis=1), vec[w, 0, body_rows])
            vec[w, tiles - 1, body_rows, :] = jnp.where(
                wide_lane >= LANES - HALO, side, vec[w, tiles - 1, body_rows])

    with jax.named_scope("fines"):
        half = rows // 2
        for w in range(ITERS):
            own = pooled(
                lambda tile, line: jnp.concatenate([
                    vec[w, 2 * q + tile, pl.ds(TOP + line, half, stride=2), :]
                    for q in range(tiles // 2)], axis=0),
                2, pool2)
            for q in range(tiles // 2):
                fines[w, q] = own[q * half:(q + 1) * half]

    with jax.named_scope("tell_first"):
        pl.when(jnp.logical_and(first_col, there[0, 1]))(tell_rest)

    if chips == 4:
        with jax.named_scope("far"):
            for w in range(ITERS):
                wait_bytes(some(w, 1), far_recv.at[w])
                to_partner(w, same_core(across))

    with jax.named_scope("wait_patch"):
        patches = patch.at[pl.ds(0, n_row - 1)]
        wait_bytes(patches, patch_recv)
    with jax.named_scope("prepare"):
        for pair in range(n_row // 2):
            for w in range(ITERS):
                at = len(lines_of) + w
                both = patch[2 * pair, at:at + 1, :] + patch[2 * pair + 1, at:at + 1, :]
                turned = jnp.transpose(jnp.broadcast_to(both, (8, LANES)))
                for end in range(2):
                    part_here = turned[2 * quad * end:2 * quad * (end + 1), 0:1]
                    sides[w, end, pl.ds(2 * pair * quad, 2 * quad), :] = jnp.broadcast_to(
                        part_here, (2 * quad, LANES))

    every_core = mids.at[:, :, pl.ds(0, chips * quad)]
    with jax.named_scope("wait_forwards"):
        wait_bytes(mids.at[:, :, pl.ds(0, (chips - 1) * quad)], mid_send)
        wait_bytes(every_core, fwd_send)
        wait_bytes(every_core, fwd_recv)
    with jax.named_scope("apply"):
        for owner in range(n_row):
            for at, (w, e, q) in enumerate(lines_of):
                mids[w, q, pl.ds(owner * quad + ends_of[e][0], 1), :] = patch[
                    owner, at:at + 1, :]
        all_lane = lane_of((n_row * quad, LANES))
        for w in range(ITERS):
            for end, q, lane in ((0, 0, 0), (1, tiles // 4 - 1, LANES - 1)):
                mids[w, q] = jnp.where(all_lane == lane, sides[w, end], mids[w, q])

    with jax.named_scope("wait_moments"):
        everyone = moment.at[pl.ds(0, n - 1)]
        wait_bytes(everyone, mom_recv)
    with jax.named_scope("coefs"):
        total = jnp.sum(moment[...], axis=0)
        moments = [
            (0.25 ** i * (1.0 if i < 2 * ITERS - 1 else 2.0))
            * jnp.sum(jnp.where(lane1 == i, total, 0.0), axis=1, keepdims=True)
            for i in range(2 * ITERS)
        ]
        for w, c in enumerate(coefficients(moments)):
            coord_ref[w] = jnp.broadcast_to(0.25 ** w * c, (8, LANES))

    with jax.named_scope("wait_sends"):
        for exists, copy, back in sends:
            pl.when(exists)(copy.wait_send)
        wait_bytes(everyone, mom_send)
        wait_bytes(patches, patch_send)


def finish_kernel(
    rows, cols, vec, fines, mids, coord_ref, blend_out, fine_out, mid_out, coarse_out,
    blend, fine, mid, coarse, out_sem,
):
    tiles = cols // LANES

    def leave(which, source, target, q):
        pltpu.make_async_copy(
            source.at[q], target.at[:, pl.ds(q * LANES, LANES)], out_sem.at[which]).start()

    def combine(load, target, height):
        coords = [coord_ref[w] for w in range(ITERS)]

        def body(g, _):
            start = pl.multiple_of(g * 8, 8)
            strip = None
            for w in range(ITERS):
                term = coords[w] * load(w, start)
                strip = term if strip is None else strip + term
            target[pl.ds(start, 8), :] = strip
            return 0

        lax.fori_loop(0, height // 8, body, 0, unroll=height // 8)

    tall = mid.shape[1]
    with jax.named_scope("mid"):
        for q in range(mid.shape[0]):
            combine(lambda w, start: mids[w, q, pl.ds(start, 8), :], mid.at[q], tall)
            leave(1, mid, mid_out, q)
    with jax.named_scope("coarse"):
        pool2 = pool_matrix(2)
        for q in range(coarse.shape[0]):
            coarse[q] = pooled(
                lambda tile, line: mid[2 * q + tile, pl.ds(line, tall // 2, stride=2), :], 2, pool2)
    with jax.named_scope("blend"):
        for t in range(tiles):
            combine(lambda w, start: vec[w, t, pl.ds(start + TOP, 8), :], blend.at[t], rows)
            leave(0, blend, blend_out, t)
    with jax.named_scope("fine"):
        for q in range(tiles // 2):
            combine(lambda w, start: fines[w, q, pl.ds(start, 8), :], fine.at[q], rows // 2)
            leave(2, fine, fine_out, q)
    with jax.named_scope("coarse_out"):
        for q in range(coarse.shape[0]):
            leave(3, coarse, coarse_out, q)
    with jax.named_scope("wait_out"):
        for which, ref in enumerate((blend, mid, fine, coarse)):
            pltpu.make_async_copy(ref, ref, out_sem.at[which]).wait()


def per_device(n_row, n_col, sources, labels):
    kinds, rows, cols = sources.shape
    n = n_row * n_col
    tiles = cols // LANES
    tall = rows + 2 * TOP
    n_pack = HALO * (kinds + 1)
    f32 = jnp.float32
    vmem = pl.BlockSpec(memory_space=pltpu.VMEM)
    hbm = pl.BlockSpec(memory_space=pltpu.HBM)
    up_lines, down_lines = ((kinds * d + d - 1) * tiles for d in (HALO, HALO - 1))
    mid_rows, coarse_rows = n_row * rows // 4, n_row * rows // 8
    chips = n_row // 2
    dma = pltpu.SemaphoreType.DMA
    vec, fines, mids, coords = pl.pallas_call(
        functools.partial(gather_kernel, n_row, n_col, rows, cols, kinds),
        out_shape=(
            jax.ShapeDtypeStruct((ITERS, tiles + 1, tall, LANES), f32),
            jax.ShapeDtypeStruct((ITERS, tiles // 2, rows // 2, LANES), f32),
            jax.ShapeDtypeStruct((ITERS, tiles // 4, mid_rows, LANES), f32),
            jax.ShapeDtypeStruct((ITERS, 8, LANES), f32),
        ),
        in_specs=[hbm] * 2,
        out_specs=(vmem,) * 4,
        scratch_shapes=[
            pltpu.VMEM((kinds, tiles + 1, tall, LANES), f32),
            pltpu.VMEM((tiles + 1, tall, LANES), jnp.int32),
            pltpu.VMEM((kinds, 2, 8, cols), f32),
            pltpu.VMEM((2, 8, cols), jnp.int32),
            pltpu.VMEM((up_lines, LANES), f32),
            pltpu.VMEM((down_lines, LANES), f32),
            pltpu.VMEM((2, n_pack, rows), f32),
            pltpu.VMEM((2, 2, n_pack, LANES), f32),
            pltpu.VMEM((up_lines, LANES), f32),
            pltpu.VMEM((down_lines, LANES), f32),
            pltpu.VMEM((2, n_pack, rows), f32),
            pltpu.VMEM((2, 2, n_pack, LANES), f32),
            pltpu.VMEM((2 * ITERS, 8, LANES), f32),
            pltpu.VMEM((n, 1, LANES), f32),
            pltpu.VMEM((4, ITERS * (tiles // 2), LANES), f32),
            pltpu.VMEM((n_row, ITERS * (tiles // 2) + 4, LANES), f32),
            pltpu.VMEM((ITERS, 2, mid_rows, LANES), f32),
            dma((6,)),
            dma((8,)),
            dma((8,)),
            pltpu.SemaphoreType.REGULAR((2,)),
            dma,
            dma,
            dma,
            dma((ITERS,)),
            dma((ITERS,)),
            dma,
            dma,
            dma,
            dma,
        ],
        compiler_params=pltpu.CompilerParams(
            collective_id=0, has_side_effects=True, vmem_limit_bytes=24 * 2**20),
    )(
        pltpu.with_memory_space_constraint(sources, pltpu.HBM),
        pltpu.with_memory_space_constraint(labels, pltpu.HBM),
    )
    return pl.pallas_call(
        functools.partial(finish_kernel, rows, cols),
        out_shape=(
            jax.ShapeDtypeStruct((rows, cols), f32),
            jax.ShapeDtypeStruct((rows // 2, cols // 2), f32),
            jax.ShapeDtypeStruct((mid_rows, cols // 4), f32),
            jax.ShapeDtypeStruct((coarse_rows, cols // 8), f32),
        ),
        in_specs=[vmem] * 4,
        out_specs=(hbm,) * 4,
        scratch_shapes=[
            pltpu.VMEM((tiles, rows, LANES), f32),
            pltpu.VMEM((tiles // 2, rows // 2, LANES), f32),
            pltpu.VMEM((tiles // 4, mid_rows, LANES), f32),
            pltpu.VMEM((tiles // 8, coarse_rows, LANES), f32),
            dma((4,)),
        ],
        compiler_params=pltpu.CompilerParams(vmem_limit_bytes=24 * 2**20),
    )(vec, fines, mids, coords)


def solution(mesh):
    sizes = dict(mesh.shape)
    return jax.shard_map(
        functools.partial(per_device, sizes["row"], sizes["col"]),
        mesh=mesh,
        in_specs=(P(None, "row", "col"), P("row", "col")),
        out_specs=(P("row", "col"), P("row", "col"), P(None, "col"), P(None, "col")),
        check_vma=False,
    )
```

```python
import functools

import jax
import jax.numpy as jnp
from jax import lax
from jax.experimental import pallas as pl
from jax.experimental.pallas import tpu as pltpu
from jax.sharding import PartitionSpec as P

ITERS = 3
MESH = pl.DeviceIdType.MESH
HALO = 4
TOP = 8
LANES = 128
SIDES = ((-1, -1), (-1, 1), (1, -1), (1, 1), (-1, 0), (1, 0), (0, -1), (0, 1))


def lane_of(shape):
    return lax.broadcasted_iota(jnp.int32, shape, len(shape) - 1)


def line_of(shape):
    return lax.broadcasted_iota(jnp.int32, shape, len(shape) - 2)


def lines(ref, index, start):
    return ref[index + (pl.ds(start, 8), slice(None))]


def beside_ring(mid):
    tiles = mid.shape[0]
    lane = lane_of(mid.shape)
    left = pltpu.roll(mid, 1, axis=2)
    right = pltpu.roll(mid, LANES - 1, axis=2)
    from_left = jnp.concatenate([left[tiles - 1:], left[:tiles - 1]], axis=0)
    from_right = jnp.concatenate([right[1:], right[:1]], axis=0)
    return jnp.where(lane == 0, from_left, left) + jnp.where(lane == LANES - 1, from_right, right)


def beside_tile(mid):
    return pltpu.roll(mid, 1, axis=1) + pltpu.roll(mid, LANES - 1, axis=1)


def neighbour_sum(ref, index, start, mid, beside):
    return (lines(ref, index, start - 1) + lines(ref, index, start + 1)) + beside(mid)


def right_side(src, lab, tile, start, beside):
    here = lines(lab, (tile,), start)
    total = None
    for k in reversed(range(src.shape[0])):
        mid = lines(src, (k, tile), start)
        term = 4.0 * mid - neighbour_sum(src, (k, tile), start, mid, beside)
        total = term if total is None else jnp.where(here == k, term, total)
    return total


def from_left(values):
    lane = lane_of(values.shape)
    moved = pltpu.roll(values, 1, axis=2)
    return jnp.where(lane == 0, jnp.concatenate([moved[-1:], moved[:-1]], axis=0), moved)


def from_right(values):
    lane = lane_of(values.shape)
    moved = pltpu.roll(values, LANES - 1, axis=2)
    return jnp.where(lane == LANES - 1, jnp.concatenate([moved[1:], moved[:1]], axis=0), moved)


def chosen(here, values):
    total = values[-1]
    for k in reversed(range(len(values) - 1)):
        total = jnp.where(here == k, values[k], total)
    return total


def beside_chosen(src, lab, tile, start):
    here = lines(lab, (tile,), start)
    mids = [lines(src, (k, tile), start) for k in range(src.shape[0])]
    return chosen(from_right(here), mids), chosen(from_left(here), mids)


def right_side_ring(src, lab, tile, start, left, right):
    here = lines(lab, (tile,), start)
    crosses = [
        4.0 * lines(src, (k, tile), start)
        - (lines(src, (k, tile), start - 1) + lines(src, (k, tile), start + 1))
        for k in range(src.shape[0])
    ]
    return chosen(here, crosses) - (from_left(left) + from_right(right))


def quadratic(left, right, moments, shift):
    total = None
    for i, a in enumerate(left):
        for j, b in enumerate(right):
            term = a * b * moments[i + j + shift]
            total = term if total is None else total + term
    return total


def padded_sum(a, b):
    if len(a) < len(b):
        a, b = b, a
    return [x + b[i] if i < len(b) else x for i, x in enumerate(a)]


def coefficients(moments):
    residual = [jnp.ones_like(moments[0])]
    direction = residual
    solution_coords = [jnp.zeros_like(moments[0])]
    norm_now = moments[0]
    for iteration in range(ITERS):
        applied_dot = 4.0 * (
            quadratic(direction, direction, moments, 0)
            - quadratic(direction, direction, moments, 1)
        )
        step = norm_now / applied_dot
        solution_coords = padded_sum(solution_coords, [step * d for d in direction])
        if iteration + 1 < ITERS:
            moved = [-4.0 * step * d for d in direction]
            residual = padded_sum(residual, moved)
            residual = padded_sum(residual, [jnp.zeros_like(step)] + [-m for m in moved])
            norm_next = quadratic(residual, residual, moments, 0)
            ratio = norm_next / norm_now
            direction = padded_sum(residual, [ratio * d for d in direction])
            norm_now = norm_next
    return solution_coords


def split_dot(values, pool):
    pieces = []
    for _ in range(3):
        pieces.append(values.astype(jnp.bfloat16))
        values = values - pieces[-1].astype(jnp.float32)
    parts = jnp.dot(jnp.concatenate(pieces, axis=0), pool, preferred_element_type=jnp.float32)
    size = values.shape[0]
    return (parts[0:size] + parts[size:2 * size]) + parts[2 * size:]


def pooled(load, stride, pool):
    parts = []
    for tile in range(stride):
        part = load(tile, 0)
        for line in range(1, stride):
            part = part + load(tile, line)
        parts.append(part)
    return split_dot(jnp.concatenate(parts, axis=1), pool)


def pool_matrix(stride):
    shape = (LANES * stride, LANES)
    source, target = (lax.broadcasted_iota(jnp.int32, shape, d) for d in range(2))
    return jnp.where(source // stride == target, 1.0 / (stride * stride), 0.0).astype(jnp.bfloat16)


def gather_kernel(
    n_row, n_col, rows, cols, kinds,
    src_hbm, lab_hbm, vec, fines, mids, coord_ref,
    src, lab, edge, edge_lab, pack_up, pack_down, pack_c, pack_d, got_up, got_down, got_c, got_d,
    part, moment, band, patch, sides, token, load_sem, send_sem, recv_sem, chain,
    tell_send, mom_recv, mid_send, near_recv, far_recv, fwd_recv, patch_recv,
):
    tiles = cols // LANES
    side_tile = tiles
    main = slice(0, tiles)
    body_rows = pl.ds(TOP, rows)
    n = n_row * n_col
    row, col = lax.axis_index("row"), lax.axis_index("col")
    me = row * n_col + col
    f32 = jnp.float32

    first_row, last_row = row == 0, row == n_row - 1
    first_col, last_col = col == 0, col == n_col - 1
    there = {
        (dr, dc): functools.reduce(jnp.logical_and, [
            jnp.logical_not(edge) for step, edge in (
                (dr < 0, first_row), (dr > 0, last_row), (dc < 0, first_col), (dc > 0, last_col))
            if step])
        for dr, dc in SIDES
    }

    def other_row(step):
        return jnp.where(step >= row, step + 1, step)

    def for_other_rows(act):
        def body(step, _):
            act(other_row(step))
            return 0

        lax.fori_loop(0, n_row - 1, body, 0)

    barrier = pltpu.get_barrier_semaphore()

    def greet(r, c):
        pl.semaphore_signal(barrier, inc=1, device_id=(r, c), device_id_type=MESH)

    greeters = n_row - 1
    for dr, dc in SIDES:
        if dc:
            pl.when(there[dr, dc])(functools.partial(
                greet, jnp.clip(row + dr, 0, n_row - 1), jnp.clip(col + dc, 0, n_col - 1)))
            greeters = greeters + jnp.where(there[dr, dc], 1, 0)
    def plane_load(k, t, wave):
        lanes = pl.ds(t * LANES, LANES)
        if k < kinds:
            return pltpu.make_async_copy(
                src_hbm.at[k, :, lanes], src.at[k, t, body_rows], load_sem.at[wave])
        return pltpu.make_async_copy(
            lab_hbm.at[:, lanes], lab.at[t, body_rows], load_sem.at[wave])

    def edge_load(k, side):
        here = pl.ds(0 if side == 0 else rows - 8, 8)
        if k < kinds:
            return pltpu.make_async_copy(src_hbm.at[k, here], edge.at[k, side], load_sem.at[0])
        return pltpu.make_async_copy(lab_hbm.at[here], edge_lab.at[side], load_sem.at[0])

    def wait_bytes(ref, sem):
        pltpu.make_async_copy(ref, ref, sem).wait()

    for k in range(kinds + 1):
        for side in range(2):
            edge_load(k, side).start()
    for k in range(kinds + 1):
        for t in (0, tiles - 1):
            plane_load(k, t, 0).start()
    for_other_rows(lambda r: greet(r, col))
    for t in range(1, tiles - 1):
        for k in range(kinds + 1):
            plane_load(k, t, 1).start()

    pad = jnp.zeros((tiles + 1, 8, LANES), f32)
    for start in (0, TOP + rows):
        for k in range(kinds):
            src[k, :, pl.ds(start, 8), :] = pad
        lab[:, pl.ds(start, 8), :] = pad.astype(jnp.int32)
        for w in range(ITERS):
            vec[w, :, pl.ds(start, 8), :] = pad

    def row_part(side, k, t):
        depth = HALO - side
        each = kinds * depth + depth - 1
        return (depth if k < kinds else depth - 1), t * each + k * depth

    n_pack = HALO * (kinds + 1)
    with jax.named_scope("wait_first"):
        wait_bytes(token.at[pl.ds(0, 2 * (kinds + 1) * (8 * tiles + rows))], load_sem.at[0])
    with jax.named_scope("pack"):
        for side in range(2):
            for k in range(kinds + 1):
                for t in range(tiles):
                    lanes = pl.ds(t * LANES, LANES)
                    depth, at = row_part(side, k, t)
                    lines_here = pl.ds(0 if side == 0 else 8 - depth, depth)
                    if k < kinds:
                        value = edge[k, side, lines_here, lanes]
                    else:
                        value = edge_lab[side, lines_here, lanes].astype(f32)
                    (pack_up if side == 0 else pack_down)[pl.ds(at, depth), :] = value
                for end, t in enumerate((0, tiles - 1)):
                    lanes = pl.ds(t * LANES, LANES)
                    lines_here = pl.ds(0 if side == 0 else 8 - HALO, HALO)
                    if k < kinds:
                        value = edge[k, side, lines_here, lanes]
                    else:
                        value = edge_lab[side, lines_here, lanes].astype(f32)
                    pack_d[side, end, pl.ds(HALO * k, HALO), :] = value
        wide_lane = lane_of((rows, LANES))
        for k in range(kinds + 1):
            if k < kinds:
                first, last = src[k, 0, body_rows], src[k, tiles - 1, body_rows]
            else:
                first, last = lab[0, body_rows].astype(f32), lab[tiles - 1, body_rows].astype(f32)
            both = jnp.where(wide_lane < LANES // 2, first, last)
            turned = jnp.transpose(both)
            at = pl.ds(HALO * k, HALO)
            pack_c[0, at, :] = turned[0:HALO]
            pack_c[1, at, :] = turned[LANES - HALO:LANES]

    with jax.named_scope("barrier"):
        pl.semaphore_wait(barrier, greeters)

    def place(dr, dc):
        return (0 if dr < 0 else 1) if dc == 0 else 2 if dr == 0 else 3

    for dr, dc in SIDES:
        mine_r, mine_c = (0 if dr < 0 else 1), (0 if dc < 0 else 1)
        if dc == 0:
            source, target = (pack_up, got_up) if dr < 0 else (pack_down, got_down)
        elif dr == 0:
            source, target = pack_c.at[mine_c], got_c.at[1 - mine_c]
        else:
            source = pack_d.at[mine_r, mine_c]
            target = got_d.at[1 - mine_r, 1 - mine_c]
        device = (
            jnp.clip(row + dr, 0, n_row - 1),
            jnp.clip(col + dc, 0, n_col - 1),
        )
        pl.when(there[dr, dc])(pltpu.make_async_remote_copy(
            src_ref=source, dst_ref=target, send_sem=send_sem.at[place(dr, dc)],
            recv_sem=recv_sem.at[place(-dr, -dc)], device_id=device, device_id_type=MESH,
        ).start)

    def wait_halos(sem, above, below):
        pl.when(there[-1, 0])(lambda: wait_bytes(above, sem.at[0]))
        pl.when(there[1, 0])(lambda: wait_bytes(below, sem.at[1]))
        beside_rows = jnp.where(there[-1, 0], 1, 0) + jnp.where(there[1, 0], 1, 0)
        beside_cols = jnp.where(there[0, -1], 1, 0) + jnp.where(there[0, 1], 1, 0)
        corners = beside_rows * beside_cols
        pl.when(beside_cols == 2)(lambda: wait_bytes(got_c, sem.at[2]))
        pl.when(beside_cols == 1)(lambda: wait_bytes(got_c.at[0], sem.at[2]))
        pl.when(corners == 4)(lambda: wait_bytes(got_d, sem.at[3]))
        pl.when(corners == 2)(lambda: wait_bytes(got_d.at[0], sem.at[3]))
        pl.when(corners == 1)(lambda: wait_bytes(got_d.at[0, 0], sem.at[3]))

    def pass_on(dc):
        pl.semaphore_signal(
            chain.at[0 if dc > 0 else 1], inc=1,
            device_id=(row, jnp.clip(col + dc, 0, n_col - 1)), device_id_type=MESH)

    def hear(dc):
        pl.semaphore_wait(chain.at[0 if dc > 0 else 1], 1)

    def relay(dc):
        hear(dc)
        pass_on(dc)

    inner_col = jnp.logical_and(there[0, 1], there[0, -1])
    upper_half = 2 * col >= n_col
    pl.when(jnp.logical_and(first_col, there[0, 1]))(lambda: pass_on(1))
    pl.when(jnp.logical_and(last_col, there[0, -1]))(lambda: pass_on(-1))

    with jax.named_scope("wait_later"):
        wait_bytes(token.at[pl.ds(0, (kinds + 1) * (tiles - 2) * rows)], load_sem.at[1])
    groups = rows // 8
    lane_r = lane_of((tiles, 8, LANES))
    lane_t = lane_of((8, LANES))
    line_t = line_of((8, LANES))

    def whole_loop(count, act):
        def body(i, _):
            act(i)
            return 0

        lax.fori_loop(0, count, body, 0, unroll=count)

    def save(which, tile, start, value):
        vec[which, tile, pl.ds(start, 8), :] = value

    def applied(which, tile, start, beside):
        mid = lines(vec, (which, tile), start)
        return neighbour_sum(vec, (which, tile), start, mid, beside)

    with jax.named_scope("main_b"):
        def choose(i):
            start = TOP + 8 * i
            left, right = beside_chosen(src, lab, main, start)
            save(1, main, start, left)
            save(2, main, start, right)

        whole_loop(groups, choose)
        whole_loop(groups, lambda i: save(0, main, TOP + 8 * i, right_side_ring(
            src, lab, main, TOP + 8 * i,
            lines(vec, (1, main), TOP + 8 * i), lines(vec, (2, main), TOP + 8 * i))))

    def inner(which):
        whole_loop(groups, lambda i: save(
            which, main, TOP + 8 * i, applied(which - 1, main, TOP + 8 * i, beside_ring)))


    chips = n_row // 2
    core = lax.rem(row, 2)
    chip = lax.div(row, 2)
    partner = row + 1 - 2 * core
    quad = rows // 4
    pool4, pool2 = pool_matrix(4), pool_matrix(2)

    def blocks(count):
        return mids.at[:, :, pl.ds(0, count * quad)]

    def hand(w, owner, target, send, recv):
        block = mids.at[w, :, pl.ds(pl.multiple_of(owner * quad, 8), quad)]
        pltpu.make_async_remote_copy(
            src_ref=block, dst_ref=block, send_sem=send, recv_sem=recv,
            device_id=(target, col), device_id_type=MESH).start()

    def same_core(q):
        return 2 * q + core

    def to_partner(w, owner):
        hand(w, owner, partner, mid_send, fwd_recv)

    others = [lax.rem(chip + step, chips) for step in range(1, chips)]
    if chips == 4:
        others = [chip + 1 - 2 * lax.rem(chip, 2), chip + 2 - 4 * lax.div(chip, 2), 3 - chip]
    others = [same_core(q) for q in others]
    near, far = others[:-1], others[-1]

    def send_early(w):
        own = pooled(
            lambda tile, line: jnp.concatenate([
                vec[w, 4 * q + tile, pl.ds(TOP + line, quad, stride=4), :]
                for q in range(tiles // 4)], axis=0),
            4, pool4)
        for q in range(tiles // 4):
            mids[w, q, pl.ds(pl.multiple_of(row * quad, 8), quad), :] = own[
                q * quad:(q + 1) * quad]
        for target in near:
            hand(w, row, target, mid_send, near_recv)
        hand(w, row, far, mid_send, far_recv)
        to_partner(w, row)

    with jax.named_scope("main_v"):
        for w in range(1, ITERS):
            inner(w)
            send_early(w - 1)
        send_early(ITERS - 1)

    def products(tile, start, right_of, keep):
        powers = [lines(vec, (w, tile), start) for w in range(ITERS)]
        powers.append(lines(vec, (ITERS - 1, tile), start + 1) + right_of(powers[-1]))
        kept = [keep(p) for p in powers[:ITERS]]
        return [kept[i // 2] * powers[(i + 1) // 2] for i in range(2 * ITERS)]

    def right_ring(mid):
        right = pltpu.roll(mid, LANES - 1, axis=2)
        return jnp.where(
            lane_r == LANES - 1, jnp.concatenate([right[1:], right[:1]], axis=0), right)

    def right_tile(mid):
        return pltpu.roll(mid, LANES - 1, axis=1)

    def keep_main(p):
        edge_lane = lane_of((1, 8, LANES))
        return jnp.concatenate([
            jnp.where(edge_lane < HALO, 0.0, p[0:1]), p[1:tiles - 1],
            jnp.where(edge_lane >= LANES - HALO, 0.0, p[tiles - 1:]),
        ], axis=0)

    def fold(value):
        if len(value.shape) == 2:
            return value
        total = value[0]
        for t in range(1, value.shape[0]):
            total = total + value[t]
        return total

    with jax.named_scope("main_m"):
        def main_body(i, sums):
            new = products(main, TOP + HALO + 8 * i, right_ring, keep_main)
            return tuple(s + fold(p) for s, p in zip(sums, new))

        zero8 = jnp.zeros((8, LANES), f32)
        sums = lax.fori_loop(
            0, groups - 1, main_body, tuple(zero8 for _ in range(2 * ITERS)), unroll=groups - 1)
        for i, s in enumerate(sums):
            part[i] = s
    with jax.named_scope("side_fill"):
        for k in range(kinds + 1):
            if k < kinds:
                first, last = src[k, 0, body_rows], src[k, tiles - 1, body_rows]
                src[k, side_tile, body_rows, :] = jnp.where(
                    wide_lane < LANES // 2, pltpu.roll(first, 2 * HALO, axis=1), last)
            else:
                first, last = lab[0, body_rows], lab[tiles - 1, body_rows]
                lab[side_tile, body_rows, :] = jnp.where(
                    wide_lane < LANES // 2, pltpu.roll(first, 2 * HALO, axis=1), last)

    with jax.named_scope("relay"):
        pl.when(inner_col)(lambda: relay(1))
        pl.when(jnp.logical_and(inner_col, upper_half))(lambda: relay(-1))

    with jax.named_scope("wait_halo"):
        wait_halos(recv_sem, got_down, got_up)

    with jax.named_scope("unpack"):
        for k in range(kinds + 1):
            at = pl.ds(HALO * k, HALO)
            right = jnp.where(last_col, 0.0, got_c[1, at, :])
            left = jnp.where(first_col, 0.0, got_c[0, at, :])
            turned = jnp.transpose(jnp.concatenate([right, left], axis=0))
            if k < kinds:
                src[k, side_tile, body_rows, 0:2 * HALO] = turned
            else:
                lab[side_tile, body_rows, 0:2 * HALO] = turned.astype(jnp.int32)
        corner_lane = lane_of((HALO, LANES))
        for side in range(2):
            missing = first_row if side == 0 else last_row
            got = got_down if side == 0 else got_up
            for k in range(kinds + 1):
                wide = []
                for t in range(tiles):
                    depth, at = row_part(1 - side, k, t)
                    wide.append(jnp.where(missing, 0.0, got[pl.ds(at, depth), :]))
                shift = HALO - depth if side == 0 else 0
                near_lines = slice(shift, shift + depth)
                at = pl.ds(HALO * k, HALO)
                right = jnp.where(missing | last_col, 0.0, got_d[side, 1, at, :])[near_lines]
                left = jnp.where(missing | first_col, 0.0, got_d[side, 0, at, :])[near_lines]
                corner_lane = lane_of((depth, LANES))
                moved = pltpu.roll(
                    jnp.where(corner_lane >= LANES - HALO, left, wide[0]), 2 * HALO, axis=1)
                own = jnp.where(corner_lane < LANES // 2, moved, wide[-1])
                wide.append(jnp.where(corner_lane < HALO, right, own))
                base = TOP - depth if side == 0 else TOP + rows
                for t, value in enumerate(wide):
                    if k < kinds:
                        src[k, t, pl.ds(base, depth), :] = value
                    else:
                        lab[t, pl.ds(base, depth), :] = value.astype(jnp.int32)

    off_lane = ((lane_t < HALO) & last_col) | ((lane_t >= HALO) & (lane_t < 2 * HALO) & first_col)
    off_top = (line_t < HALO) & first_row
    off_bottom = (line_t >= HALO) & last_row
    ends = ((TOP - HALO, off_top), (TOP + rows - HALO, off_bottom))

    def frame(which):
        def value(tile, start, beside):
            if which == 0:
                return right_side(src, lab, tile, start, beside)
            return applied(which - 1, tile, start, beside)

        def side_group(start, off):
            save(which, side_tile, start, jnp.where(off, 0.0, value(side_tile, start, beside_tile)))

        side_group(ends[0][0], off_top | off_lane)
        whole_loop(groups - 1, lambda i: side_group(TOP + HALO + 8 * i, off_lane))
        side_group(ends[1][0], off_bottom | off_lane)
        for start, off in ends:
            save(which, main, start, jnp.where(off[None], 0.0, value(main, start, beside_ring)))

    with jax.named_scope("frames"):
        for which in range(ITERS):
            frame(which)

    with jax.named_scope("moments"):
        sums = [part[i] for i in range(2 * ITERS)]
        on_side = ((lane_t >= 2 * HALO) & (lane_t < 3 * HALO)) | (lane_t >= LANES - HALO)

        def side_body(i, sums):
            new = products(
                side_tile, TOP + 8 * i, right_tile, lambda p: jnp.where(on_side, p, 0.0))
            return tuple(s + p for s, p in zip(sums, new))

        sums = lax.fori_loop(0, groups, side_body, tuple(sums), unroll=groups)
        for (start, _), on in zip(ends, (line_t >= HALO, line_t < HALO)):
            new = products(main, start, right_ring, lambda p: jnp.where(on[None], keep_main(p), 0.0))
            sums = [s + fold(p) for s, p in zip(sums, new)]
        lane1 = lane_of((1, LANES))
        mine = jnp.zeros((1, LANES), f32)
        for i, s in enumerate(sums):
            mine = jnp.where(lane1 == i, jnp.sum(s, keepdims=True), mine)
        moment[me] = mine

    with jax.named_scope("send_moments"):
        pl.when(jnp.logical_and(last_col, there[0, -1]))(lambda: hear(1))

        def tell(r, c):
            pltpu.make_async_remote_copy(
                src_ref=moment.at[me], dst_ref=moment.at[me], send_sem=tell_send, recv_sem=mom_recv,
                device_id=(r, c), device_id_type=MESH).start()

        def tell_block(c):
            def body(r, _):
                tell(r, c)
                return 0

            lax.fori_loop(0, n_row, body, 0)

        for c in range(n_col - 1):
            pl.when(c < col)(functools.partial(tell_block, c))
        for_other_rows(lambda r: tell(r, col))
        pl.when(jnp.logical_and(inner_col, jnp.logical_not(upper_half)))(lambda: relay(-1))

    def tell_rest():
        pl.when(first_col)(lambda: hear(-1))
        for c in range(1, n_col):
            pl.when(c > col)(functools.partial(tell_block, c))

    with jax.named_scope("tell_inner"):
        pl.when(inner_col)(tell_rest)

    ends_of = ((0, TOP), (quad - 1, TOP + rows - 4))
    lines_of = [(w, e, q) for w in range(ITERS) for e in range(2) for q in range(tiles // 4)]
    with jax.named_scope("patch"):
        for at, (w, e, q) in enumerate(lines_of):
            for i in range(4):
                four = vec[w, 4 * q + i, pl.ds(ends_of[e][1], 4), :]
                band[i, at:at + 1, :] = jnp.sum(four, axis=0, keepdims=True)
        wide = jnp.concatenate([band[i] for i in range(4)], axis=1)
        patch[row, 0:wide.shape[0], :] = split_dot(wide, pool4)
        odd = lax.rem(row, 2) == 1
        row_lane = lane_of((1, rows))
        for w in range(ITERS):
            flat = vec[w, side_tile, pl.ds(TOP, quad, stride=4), :]
            for line in range(1, 4):
                flat = flat + vec[w, side_tile, pl.ds(TOP + line, quad, stride=4), :]
            even_part, odd_part = jnp.where(odd, 0.0, flat), jnp.where(odd, flat, 0.0)
            turned = jnp.transpose(jnp.concatenate([even_part, odd_part] * 2, axis=0))
            left = jnp.sum(turned[2 * HALO:3 * HALO], axis=0, keepdims=True)
            right = jnp.sum(turned[LANES - HALO:], axis=0, keepdims=True)
            at = len(lines_of) + w
            patch[row, at:at + 1, :] = jnp.where(row_lane < 2 * quad, left, right) * (1.0 / 16)
        for_other_rows(lambda r: pltpu.make_async_remote_copy(
            src_ref=patch.at[row], dst_ref=patch.at[row], send_sem=tell_send,
            recv_sem=patch_recv, device_id=(r, col), device_id_type=MESH).start())

    with jax.named_scope("near"):
        wait_bytes(blocks(len(near)), near_recv)
        for w in range(ITERS):
            for owner in near:
                to_partner(w, owner)

    with jax.named_scope("merge"):
        for w in range(ITERS):
            side = vec[w, side_tile, body_rows]
            vec[w, 0, body_rows, :] = jnp.where(
                wide_lane < HALO, pltpu.roll(side, LANES - 2 * HALO, axis=1), vec[w, 0, body_rows])
            vec[w, tiles - 1, body_rows, :] = jnp.where(
                wide_lane >= LANES - HALO, side, vec[w, tiles - 1, body_rows])

    with jax.named_scope("fines"):
        half = rows // 2
        for w in range(ITERS):
            own = pooled(
                lambda tile, line: jnp.concatenate([
                    vec[w, 2 * q + tile, pl.ds(TOP + line, half, stride=2), :]
                    for q in range(tiles // 2)], axis=0),
                2, pool2)
            for q in range(tiles // 2):
                fines[w, q] = own[q * half:(q + 1) * half]

    with jax.named_scope("tell_first"):
        pl.when(jnp.logical_and(first_col, there[0, 1]))(tell_rest)

    with jax.named_scope("far"):
        wait_bytes(blocks(1), far_recv)
        for w in range(ITERS):
            to_partner(w, far)

    with jax.named_scope("wait_patch"):
        patches = patch.at[pl.ds(0, n_row - 1)]
        wait_bytes(patches, patch_recv)
    with jax.named_scope("prepare"):
        for pair in range(n_row // 2):
            for w in range(ITERS):
                at = len(lines_of) + w
                both = patch[2 * pair, at:at + 1, :] + patch[2 * pair + 1, at:at + 1, :]
                turned = jnp.transpose(jnp.broadcast_to(both, (8, LANES)))
                for end in range(2):
                    part_here = turned[2 * quad * end:2 * quad * (end + 1), 0:1]
                    sides[w, end, pl.ds(2 * pair * quad, 2 * quad), :] = jnp.broadcast_to(
                        part_here, (2 * quad, LANES))

    with jax.named_scope("wait_forwards"):
        wait_bytes(blocks(2 * chips - 1), mid_send)
        wait_bytes(blocks(chips), fwd_recv)
    with jax.named_scope("apply"):
        for owner in range(n_row):
            for at, (w, e, q) in enumerate(lines_of):
                mids[w, q, pl.ds(owner * quad + ends_of[e][0], 1), :] = patch[
                    owner, at:at + 1, :]
        all_lane = lane_of((n_row * quad, LANES))
        for w in range(ITERS):
            for end, q, lane in ((0, 0, 0), (1, tiles // 4 - 1, LANES - 1)):
                mids[w, q] = jnp.where(all_lane == lane, sides[w, end], mids[w, q])

    with jax.named_scope("wait_moments"):
        everyone = moment.at[pl.ds(0, n - 1)]
        wait_bytes(everyone, mom_recv)
    with jax.named_scope("coefs"):
        total = jnp.sum(moment[...], axis=0)
        moments = [
            (0.25 ** i * (1.0 if i < 2 * ITERS - 1 else 2.0))
            * jnp.sum(jnp.where(lane1 == i, total, 0.0), axis=1, keepdims=True)
            for i in range(2 * ITERS)
        ]
        for w, c in enumerate(coefficients(moments)):
            coord_ref[w] = jnp.broadcast_to(0.25 ** w * c, (8, LANES))

    with jax.named_scope("wait_sends"):
        wait_halos(send_sem, got_up, got_down)
        wait_bytes(token.at[pl.ds(0, n - 1 + (n_row - 1) * patch.shape[1])], tell_send)


def finish_kernel(
    rows, cols, vec, fines, mids, coord_ref, blend_out, fine_out, mid_out, coarse_out,
    blend, fine, mid, coarse, out_sem,
):
    tiles = cols // LANES

    def leave(which, source, target, q):
        pltpu.make_async_copy(
            source.at[q], target.at[:, pl.ds(q * LANES, LANES)], out_sem.at[which]).start()

    def combine(load, target, height):
        coords = [coord_ref[w] for w in range(ITERS)]

        def body(g, _):
            start = pl.multiple_of(g * 8, 8)
            strip = None
            for w in range(ITERS):
                term = coords[w] * load(w, start)
                strip = term if strip is None else strip + term
            target[pl.ds(start, 8), :] = strip
            return 0

        lax.fori_loop(0, height // 8, body, 0, unroll=height // 8)

    tall = mid.shape[1]
    with jax.named_scope("mid"):
        for q in range(mid.shape[0]):
            combine(lambda w, start: mids[w, q, pl.ds(start, 8), :], mid.at[q], tall)
            leave(1, mid, mid_out, q)
    with jax.named_scope("coarse"):
        pool2 = pool_matrix(2)
        for q in range(coarse.shape[0]):
            coarse[q] = pooled(
                lambda tile, line: mid[2 * q + tile, pl.ds(line, tall // 2, stride=2), :], 2, pool2)
    with jax.named_scope("blend"):
        for t in range(tiles):
            combine(lambda w, start: vec[w, t, pl.ds(start + TOP, 8), :], blend.at[t], rows)
            leave(0, blend, blend_out, t)
    with jax.named_scope("fine"):
        for q in range(tiles // 2):
            combine(lambda w, start: fines[w, q, pl.ds(start, 8), :], fine.at[q], rows // 2)
            leave(2, fine, fine_out, q)
    with jax.named_scope("coarse_out"):
        for q in range(coarse.shape[0]):
            leave(3, coarse, coarse_out, q)
    with jax.named_scope("wait_out"):
        for which, ref in enumerate((blend, mid, fine, coarse)):
            pltpu.make_async_copy(ref, ref, out_sem.at[which]).wait()


def per_device(n_row, n_col, sources, labels):
    kinds, rows, cols = sources.shape
    n = n_row * n_col
    tiles = cols // LANES
    tall = rows + 2 * TOP
    n_pack = HALO * (kinds + 1)
    f32 = jnp.float32
    vmem = pl.BlockSpec(memory_space=pltpu.VMEM)
    hbm = pl.BlockSpec(memory_space=pltpu.HBM)
    up_lines, down_lines = ((kinds * d + d - 1) * tiles for d in (HALO, HALO - 1))
    token_lines = (kinds + 1) * max(2 * (8 * tiles + rows), (tiles - 2) * rows)
    mid_rows, coarse_rows = n_row * rows // 4, n_row * rows // 8
    chips = n_row // 2
    dma = pltpu.SemaphoreType.DMA
    vec, fines, mids, coords = pl.pallas_call(
        functools.partial(gather_kernel, n_row, n_col, rows, cols, kinds),
        out_shape=(
            jax.ShapeDtypeStruct((ITERS, tiles + 1, tall, LANES), f32),
            jax.ShapeDtypeStruct((ITERS, tiles // 2, rows // 2, LANES), f32),
            jax.ShapeDtypeStruct((ITERS, tiles // 4, mid_rows, LANES), f32),
            jax.ShapeDtypeStruct((ITERS, 8, LANES), f32),
        ),
        in_specs=[hbm] * 2,
        out_specs=(vmem,) * 4,
        scratch_shapes=[
            pltpu.VMEM((kinds, tiles + 1, tall, LANES), f32),
            pltpu.VMEM((tiles + 1, tall, LANES), jnp.int32),
            pltpu.VMEM((kinds, 2, 8, cols), f32),
            pltpu.VMEM((2, 8, cols), jnp.int32),
            pltpu.VMEM((up_lines, LANES), f32),
            pltpu.VMEM((down_lines, LANES), f32),
            pltpu.VMEM((2, n_pack, rows), f32),
            pltpu.VMEM((2, 2, n_pack, LANES), f32),
            pltpu.VMEM((up_lines, LANES), f32),
            pltpu.VMEM((down_lines, LANES), f32),
            pltpu.VMEM((2, n_pack, rows), f32),
            pltpu.VMEM((2, 2, n_pack, LANES), f32),
            pltpu.VMEM((2 * ITERS, 8, LANES), f32),
            pltpu.VMEM((n, 1, LANES), f32),
            pltpu.VMEM((4, ITERS * (tiles // 2), LANES), f32),
            pltpu.VMEM((n_row, ITERS * (tiles // 2) + 4, LANES), f32),
            pltpu.VMEM((ITERS, 2, mid_rows, LANES), f32),
            pltpu.VMEM((token_lines, LANES), f32),
            dma((2,)),
            dma((4,)),
            dma((4,)),
            pltpu.SemaphoreType.REGULAR((2,)),
            dma,
            dma,
            dma,
            dma,
            dma,
            dma,
            dma,
        ],
        compiler_params=pltpu.CompilerParams(
            collective_id=0, has_side_effects=True, vmem_limit_bytes=24 * 2**20),
    )(
        pltpu.with_memory_space_constraint(sources, pltpu.HBM),
        pltpu.with_memory_space_constraint(labels, pltpu.HBM),
    )
    return pl.pallas_call(
        functools.partial(finish_kernel, rows, cols),
        out_shape=(
            jax.ShapeDtypeStruct((rows, cols), f32),
            jax.ShapeDtypeStruct((rows // 2, cols // 2), f32),
            jax.ShapeDtypeStruct((mid_rows, cols // 4), f32),
            jax.ShapeDtypeStruct((coarse_rows, cols // 8), f32),
        ),
        in_specs=[vmem] * 4,
        out_specs=(hbm,) * 4,
        scratch_shapes=[
            pltpu.VMEM((tiles, rows, LANES), f32),
            pltpu.VMEM((tiles // 2, rows // 2, LANES), f32),
            pltpu.VMEM((tiles // 4, mid_rows, LANES), f32),
            pltpu.VMEM((tiles // 8, coarse_rows, LANES), f32),
            dma((4,)),
        ],
        compiler_params=pltpu.CompilerParams(vmem_limit_bytes=24 * 2**20),
    )(vec, fines, mids, coords)


def solution(mesh):
    sizes = dict(mesh.shape)
    return jax.shard_map(
        functools.partial(per_device, sizes["row"], sizes["col"]),
        mesh=mesh,
        in_specs=(P(None, "row", "col"), P("row", "col")),
        out_specs=(P("row", "col"), P("row", "col"), P(None, "col"), P(None, "col")),
        check_vma=False,
    )
```

```python
import functools

import jax
import jax.numpy as jnp
from jax import lax
from jax.experimental import pallas as pl
from jax.experimental.pallas import tpu as pltpu
from jax.sharding import PartitionSpec as P

ITERS = 3
MESH = pl.DeviceIdType.MESH
HALO = 4
TOP = 8
LANES = 128
SIDES = ((-1, -1), (-1, 1), (1, -1), (1, 1), (-1, 0), (1, 0), (0, -1), (0, 1))


def lane_of(shape):
    return lax.broadcasted_iota(jnp.int32, shape, len(shape) - 1)


def line_of(shape):
    return lax.broadcasted_iota(jnp.int32, shape, len(shape) - 2)


def lines(ref, index, start):
    return ref[index + (pl.ds(start, 8), slice(None))]


def beside_ring(mid):
    tiles = mid.shape[0]
    lane = lane_of(mid.shape)
    left = pltpu.roll(mid, 1, axis=2)
    right = pltpu.roll(mid, LANES - 1, axis=2)
    from_left = jnp.concatenate([left[tiles - 1:], left[:tiles - 1]], axis=0)
    from_right = jnp.concatenate([right[1:], right[:1]], axis=0)
    return jnp.where(lane == 0, from_left, left) + jnp.where(lane == LANES - 1, from_right, right)


def beside_tile(mid):
    return pltpu.roll(mid, 1, axis=1) + pltpu.roll(mid, LANES - 1, axis=1)


def neighbour_sum(ref, index, start, mid, beside):
    return (lines(ref, index, start - 1) + lines(ref, index, start + 1)) + beside(mid)


def right_side(src, lab, tile, start, beside):
    here = lines(lab, (tile,), start)
    total = None
    for k in reversed(range(src.shape[0])):
        mid = lines(src, (k, tile), start)
        term = 4.0 * mid - neighbour_sum(src, (k, tile), start, mid, beside)
        total = term if total is None else jnp.where(here == k, term, total)
    return total


def from_left(values):
    lane = lane_of(values.shape)
    moved = pltpu.roll(values, 1, axis=2)
    return jnp.where(lane == 0, jnp.concatenate([moved[-1:], moved[:-1]], axis=0), moved)


def from_right(values):
    lane = lane_of(values.shape)
    moved = pltpu.roll(values, LANES - 1, axis=2)
    return jnp.where(lane == LANES - 1, jnp.concatenate([moved[1:], moved[:1]], axis=0), moved)


def chosen(here, values):
    total = values[-1]
    for k in reversed(range(len(values) - 1)):
        total = jnp.where(here == k, values[k], total)
    return total


def beside_chosen(src, lab, tile, start):
    here = lines(lab, (tile,), start)
    mids = [lines(src, (k, tile), start) for k in range(src.shape[0])]
    return chosen(from_right(here), mids), chosen(from_left(here), mids)


def right_side_ring(src, lab, tile, start, left, right):
    here = lines(lab, (tile,), start)
    crosses = [
        4.0 * lines(src, (k, tile), start)
        - (lines(src, (k, tile), start - 1) + lines(src, (k, tile), start + 1))
        for k in range(src.shape[0])
    ]
    return chosen(here, crosses) - (from_left(left) + from_right(right))


def quadratic(left, right, moments, shift):
    total = None
    for i, a in enumerate(left):
        for j, b in enumerate(right):
            term = a * b * moments[i + j + shift]
            total = term if total is None else total + term
    return total


def padded_sum(a, b):
    if len(a) < len(b):
        a, b = b, a
    return [x + b[i] if i < len(b) else x for i, x in enumerate(a)]


def coefficients(moments):
    residual = [jnp.ones_like(moments[0])]
    direction = residual
    solution_coords = [jnp.zeros_like(moments[0])]
    norm_now = moments[0]
    for iteration in range(ITERS):
        applied_dot = 4.0 * (
            quadratic(direction, direction, moments, 0)
            - quadratic(direction, direction, moments, 1)
        )
        step = norm_now / applied_dot
        solution_coords = padded_sum(solution_coords, [step * d for d in direction])
        if iteration + 1 < ITERS:
            moved = [-4.0 * step * d for d in direction]
            residual = padded_sum(residual, moved)
            residual = padded_sum(residual, [jnp.zeros_like(step)] + [-m for m in moved])
            norm_next = quadratic(residual, residual, moments, 0)
            ratio = norm_next / norm_now
            direction = padded_sum(residual, [ratio * d for d in direction])
            norm_now = norm_next
    return solution_coords


def split_dot(values, pool):
    pieces = []
    for _ in range(3):
        pieces.append(values.astype(jnp.bfloat16))
        values = values - pieces[-1].astype(jnp.float32)
    parts = jnp.dot(jnp.concatenate(pieces, axis=0), pool, preferred_element_type=jnp.float32)
    size = values.shape[0]
    return (parts[0:size] + parts[size:2 * size]) + parts[2 * size:]


def pooled(load, stride, pool):
    parts = []
    for tile in range(stride):
        part = load(tile, 0)
        for line in range(1, stride):
            part = part + load(tile, line)
        parts.append(part)
    return split_dot(jnp.concatenate(parts, axis=1), pool)


def pool_matrix(stride):
    shape = (LANES * stride, LANES)
    source, target = (lax.broadcasted_iota(jnp.int32, shape, d) for d in range(2))
    return jnp.where(source // stride == target, 1.0 / (stride * stride), 0.0).astype(jnp.bfloat16)


def gather_kernel(
    n_row, n_col, rows, cols, kinds,
    src_hbm, lab_hbm, vec, fines, mids, coord_ref,
    src, lab, edge, edge_lab, pack_up, pack_down, pack_c, pack_d, got_up, got_down, got_c, got_d,
    part, moment, band, patch, sides, token, load_sem, send_sem, recv_sem, chain,
    tell_send, mom_recv, mid_send, chip_recv, fwd_recv, patch_recv,
):
    tiles = cols // LANES
    side_tile = tiles
    main = slice(0, tiles)
    body_rows = pl.ds(TOP, rows)
    n = n_row * n_col
    row, col = lax.axis_index("row"), lax.axis_index("col")
    me = row * n_col + col
    f32 = jnp.float32

    first_row, last_row = row == 0, row == n_row - 1
    first_col, last_col = col == 0, col == n_col - 1
    there = {
        (dr, dc): functools.reduce(jnp.logical_and, [
            jnp.logical_not(edge) for step, edge in (
                (dr < 0, first_row), (dr > 0, last_row), (dc < 0, first_col), (dc > 0, last_col))
            if step])
        for dr, dc in SIDES
    }

    def other_row(step):
        return jnp.where(step >= row, step + 1, step)

    def for_other_rows(act):
        def body(step, _):
            act(other_row(step))
            return 0

        lax.fori_loop(0, n_row - 1, body, 0)

    barrier = pltpu.get_barrier_semaphore()

    def greet(r, c):
        pl.semaphore_signal(barrier, inc=1, device_id=(r, c), device_id_type=MESH)

    greeters = n_row - 1
    for dr, dc in SIDES:
        if dc:
            pl.when(there[dr, dc])(functools.partial(
                greet, jnp.clip(row + dr, 0, n_row - 1), jnp.clip(col + dc, 0, n_col - 1)))
            greeters = greeters + jnp.where(there[dr, dc], 1, 0)
    def plane_load(k, t, wave):
        lanes = pl.ds(t * LANES, LANES)
        if k < kinds:
            return pltpu.make_async_copy(
                src_hbm.at[k, :, lanes], src.at[k, t, body_rows], load_sem.at[wave])
        return pltpu.make_async_copy(
            lab_hbm.at[:, lanes], lab.at[t, body_rows], load_sem.at[wave])

    def edge_load(k, side):
        here = pl.ds(0 if side == 0 else rows - 8, 8)
        if k < kinds:
            return pltpu.make_async_copy(src_hbm.at[k, here], edge.at[k, side], load_sem.at[0])
        return pltpu.make_async_copy(lab_hbm.at[here], edge_lab.at[side], load_sem.at[0])

    def wait_bytes(ref, sem):
        pltpu.make_async_copy(ref, ref, sem).wait()

    for k in range(kinds + 1):
        for side in range(2):
            edge_load(k, side).start()
    for k in range(kinds + 1):
        for t in (0, tiles - 1):
            plane_load(k, t, 0).start()
    for_other_rows(lambda r: greet(r, col))
    for t in range(1, tiles - 1):
        for k in range(kinds + 1):
            plane_load(k, t, 1).start()

    pad = jnp.zeros((tiles + 1, 8, LANES), f32)
    for start in (0, TOP + rows):
        for k in range(kinds):
            src[k, :, pl.ds(start, 8), :] = pad
        lab[:, pl.ds(start, 8), :] = pad.astype(jnp.int32)
        for w in range(ITERS):
            vec[w, :, pl.ds(start, 8), :] = pad

    def row_part(side, k, t):
        depth = HALO - side
        each = kinds * depth + depth - 1
        return (depth if k < kinds else depth - 1), t * each + k * depth

    n_pack = HALO * (kinds + 1)
    with jax.named_scope("wait_first"):
        wait_bytes(token.at[pl.ds(0, 2 * (kinds + 1) * (8 * tiles + rows))], load_sem.at[0])
    with jax.named_scope("pack"):
        for side in range(2):
            for k in range(kinds + 1):
                for t in range(tiles):
                    lanes = pl.ds(t * LANES, LANES)
                    depth, at = row_part(side, k, t)
                    lines_here = pl.ds(0 if side == 0 else 8 - depth, depth)
                    if k < kinds:
                        value = edge[k, side, lines_here, lanes]
                    else:
                        value = edge_lab[side, lines_here, lanes].astype(f32)
                    (pack_up if side == 0 else pack_down)[pl.ds(at, depth), :] = value
                for end, t in enumerate((0, tiles - 1)):
                    lanes = pl.ds(t * LANES, LANES)
                    lines_here = pl.ds(0 if side == 0 else 8 - HALO, HALO)
                    if k < kinds:
                        value = edge[k, side, lines_here, lanes]
                    else:
                        value = edge_lab[side, lines_here, lanes].astype(f32)
                    pack_d[side, end, pl.ds(HALO * k, HALO), :] = value
        wide_lane = lane_of((rows, LANES))
        for k in range(kinds + 1):
            if k < kinds:
                first, last = src[k, 0, body_rows], src[k, tiles - 1, body_rows]
            else:
                first, last = lab[0, body_rows].astype(f32), lab[tiles - 1, body_rows].astype(f32)
            both = jnp.where(wide_lane < LANES // 2, first, last)
            turned = jnp.transpose(both)
            at = pl.ds(HALO * k, HALO)
            pack_c[0, at, :] = turned[0:HALO]
            pack_c[1, at, :] = turned[LANES - HALO:LANES]

    with jax.named_scope("barrier"):
        pl.semaphore_wait(barrier, greeters)

    def place(dr, dc):
        return (0 if dr < 0 else 1) if dc == 0 else 2 if dr == 0 else 3

    for dr, dc in SIDES:
        mine_r, mine_c = (0 if dr < 0 else 1), (0 if dc < 0 else 1)
        if dc == 0:
            source, target = (pack_up, got_up) if dr < 0 else (pack_down, got_down)
        elif dr == 0:
            source, target = pack_c.at[mine_c], got_c.at[1 - mine_c]
        else:
            source = pack_d.at[mine_r, mine_c]
            target = got_d.at[1 - mine_r, 1 - mine_c]
        device = (
            jnp.clip(row + dr, 0, n_row - 1),
            jnp.clip(col + dc, 0, n_col - 1),
        )
        pl.when(there[dr, dc])(pltpu.make_async_remote_copy(
            src_ref=source, dst_ref=target, send_sem=send_sem.at[place(dr, dc)],
            recv_sem=recv_sem.at[place(-dr, -dc)], device_id=device, device_id_type=MESH,
        ).start)

    beside_rows = jnp.where(there[-1, 0], 1, 0) + jnp.where(there[1, 0], 1, 0)
    beside_cols = jnp.where(there[0, -1], 1, 0) + jnp.where(there[0, 1], 1, 0)
    corners = beside_rows * beside_cols

    def wait_rows(sem, above, below):
        pl.when(there[-1, 0])(lambda: wait_bytes(above, sem.at[0]))
        pl.when(there[1, 0])(lambda: wait_bytes(below, sem.at[1]))
        pl.when(corners == 4)(lambda: wait_bytes(got_d, sem.at[3]))
        pl.when(corners == 2)(lambda: wait_bytes(got_d.at[0], sem.at[3]))
        pl.when(corners == 1)(lambda: wait_bytes(got_d.at[0, 0], sem.at[3]))

    def wait_columns(sem):
        pl.when(beside_cols == 2)(lambda: wait_bytes(got_c, sem.at[2]))
        pl.when(beside_cols == 1)(lambda: wait_bytes(got_c.at[0], sem.at[2]))

    def pass_on(dc):
        pl.semaphore_signal(
            chain.at[0 if dc > 0 else 1], inc=1,
            device_id=(row, jnp.clip(col + dc, 0, n_col - 1)), device_id_type=MESH)

    def hear(dc):
        pl.semaphore_wait(chain.at[0 if dc > 0 else 1], 1)

    def relay(dc):
        hear(dc)
        pass_on(dc)

    inner_col = jnp.logical_and(there[0, 1], there[0, -1])
    upper_half = 2 * col >= n_col
    pl.when(jnp.logical_and(first_col, there[0, 1]))(lambda: pass_on(1))
    pl.when(jnp.logical_and(last_col, there[0, -1]))(lambda: pass_on(-1))

    with jax.named_scope("wait_later"):
        wait_bytes(token.at[pl.ds(0, (kinds + 1) * (tiles - 2) * rows)], load_sem.at[1])
    groups = rows // 8
    lane_r = lane_of((tiles, 8, LANES))
    lane_t = lane_of((8, LANES))
    line_t = line_of((8, LANES))

    def whole_loop(count, act):
        def body(i, _):
            act(i)
            return 0

        lax.fori_loop(0, count, body, 0, unroll=count)

    def save(which, tile, start, value):
        vec[which, tile, pl.ds(start, 8), :] = value

    def applied(which, tile, start, beside):
        mid = lines(vec, (which, tile), start)
        return neighbour_sum(vec, (which, tile), start, mid, beside)

    with jax.named_scope("main_b"):
        def choose(i):
            start = TOP + 8 * i
            left, right = beside_chosen(src, lab, main, start)
            save(1, main, start, left)
            save(2, main, start, right)

        whole_loop(groups, choose)
        whole_loop(groups, lambda i: save(0, main, TOP + 8 * i, right_side_ring(
            src, lab, main, TOP + 8 * i,
            lines(vec, (1, main), TOP + 8 * i), lines(vec, (2, main), TOP + 8 * i))))

    def inner(which):
        whole_loop(groups, lambda i: save(
            which, main, TOP + 8 * i, applied(which - 1, main, TOP + 8 * i, beside_ring)))


    chips = n_row // 2
    core = lax.rem(row, 2)
    chip = lax.div(row, 2)
    partner = row + 1 - 2 * core
    quad = rows // 4
    pool4, pool2 = pool_matrix(4), pool_matrix(2)

    def blocks(count, w=slice(None)):
        return mids.at[w, :, pl.ds(0, count * quad)]

    def hand(w, owner, target, send, recv):
        block = mids.at[w, :, pl.ds(pl.multiple_of(owner * quad, 8), quad)]
        pltpu.make_async_remote_copy(
            src_ref=block, dst_ref=block, send_sem=send, recv_sem=recv,
            device_id=(target, col), device_id_type=MESH).start()

    def same_core(q):
        return 2 * q + core

    def to_partner(w, owner):
        hand(w, owner, partner, mid_send, fwd_recv)

    others = [lax.rem(chip + step, chips) for step in range(1, chips)]
    if chips == 4:
        others = [3 - chip, chip + 1 - 2 * lax.rem(chip, 2), chip + 2 - 4 * lax.div(chip, 2)]
    others = [same_core(q) for q in others]

    def send_early(w):
        own = pooled(
            lambda tile, line: jnp.concatenate([
                vec[w, 4 * q + tile, pl.ds(TOP + line, quad, stride=4), :]
                for q in range(tiles // 4)], axis=0),
            4, pool4)
        for q in range(tiles // 4):
            mids[w, q, pl.ds(pl.multiple_of(row * quad, 8), quad), :] = own[
                q * quad:(q + 1) * quad]
        for target in others:
            hand(w, row, target, mid_send, chip_recv.at[w])
        to_partner(w, row)

    with jax.named_scope("main_v"):
        for w in range(1, ITERS):
            inner(w)
            send_early(w - 1)
        send_early(ITERS - 1)

    def products(tile, start, right_of, keep):
        powers = [lines(vec, (w, tile), start) for w in range(ITERS)]
        powers.append(lines(vec, (ITERS - 1, tile), start + 1) + right_of(powers[-1]))
        kept = [keep(p) for p in powers[:ITERS]]
        return [kept[i // 2] * powers[(i + 1) // 2] for i in range(2 * ITERS)]

    def right_ring(mid):
        right = pltpu.roll(mid, LANES - 1, axis=2)
        return jnp.where(
            lane_r == LANES - 1, jnp.concatenate([right[1:], right[:1]], axis=0), right)

    def right_tile(mid):
        return pltpu.roll(mid, LANES - 1, axis=1)

    def keep_main(p):
        edge_lane = lane_of((1, 8, LANES))
        return jnp.concatenate([
            jnp.where(edge_lane < HALO, 0.0, p[0:1]), p[1:tiles - 1],
            jnp.where(edge_lane >= LANES - HALO, 0.0, p[tiles - 1:]),
        ], axis=0)

    def fold(value):
        if len(value.shape) == 2:
            return value
        total = value[0]
        for t in range(1, value.shape[0]):
            total = total + value[t]
        return total

    with jax.named_scope("main_m"):
        def main_body(i, sums):
            new = products(main, TOP + HALO + 8 * i, right_ring, keep_main)
            return tuple(s + fold(p) for s, p in zip(sums, new))

        zero8 = jnp.zeros((8, LANES), f32)
        sums = lax.fori_loop(
            0, groups - 1, main_body, tuple(zero8 for _ in range(2 * ITERS)), unroll=groups - 1)
        for i, s in enumerate(sums):
            part[i] = s
    with jax.named_scope("side_fill"):
        for k in range(kinds + 1):
            if k < kinds:
                first, last = src[k, 0, body_rows], src[k, tiles - 1, body_rows]
                src[k, side_tile, body_rows, :] = jnp.where(
                    wide_lane < LANES // 2, pltpu.roll(first, 2 * HALO, axis=1), last)
            else:
                first, last = lab[0, body_rows], lab[tiles - 1, body_rows]
                lab[side_tile, body_rows, :] = jnp.where(
                    wide_lane < LANES // 2, pltpu.roll(first, 2 * HALO, axis=1), last)

    with jax.named_scope("relay"):
        pl.when(inner_col)(lambda: relay(1))
        pl.when(jnp.logical_and(inner_col, upper_half))(lambda: relay(-1))

    with jax.named_scope("wait_cols"):
        wait_columns(recv_sem)

    with jax.named_scope("unpack_cols"):
        for k in range(kinds + 1):
            at = pl.ds(HALO * k, HALO)
            right = jnp.where(last_col, 0.0, got_c[1, at, :])
            left = jnp.where(first_col, 0.0, got_c[0, at, :])
            turned = jnp.transpose(jnp.concatenate([right, left], axis=0))
            if k < kinds:
                src[k, side_tile, body_rows, 0:2 * HALO] = turned
            else:
                lab[side_tile, body_rows, 0:2 * HALO] = turned.astype(jnp.int32)
        corner_lane = lane_of((HALO, LANES))

    off_lane = ((lane_t < HALO) & last_col) | ((lane_t >= HALO) & (lane_t < 2 * HALO) & first_col)
    off_top = (line_t < HALO) & first_row
    off_bottom = (line_t >= HALO) & last_row
    ends = ((TOP - HALO, off_top), (TOP + rows - HALO, off_bottom))

    def stage(which, tile, start, beside):
        if which == 0:
            return right_side(src, lab, tile, start, beside)
        return applied(which - 1, tile, start, beside)

    def side_groups(which, begin, end):
        for i in range(begin, end):
            start = TOP - HALO + 8 * i
            off = off_lane
            if i == 0:
                off = off | off_top
            if i == groups:
                off = off | off_bottom
            save(which, side_tile, start, jnp.where(
                off, 0.0, stage(which, side_tile, start, beside_tile)))

    def side_inner(which):
        begin = TOP + HALO + 8 * which
        count = groups - 1 - 2 * which
        whole_loop(count, lambda i: save(
            which, side_tile, begin + 8 * i, jnp.where(
                off_lane, 0.0, stage(which, side_tile, begin + 8 * i, beside_tile))))

    on_side = ((lane_t >= 2 * HALO) & (lane_t < 3 * HALO)) | (lane_t >= LANES - HALO)

    def side_sums(begin, end, sums):
        def body(i, sums):
            new = products(
                side_tile, TOP + 8 * (begin + i), right_tile, lambda p: jnp.where(on_side, p, 0.0))
            return tuple(s + p for s, p in zip(sums, new))

        return list(lax.fori_loop(0, end - begin, body, tuple(sums), unroll=end - begin))

    with jax.named_scope("side_inner"):
        for which in range(ITERS):
            side_inner(which)
        for i, s in enumerate(side_sums(ITERS, groups - ITERS, [part[i] for i in range(2 * ITERS)])):
            part[i] = s

    with jax.named_scope("wait_halo"):
        wait_rows(recv_sem, got_down, got_up)

    with jax.named_scope("unpack"):
        for side in range(2):
            missing = first_row if side == 0 else last_row
            got = got_down if side == 0 else got_up
            for k in range(kinds + 1):
                wide = []
                for t in range(tiles):
                    depth, at = row_part(1 - side, k, t)
                    wide.append(jnp.where(missing, 0.0, got[pl.ds(at, depth), :]))
                shift = HALO - depth if side == 0 else 0
                near_lines = slice(shift, shift + depth)
                at = pl.ds(HALO * k, HALO)
                right = jnp.where(missing | last_col, 0.0, got_d[side, 1, at, :])[near_lines]
                left = jnp.where(missing | first_col, 0.0, got_d[side, 0, at, :])[near_lines]
                corner_lane = lane_of((depth, LANES))
                moved = pltpu.roll(
                    jnp.where(corner_lane >= LANES - HALO, left, wide[0]), 2 * HALO, axis=1)
                own = jnp.where(corner_lane < LANES // 2, moved, wide[-1])
                wide.append(jnp.where(corner_lane < HALO, right, own))
                base = TOP - depth if side == 0 else TOP + rows
                for t, value in enumerate(wide):
                    if k < kinds:
                        src[k, t, pl.ds(base, depth), :] = value
                    else:
                        lab[t, pl.ds(base, depth), :] = value.astype(jnp.int32)

    with jax.named_scope("frames"):
        for which in range(ITERS):
            side_groups(which, 0, 1 + which)
            side_groups(which, groups - which, groups + 1)
            for start, off in ends:
                save(which, main, start, jnp.where(
                    off[None], 0.0, stage(which, main, start, beside_ring)))

    with jax.named_scope("moments"):
        sums = side_sums(0, ITERS, [part[i] for i in range(2 * ITERS)])
        sums = side_sums(groups - ITERS, groups, sums)
        for (start, _), on in zip(ends, (line_t >= HALO, line_t < HALO)):
            new = products(main, start, right_ring, lambda p: jnp.where(on[None], keep_main(p), 0.0))
            sums = [s + fold(p) for s, p in zip(sums, new)]
        lane1 = lane_of((1, LANES))
        mine = jnp.zeros((1, LANES), f32)
        for i, s in enumerate(sums):
            mine = jnp.where(lane1 == i, jnp.sum(s, keepdims=True), mine)
        moment[me] = mine

    with jax.named_scope("send_moments"):
        pl.when(jnp.logical_and(last_col, there[0, -1]))(lambda: hear(1))

        def tell(r, c):
            pltpu.make_async_remote_copy(
                src_ref=moment.at[me], dst_ref=moment.at[me], send_sem=tell_send, recv_sem=mom_recv,
                device_id=(r, c), device_id_type=MESH).start()

        def tell_block(c):
            def body(r, _):
                tell(r, c)
                return 0

            lax.fori_loop(0, n_row, body, 0)

        for c in range(n_col - 1):
            pl.when(c < col)(functools.partial(tell_block, c))
        for_other_rows(lambda r: tell(r, col))
        pl.when(jnp.logical_and(inner_col, jnp.logical_not(upper_half)))(lambda: relay(-1))

    def tell_rest():
        pl.when(first_col)(lambda: hear(-1))
        for c in range(1, n_col):
            pl.when(c > col)(functools.partial(tell_block, c))

    with jax.named_scope("tell_inner"):
        pl.when(inner_col)(tell_rest)

    ends_of = ((0, TOP), (quad - 1, TOP + rows - 4))
    lines_of = [(w, e, q) for w in range(ITERS) for e in range(2) for q in range(tiles // 4)]
    with jax.named_scope("patch"):
        for at, (w, e, q) in enumerate(lines_of):
            for i in range(4):
                four = vec[w, 4 * q + i, pl.ds(ends_of[e][1], 4), :]
                band[i, at:at + 1, :] = jnp.sum(four, axis=0, keepdims=True)
        wide = jnp.concatenate([band[i] for i in range(4)], axis=1)
        patch[row, 0:wide.shape[0], :] = split_dot(wide, pool4)
        odd = lax.rem(row, 2) == 1
        row_lane = lane_of((1, rows))
        for w in range(ITERS):
            flat = vec[w, side_tile, pl.ds(TOP, quad, stride=4), :]
            for line in range(1, 4):
                flat = flat + vec[w, side_tile, pl.ds(TOP + line, quad, stride=4), :]
            even_part, odd_part = jnp.where(odd, 0.0, flat), jnp.where(odd, flat, 0.0)
            turned = jnp.transpose(jnp.concatenate([even_part, odd_part] * 2, axis=0))
            left = jnp.sum(turned[2 * HALO:3 * HALO], axis=0, keepdims=True)
            right = jnp.sum(turned[LANES - HALO:], axis=0, keepdims=True)
            at = len(lines_of) + w
            patch[row, at:at + 1, :] = jnp.where(row_lane < 2 * quad, left, right) * (1.0 / 16)
        for_other_rows(lambda r: pltpu.make_async_remote_copy(
            src_ref=patch.at[row], dst_ref=patch.at[row], send_sem=tell_send,
            recv_sem=patch_recv, device_id=(r, col), device_id_type=MESH).start())

    with jax.named_scope("merge"):
        for w in range(ITERS):
            side = vec[w, side_tile, body_rows]
            vec[w, 0, body_rows, :] = jnp.where(
                wide_lane < HALO, pltpu.roll(side, LANES - 2 * HALO, axis=1), vec[w, 0, body_rows])
            vec[w, tiles - 1, body_rows, :] = jnp.where(
                wide_lane >= LANES - HALO, side, vec[w, tiles - 1, body_rows])

    with jax.named_scope("fines"):
        half = rows // 2
        for w in range(ITERS):
            own = pooled(
                lambda tile, line: jnp.concatenate([
                    vec[w, 2 * q + tile, pl.ds(TOP + line, half, stride=2), :]
                    for q in range(tiles // 2)], axis=0),
                2, pool2)
            for q in range(tiles // 2):
                fines[w, q] = own[q * half:(q + 1) * half]

    with jax.named_scope("tell_first"):
        pl.when(jnp.logical_and(first_col, there[0, 1]))(tell_rest)

    with jax.named_scope("near"):
        for w in range(ITERS):
            wait_bytes(blocks(chips - 1, w), chip_recv.at[w])
            for owner in others:
                to_partner(w, owner)

    with jax.named_scope("wait_patch"):
        patches = patch.at[pl.ds(0, n_row - 1)]
        wait_bytes(patches, patch_recv)
    with jax.named_scope("prepare"):
        for pair in range(n_row // 2):
            for w in range(ITERS):
                at = len(lines_of) + w
                both = patch[2 * pair, at:at + 1, :] + patch[2 * pair + 1, at:at + 1, :]
                turned = jnp.transpose(jnp.broadcast_to(both, (8, LANES)))
                for end in range(2):
                    part_here = turned[2 * quad * end:2 * quad * (end + 1), 0:1]
                    sides[w, end, pl.ds(2 * pair * quad, 2 * quad), :] = jnp.broadcast_to(
                        part_here, (2 * quad, LANES))

    with jax.named_scope("wait_forwards"):
        wait_bytes(blocks(2 * chips - 1), mid_send)
        wait_bytes(blocks(chips), fwd_recv)
    with jax.named_scope("apply"):
        for owner in range(n_row):
            for at, (w, e, q) in enumerate(lines_of):
                mids[w, q, pl.ds(owner * quad + ends_of[e][0], 1), :] = patch[
                    owner, at:at + 1, :]
        all_lane = lane_of((n_row * quad, LANES))
        for w in range(ITERS):
            for end, q, lane in ((0, 0, 0), (1, tiles // 4 - 1, LANES - 1)):
                mids[w, q] = jnp.where(all_lane == lane, sides[w, end], mids[w, q])

    with jax.named_scope("wait_moments"):
        everyone = moment.at[pl.ds(0, n - 1)]
        wait_bytes(everyone, mom_recv)
    with jax.named_scope("coefs"):
        total = jnp.sum(moment[...], axis=0)
        moments = [
            (0.25 ** i * (1.0 if i < 2 * ITERS - 1 else 2.0))
            * jnp.sum(jnp.where(lane1 == i, total, 0.0), axis=1, keepdims=True)
            for i in range(2 * ITERS)
        ]
        for w, c in enumerate(coefficients(moments)):
            coord_ref[w] = jnp.broadcast_to(0.25 ** w * c, (8, LANES))

    with jax.named_scope("wait_sends"):
        wait_rows(send_sem, got_up, got_down)
        wait_columns(send_sem)
        wait_bytes(token.at[pl.ds(0, n - 1 + (n_row - 1) * patch.shape[1])], tell_send)


def finish_kernel(
    rows, cols, vec, fines, mids, coord_ref, blend_out, fine_out, mid_out, coarse_out,
    blend, fine, mid, coarse, out_sem,
):
    tiles = cols // LANES

    def leave(which, source, target, q):
        pltpu.make_async_copy(
            source.at[q], target.at[:, pl.ds(q * LANES, LANES)], out_sem.at[which]).start()

    def combine(load, target, height):
        coords = [coord_ref[w] for w in range(ITERS)]

        def body(g, _):
            start = pl.multiple_of(g * 8, 8)
            strip = None
            for w in range(ITERS):
                term = coords[w] * load(w, start)
                strip = term if strip is None else strip + term
            target[pl.ds(start, 8), :] = strip
            return 0

        lax.fori_loop(0, height // 8, body, 0, unroll=height // 8)

    tall = mid.shape[1]
    with jax.named_scope("mid"):
        for q in range(mid.shape[0]):
            combine(lambda w, start: mids[w, q, pl.ds(start, 8), :], mid.at[q], tall)
            leave(1, mid, mid_out, q)
    with jax.named_scope("coarse"):
        pool2 = pool_matrix(2)
        for q in range(coarse.shape[0]):
            coarse[q] = pooled(
                lambda tile, line: mid[2 * q + tile, pl.ds(line, tall // 2, stride=2), :], 2, pool2)
    with jax.named_scope("blend"):
        for t in range(tiles):
            combine(lambda w, start: vec[w, t, pl.ds(start + TOP, 8), :], blend.at[t], rows)
            leave(0, blend, blend_out, t)
    with jax.named_scope("fine"):
        for q in range(tiles // 2):
            combine(lambda w, start: fines[w, q, pl.ds(start, 8), :], fine.at[q], rows // 2)
            leave(2, fine, fine_out, q)
    with jax.named_scope("coarse_out"):
        for q in range(coarse.shape[0]):
            leave(3, coarse, coarse_out, q)
    with jax.named_scope("wait_out"):
        for which, ref in enumerate((blend, mid, fine, coarse)):
            pltpu.make_async_copy(ref, ref, out_sem.at[which]).wait()


def per_device(n_row, n_col, sources, labels):
    kinds, rows, cols = sources.shape
    n = n_row * n_col
    tiles = cols // LANES
    tall = rows + 2 * TOP
    n_pack = HALO * (kinds + 1)
    f32 = jnp.float32
    vmem = pl.BlockSpec(memory_space=pltpu.VMEM)
    hbm = pl.BlockSpec(memory_space=pltpu.HBM)
    up_lines, down_lines = ((kinds * d + d - 1) * tiles for d in (HALO, HALO - 1))
    token_lines = (kinds + 1) * max(2 * (8 * tiles + rows), (tiles - 2) * rows)
    mid_rows, coarse_rows = n_row * rows // 4, n_row * rows // 8
    chips = n_row // 2
    dma = pltpu.SemaphoreType.DMA
    vec, fines, mids, coords = pl.pallas_call(
        functools.partial(gather_kernel, n_row, n_col, rows, cols, kinds),
        out_shape=(
            jax.ShapeDtypeStruct((ITERS, tiles + 1, tall, LANES), f32),
            jax.ShapeDtypeStruct((ITERS, tiles // 2, rows // 2, LANES), f32),
            jax.ShapeDtypeStruct((ITERS, tiles // 4, mid_rows, LANES), f32),
            jax.ShapeDtypeStruct((ITERS, 8, LANES), f32),
        ),
        in_specs=[hbm] * 2,
        out_specs=(vmem,) * 4,
        scratch_shapes=[
            pltpu.VMEM((kinds, tiles + 1, tall, LANES), f32),
            pltpu.VMEM((tiles + 1, tall, LANES), jnp.int32),
            pltpu.VMEM((kinds, 2, 8, cols), f32),
            pltpu.VMEM((2, 8, cols), jnp.int32),
            pltpu.VMEM((up_lines, LANES), f32),
            pltpu.VMEM((down_lines, LANES), f32),
            pltpu.VMEM((2, n_pack, rows), f32),
            pltpu.VMEM((2, 2, n_pack, LANES), f32),
            pltpu.VMEM((up_lines, LANES), f32),
            pltpu.VMEM((down_lines, LANES), f32),
            pltpu.VMEM((2, n_pack, rows), f32),
            pltpu.VMEM((2, 2, n_pack, LANES), f32),
            pltpu.VMEM((2 * ITERS, 8, LANES), f32),
            pltpu.VMEM((n, 1, LANES), f32),
            pltpu.VMEM((4, ITERS * (tiles // 2), LANES), f32),
            pltpu.VMEM((n_row, ITERS * (tiles // 2) + 4, LANES), f32),
            pltpu.VMEM((ITERS, 2, mid_rows, LANES), f32),
            pltpu.VMEM((token_lines, LANES), f32),
            dma((2,)),
            dma((4,)),
            dma((4,)),
            pltpu.SemaphoreType.REGULAR((2,)),
            dma,
            dma,
            dma,
            dma((ITERS,)),
            dma,
            dma,
        ],
        compiler_params=pltpu.CompilerParams(
            collective_id=0, has_side_effects=True, vmem_limit_bytes=24 * 2**20),
    )(
        pltpu.with_memory_space_constraint(sources, pltpu.HBM),
        pltpu.with_memory_space_constraint(labels, pltpu.HBM),
    )
    return pl.pallas_call(
        functools.partial(finish_kernel, rows, cols),
        out_shape=(
            jax.ShapeDtypeStruct((rows, cols), f32),
            jax.ShapeDtypeStruct((rows // 2, cols // 2), f32),
            jax.ShapeDtypeStruct((mid_rows, cols // 4), f32),
            jax.ShapeDtypeStruct((coarse_rows, cols // 8), f32),
        ),
        in_specs=[vmem] * 4,
        out_specs=(hbm,) * 4,
        scratch_shapes=[
            pltpu.VMEM((tiles, rows, LANES), f32),
            pltpu.VMEM((tiles // 2, rows // 2, LANES), f32),
            pltpu.VMEM((tiles // 4, mid_rows, LANES), f32),
            pltpu.VMEM((tiles // 8, coarse_rows, LANES), f32),
            dma((4,)),
        ],
        compiler_params=pltpu.CompilerParams(vmem_limit_bytes=24 * 2**20),
    )(vec, fines, mids, coords)


def solution(mesh):
    sizes = dict(mesh.shape)
    return jax.shard_map(
        functools.partial(per_device, sizes["row"], sizes["col"]),
        mesh=mesh,
        in_specs=(P(None, "row", "col"), P("row", "col")),
        out_specs=(P("row", "col"), P("row", "col"), P(None, "col"), P(None, "col")),
        check_vma=False,
    )
```

```python
import functools

import jax
import jax.numpy as jnp
from jax import lax
from jax.experimental import pallas as pl
from jax.experimental.pallas import tpu as pltpu
from jax.sharding import PartitionSpec as P

ITERS = 3
MESH = pl.DeviceIdType.MESH
HALO = 4
TOP = 8
LANES = 128
SIDES = ((1, 1), (1, -1), (-1, 1), (-1, -1), (1, 0), (-1, 0), (0, 1), (0, -1))


def lane_of(shape):
    return lax.broadcasted_iota(jnp.int32, shape, len(shape) - 1)


def line_of(shape):
    return lax.broadcasted_iota(jnp.int32, shape, len(shape) - 2)


def lines(ref, index, start):
    return ref[index + (pl.ds(start, 8), slice(None))]


def beside_ring(mid):
    tiles = mid.shape[0]
    lane = lane_of(mid.shape)
    left = pltpu.roll(mid, 1, axis=2)
    right = pltpu.roll(mid, LANES - 1, axis=2)
    from_left = jnp.concatenate([left[tiles - 1:], left[:tiles - 1]], axis=0)
    from_right = jnp.concatenate([right[1:], right[:1]], axis=0)
    return jnp.where(lane == 0, from_left, left) + jnp.where(lane == LANES - 1, from_right, right)


def beside_tile(mid):
    return pltpu.roll(mid, 1, axis=1) + pltpu.roll(mid, LANES - 1, axis=1)


def neighbour_sum(ref, index, start, mid, beside):
    return (lines(ref, index, start - 1) + lines(ref, index, start + 1)) + beside(mid)


def right_side(src, lab, tile, start, beside):
    here = lines(lab, (tile,), start)
    total = None
    for k in reversed(range(src.shape[0])):
        mid = lines(src, (k, tile), start)
        term = 4.0 * mid - neighbour_sum(src, (k, tile), start, mid, beside)
        total = term if total is None else jnp.where(here == k, term, total)
    return total


def from_left(values):
    lane = lane_of(values.shape)
    moved = pltpu.roll(values, 1, axis=2)
    return jnp.where(lane == 0, jnp.concatenate([moved[-1:], moved[:-1]], axis=0), moved)


def from_right(values):
    lane = lane_of(values.shape)
    moved = pltpu.roll(values, LANES - 1, axis=2)
    return jnp.where(lane == LANES - 1, jnp.concatenate([moved[1:], moved[:1]], axis=0), moved)


def chosen(here, values):
    total = values[-1]
    for k in reversed(range(len(values) - 1)):
        total = jnp.where(here == k, values[k], total)
    return total


def beside_chosen(src, lab, tile, start):
    here = lines(lab, (tile,), start)
    mids = [lines(src, (k, tile), start) for k in range(src.shape[0])]
    return chosen(from_right(here), mids), chosen(from_left(here), mids)


def right_side_ring(src, lab, tile, start, left, right):
    here = lines(lab, (tile,), start)
    crosses = [
        4.0 * lines(src, (k, tile), start)
        - (lines(src, (k, tile), start - 1) + lines(src, (k, tile), start + 1))
        for k in range(src.shape[0])
    ]
    return chosen(here, crosses) - (from_left(left) + from_right(right))


def quadratic(left, right, moments, shift):
    total = None
    for i, a in enumerate(left):
        for j, b in enumerate(right):
            term = a * b * moments[i + j + shift]
            total = term if total is None else total + term
    return total


def padded_sum(a, b):
    if len(a) < len(b):
        a, b = b, a
    return [x + b[i] if i < len(b) else x for i, x in enumerate(a)]


def coefficients(moments):
    residual = [jnp.ones_like(moments[0])]
    direction = residual
    solution_coords = [jnp.zeros_like(moments[0])]
    norm_now = moments[0]
    for iteration in range(ITERS):
        applied_dot = 4.0 * (
            quadratic(direction, direction, moments, 0)
            - quadratic(direction, direction, moments, 1)
        )
        step = norm_now / applied_dot
        solution_coords = padded_sum(solution_coords, [step * d for d in direction])
        if iteration + 1 < ITERS:
            moved = [-4.0 * step * d for d in direction]
            residual = padded_sum(residual, moved)
            residual = padded_sum(residual, [jnp.zeros_like(step)] + [-m for m in moved])
            norm_next = quadratic(residual, residual, moments, 0)
            ratio = norm_next / norm_now
            direction = padded_sum(residual, [ratio * d for d in direction])
            norm_now = norm_next
    return solution_coords


def split_dot(values, pool):
    pieces = []
    for _ in range(3):
        pieces.append(values.astype(jnp.bfloat16))
        values = values - pieces[-1].astype(jnp.float32)
    parts = jnp.dot(jnp.concatenate(pieces, axis=0), pool, preferred_element_type=jnp.float32)
    size = values.shape[0]
    return (parts[0:size] + parts[size:2 * size]) + parts[2 * size:]


def pooled(load, stride, pool):
    parts = []
    for tile in range(stride):
        part = load(tile, 0)
        for line in range(1, stride):
            part = part + load(tile, line)
        parts.append(part)
    return split_dot(jnp.concatenate(parts, axis=1), pool)


def pool_matrix(stride):
    shape = (LANES * stride, LANES)
    source, target = (lax.broadcasted_iota(jnp.int32, shape, d) for d in range(2))
    return jnp.where(source // stride == target, 1.0 / (stride * stride), 0.0).astype(jnp.bfloat16)


def gather_kernel(
    n_row, n_col, rows, cols, kinds,
    src_hbm, lab_hbm, vec, fines, mids, coord_ref,
    src, lab, edge, edge_lab, pack_up, pack_down, pack_c, pack_d, got_up, got_down, got_c, got_d,
    part, moment, band, patch, sides, token, load_sem, send_sem, recv_sem, chain,
    tell_send, mom_recv, mid_send, chip_recv, fwd_recv, patch_recv,
):
    tiles = cols // LANES
    side_tile = tiles
    main = slice(0, tiles)
    body_rows = pl.ds(TOP, rows)
    n = n_row * n_col
    row, col = lax.axis_index("row"), lax.axis_index("col")
    me = row * n_col + col
    f32 = jnp.float32

    first_row, last_row = row == 0, row == n_row - 1
    first_col, last_col = col == 0, col == n_col - 1
    there = {
        (dr, dc): functools.reduce(jnp.logical_and, [
            jnp.logical_not(edge) for step, edge in (
                (dr < 0, first_row), (dr > 0, last_row), (dc < 0, first_col), (dc > 0, last_col))
            if step])
        for dr, dc in SIDES
    }

    def other_row(step):
        return jnp.where(step >= row, step + 1, step)

    def for_other_rows(act):
        def body(step, _):
            act(other_row(step))
            return 0

        lax.fori_loop(0, n_row - 1, body, 0)

    barrier = pltpu.get_barrier_semaphore()

    def greet(r, c):
        pl.semaphore_signal(barrier, inc=1, device_id=(r, c), device_id_type=MESH)

    greeters = n_row - 1
    for dr, dc in ((-r, -c) for r, c in SIDES):
        if dc:
            pl.when(there[dr, dc])(functools.partial(
                greet, jnp.clip(row + dr, 0, n_row - 1), jnp.clip(col + dc, 0, n_col - 1)))
            greeters = greeters + jnp.where(there[dr, dc], 1, 0)
    def plane_load(k, t, wave):
        lanes = pl.ds(t * LANES, LANES)
        if k < kinds:
            return pltpu.make_async_copy(
                src_hbm.at[k, :, lanes], src.at[k, t, body_rows], load_sem.at[wave])
        return pltpu.make_async_copy(
            lab_hbm.at[:, lanes], lab.at[t, body_rows], load_sem.at[wave])

    def edge_load(k, side):
        here = pl.ds(0 if side == 0 else rows - 8, 8)
        if k < kinds:
            return pltpu.make_async_copy(src_hbm.at[k, here], edge.at[k, side], load_sem.at[0])
        return pltpu.make_async_copy(lab_hbm.at[here], edge_lab.at[side], load_sem.at[0])

    def wait_bytes(ref, sem):
        pltpu.make_async_copy(ref, ref, sem).wait()

    for k in range(kinds + 1):
        for side in range(2):
            edge_load(k, side).start()
    for k in range(kinds + 1):
        for t in (0, tiles - 1):
            plane_load(k, t, 0).start()
    for_other_rows(lambda r: greet(r, col))
    for t in range(1, tiles - 1):
        for k in range(kinds + 1):
            plane_load(k, t, 1).start()

    pad = jnp.zeros((tiles + 1, 8, LANES), f32)
    for start in (0, TOP + rows):
        for k in range(kinds):
            src[k, :, pl.ds(start, 8), :] = pad
        lab[:, pl.ds(start, 8), :] = pad.astype(jnp.int32)
        for w in range(ITERS):
            vec[w, :, pl.ds(start, 8), :] = pad

    def row_part(side, k, t):
        depth = HALO - side
        each = kinds * depth + depth - 1
        return (depth if k < kinds else depth - 1), t * each + k * depth

    n_pack = HALO * (kinds + 1)
    with jax.named_scope("wait_first"):
        wait_bytes(token.at[pl.ds(0, 2 * (kinds + 1) * (8 * tiles + rows))], load_sem.at[0])
    with jax.named_scope("pack"):
        for side in range(2):
            for k in range(kinds + 1):
                for t in range(tiles):
                    lanes = pl.ds(t * LANES, LANES)
                    depth, at = row_part(side, k, t)
                    lines_here = pl.ds(0 if side == 0 else 8 - depth, depth)
                    if k < kinds:
                        value = edge[k, side, lines_here, lanes]
                    else:
                        value = edge_lab[side, lines_here, lanes].astype(f32)
                    (pack_up if side == 0 else pack_down)[pl.ds(at, depth), :] = value
                for end, t in enumerate((0, tiles - 1)):
                    lanes = pl.ds(t * LANES, LANES)
                    lines_here = pl.ds(0 if side == 0 else 8 - HALO, HALO)
                    if k < kinds:
                        value = edge[k, side, lines_here, lanes]
                    else:
                        value = edge_lab[side, lines_here, lanes].astype(f32)
                    pack_d[side, end, pl.ds(HALO * k, HALO), :] = value
        wide_lane = lane_of((rows, LANES))
        for k in range(kinds + 1):
            if k < kinds:
                first, last = src[k, 0, body_rows], src[k, tiles - 1, body_rows]
            else:
                first, last = lab[0, body_rows].astype(f32), lab[tiles - 1, body_rows].astype(f32)
            both = jnp.where(wide_lane < LANES // 2, first, last)
            turned = jnp.transpose(both)
            at = pl.ds(HALO * k, HALO)
            pack_c[0, at, :] = turned[0:HALO]
            pack_c[1, at, :] = turned[LANES - HALO:LANES]

    with jax.named_scope("barrier"):
        pl.semaphore_wait(barrier, greeters)

    def place(dr, dc):
        return (0 if dr < 0 else 1) if dc == 0 else 2 if dr == 0 else 3

    for dr, dc in SIDES:
        mine_r, mine_c = (0 if dr < 0 else 1), (0 if dc < 0 else 1)
        if dc == 0:
            source, target = (pack_up, got_up) if dr < 0 else (pack_down, got_down)
        elif dr == 0:
            source, target = pack_c.at[mine_c], got_c.at[1 - mine_c]
        else:
            source = pack_d.at[mine_r, mine_c]
            target = got_d.at[1 - mine_r, 1 - mine_c]
        device = (
            jnp.clip(row + dr, 0, n_row - 1),
            jnp.clip(col + dc, 0, n_col - 1),
        )
        pl.when(there[dr, dc])(pltpu.make_async_remote_copy(
            src_ref=source, dst_ref=target, send_sem=send_sem.at[place(dr, dc)],
            recv_sem=recv_sem.at[place(-dr, -dc)], device_id=device, device_id_type=MESH,
        ).start)

    beside_rows = jnp.where(there[-1, 0], 1, 0) + jnp.where(there[1, 0], 1, 0)
    beside_cols = jnp.where(there[0, -1], 1, 0) + jnp.where(there[0, 1], 1, 0)
    corners = beside_rows * beside_cols

    def wait_rows(sem, above, below):
        pl.when(there[-1, 0])(lambda: wait_bytes(above, sem.at[0]))
        pl.when(there[1, 0])(lambda: wait_bytes(below, sem.at[1]))
        pl.when(corners == 4)(lambda: wait_bytes(got_d, sem.at[3]))
        pl.when(corners == 2)(lambda: wait_bytes(got_d.at[0], sem.at[3]))
        pl.when(corners == 1)(lambda: wait_bytes(got_d.at[0, 0], sem.at[3]))

    def wait_columns(sem):
        pl.when(beside_cols == 2)(lambda: wait_bytes(got_c, sem.at[2]))
        pl.when(beside_cols == 1)(lambda: wait_bytes(got_c.at[0], sem.at[2]))

    def pass_on(dc):
        pl.semaphore_signal(
            chain.at[0 if dc > 0 else 1], inc=1,
            device_id=(row, jnp.clip(col + dc, 0, n_col - 1)), device_id_type=MESH)

    def hear(dc):
        pl.semaphore_wait(chain.at[0 if dc > 0 else 1], 1)

    def relay(dc):
        hear(dc)
        pass_on(dc)

    inner_col = jnp.logical_and(there[0, 1], there[0, -1])
    upper_half = 2 * col >= n_col
    pl.when(jnp.logical_and(first_col, there[0, 1]))(lambda: pass_on(1))
    pl.when(jnp.logical_and(last_col, there[0, -1]))(lambda: pass_on(-1))

    with jax.named_scope("wait_later"):
        wait_bytes(token.at[pl.ds(0, (kinds + 1) * (tiles - 2) * rows)], load_sem.at[1])
    groups = rows // 8
    lane_r = lane_of((tiles, 8, LANES))
    lane_t = lane_of((8, LANES))
    line_t = line_of((8, LANES))

    def whole_loop(count, act):
        def body(i, _):
            act(i)
            return 0

        lax.fori_loop(0, count, body, 0, unroll=count)

    def save(which, tile, start, value):
        vec[which, tile, pl.ds(start, 8), :] = value

    def applied(which, tile, start, beside):
        mid = lines(vec, (which, tile), start)
        return neighbour_sum(vec, (which, tile), start, mid, beside)

    with jax.named_scope("main_b"):
        def choose(i):
            start = TOP + 8 * i
            left, right = beside_chosen(src, lab, main, start)
            save(1, main, start, left)
            save(2, main, start, right)

        whole_loop(groups, choose)
        whole_loop(groups, lambda i: save(0, main, TOP + 8 * i, right_side_ring(
            src, lab, main, TOP + 8 * i,
            lines(vec, (1, main), TOP + 8 * i), lines(vec, (2, main), TOP + 8 * i))))

    pl.when(jnp.logical_and(inner_col, jnp.logical_not(upper_half)))(lambda: relay(1))

    def inner(which):
        whole_loop(groups, lambda i: save(
            which, main, TOP + 8 * i, applied(which - 1, main, TOP + 8 * i, beside_ring)))


    chips = n_row // 2
    core = lax.rem(row, 2)
    chip = lax.div(row, 2)
    partner = row + 1 - 2 * core
    quad = rows // 4
    pool4, pool2 = pool_matrix(4), pool_matrix(2)

    def blocks(count, w=slice(None)):
        return mids.at[w, :, pl.ds(0, count * quad)]

    def hand(w, owner, target, send, recv):
        block = mids.at[w, :, pl.ds(pl.multiple_of(owner * quad, 8), quad)]
        pltpu.make_async_remote_copy(
            src_ref=block, dst_ref=block, send_sem=send, recv_sem=recv,
            device_id=(target, col), device_id_type=MESH).start()

    def same_core(q):
        return 2 * q + core

    def to_partner(w, owner):
        hand(w, owner, partner, mid_send, fwd_recv)

    others = [lax.rem(chip + step, chips) for step in range(1, chips)]
    if chips == 4:
        others = [3 - chip, chip + 1 - 2 * lax.rem(chip, 2), chip + 2 - 4 * lax.div(chip, 2)]
    others = [same_core(q) for q in others]

    def send_early(w):
        own = pooled(
            lambda tile, line: jnp.concatenate([
                vec[w, 4 * q + tile, pl.ds(TOP + line, quad, stride=4), :]
                for q in range(tiles // 4)], axis=0),
            4, pool4)
        for q in range(tiles // 4):
            mids[w, q, pl.ds(pl.multiple_of(row * quad, 8), quad), :] = own[
                q * quad:(q + 1) * quad]
        for target in others:
            hand(w, row, target, mid_send, chip_recv.at[w])
        to_partner(w, row)

    with jax.named_scope("main_v"):
        for w in range(1, ITERS):
            inner(w)
            send_early(w - 1)
        send_early(ITERS - 1)

    def products(tile, start, right_of, keep):
        powers = [lines(vec, (w, tile), start) for w in range(ITERS)]
        powers.append(lines(vec, (ITERS - 1, tile), start + 1) + right_of(powers[-1]))
        kept = [keep(p) for p in powers[:ITERS]]
        return [kept[i // 2] * powers[(i + 1) // 2] for i in range(2 * ITERS)]

    def right_ring(mid):
        right = pltpu.roll(mid, LANES - 1, axis=2)
        return jnp.where(
            lane_r == LANES - 1, jnp.concatenate([right[1:], right[:1]], axis=0), right)

    def right_tile(mid):
        return pltpu.roll(mid, LANES - 1, axis=1)

    def keep_main(p):
        edge_lane = lane_of((1, 8, LANES))
        return jnp.concatenate([
            jnp.where(edge_lane < HALO, 0.0, p[0:1]), p[1:tiles - 1],
            jnp.where(edge_lane >= LANES - HALO, 0.0, p[tiles - 1:]),
        ], axis=0)

    def fold(value):
        if len(value.shape) == 2:
            return value
        total = value[0]
        for t in range(1, value.shape[0]):
            total = total + value[t]
        return total

    with jax.named_scope("main_m"):
        def main_body(i, sums):
            new = products(main, TOP + HALO + 8 * i, right_ring, keep_main)
            return tuple(s + fold(p) for s, p in zip(sums, new))

        zero8 = jnp.zeros((8, LANES), f32)
        sums = lax.fori_loop(
            0, groups - 1, main_body, tuple(zero8 for _ in range(2 * ITERS)), unroll=groups - 1)
        for i, s in enumerate(sums):
            part[i] = s
    with jax.named_scope("side_fill"):
        for k in range(kinds + 1):
            if k < kinds:
                first, last = src[k, 0, body_rows], src[k, tiles - 1, body_rows]
                src[k, side_tile, body_rows, :] = jnp.where(
                    wide_lane < LANES // 2, pltpu.roll(first, 2 * HALO, axis=1), last)
            else:
                first, last = lab[0, body_rows], lab[tiles - 1, body_rows]
                lab[side_tile, body_rows, :] = jnp.where(
                    wide_lane < LANES // 2, pltpu.roll(first, 2 * HALO, axis=1), last)

    with jax.named_scope("relay"):
        pl.when(jnp.logical_and(inner_col, upper_half))(lambda: relay(1))
        pl.when(jnp.logical_and(inner_col, upper_half))(lambda: relay(-1))

    with jax.named_scope("wait_cols"):
        wait_columns(recv_sem)

    with jax.named_scope("unpack_cols"):
        for k in range(kinds + 1):
            at = pl.ds(HALO * k, HALO)
            right = jnp.where(last_col, 0.0, got_c[1, at, :])
            left = jnp.where(first_col, 0.0, got_c[0, at, :])
            turned = jnp.transpose(jnp.concatenate([right, left], axis=0))
            if k < kinds:
                src[k, side_tile, body_rows, 0:2 * HALO] = turned
            else:
                lab[side_tile, body_rows, 0:2 * HALO] = turned.astype(jnp.int32)
        corner_lane = lane_of((HALO, LANES))

    off_lane = ((lane_t < HALO) & last_col) | ((lane_t >= HALO) & (lane_t < 2 * HALO) & first_col)
    off_top = (line_t < HALO) & first_row
    off_bottom = (line_t >= HALO) & last_row
    ends = ((TOP - HALO, off_top), (TOP + rows - HALO, off_bottom))

    def stage(which, tile, start, beside):
        if which == 0:
            return right_side(src, lab, tile, start, beside)
        return applied(which - 1, tile, start, beside)

    def side_groups(which, begin, end):
        for i in range(begin, end):
            start = TOP - HALO + 8 * i
            off = off_lane
            if i == 0:
                off = off | off_top
            if i == groups:
                off = off | off_bottom
            save(which, side_tile, start, jnp.where(
                off, 0.0, stage(which, side_tile, start, beside_tile)))

    def side_inner(which):
        begin = TOP + HALO + 8 * which
        count = groups - 1 - 2 * which
        whole_loop(count, lambda i: save(
            which, side_tile, begin + 8 * i, jnp.where(
                off_lane, 0.0, stage(which, side_tile, begin + 8 * i, beside_tile))))

    on_side = ((lane_t >= 2 * HALO) & (lane_t < 3 * HALO)) | (lane_t >= LANES - HALO)

    def side_sums(begin, end, sums):
        def body(i, sums):
            new = products(
                side_tile, TOP + 8 * (begin + i), right_tile, lambda p: jnp.where(on_side, p, 0.0))
            return tuple(s + p for s, p in zip(sums, new))

        return list(lax.fori_loop(0, end - begin, body, tuple(sums), unroll=end - begin))

    with jax.named_scope("side_inner"):
        for which in range(ITERS):
            side_inner(which)
        for i, s in enumerate(side_sums(ITERS, groups - ITERS, [part[i] for i in range(2 * ITERS)])):
            part[i] = s

    with jax.named_scope("wait_halo"):
        wait_rows(recv_sem, got_down, got_up)

    with jax.named_scope("unpack"):
        for side in range(2):
            missing = first_row if side == 0 else last_row
            got = got_down if side == 0 else got_up
            for k in range(kinds + 1):
                wide = []
                for t in range(tiles):
                    depth, at = row_part(1 - side, k, t)
                    wide.append(jnp.where(missing, 0.0, got[pl.ds(at, depth), :]))
                shift = HALO - depth if side == 0 else 0
                near_lines = slice(shift, shift + depth)
                at = pl.ds(HALO * k, HALO)
                right = jnp.where(missing | last_col, 0.0, got_d[side, 1, at, :])[near_lines]
                left = jnp.where(missing | first_col, 0.0, got_d[side, 0, at, :])[near_lines]
                corner_lane = lane_of((depth, LANES))
                moved = pltpu.roll(
                    jnp.where(corner_lane >= LANES - HALO, left, wide[0]), 2 * HALO, axis=1)
                own = jnp.where(corner_lane < LANES // 2, moved, wide[-1])
                wide.append(jnp.where(corner_lane < HALO, right, own))
                base = TOP - depth if side == 0 else TOP + rows
                for t, value in enumerate(wide):
                    if k < kinds:
                        src[k, t, pl.ds(base, depth), :] = value
                    else:
                        lab[t, pl.ds(base, depth), :] = value.astype(jnp.int32)

    with jax.named_scope("frames"):
        for which in range(ITERS):
            side_groups(which, 0, 1 + which)
            side_groups(which, groups - which, groups + 1)
            for start, off in ends:
                save(which, main, start, jnp.where(
                    off[None], 0.0, stage(which, main, start, beside_ring)))

    with jax.named_scope("moments"):
        sums = side_sums(0, ITERS, [part[i] for i in range(2 * ITERS)])
        sums = side_sums(groups - ITERS, groups, sums)
        for (start, _), on in zip(ends, (line_t >= HALO, line_t < HALO)):
            new = products(main, start, right_ring, lambda p: jnp.where(on[None], keep_main(p), 0.0))
            sums = [s + fold(p) for s, p in zip(sums, new)]
        lane1 = lane_of((1, LANES))
        mine = jnp.zeros((1, LANES), f32)
        for i, s in enumerate(sums):
            mine = jnp.where(lane1 == i, jnp.sum(s, keepdims=True), mine)
        moment[me] = mine

    with jax.named_scope("send_moments"):
        pl.when(jnp.logical_and(last_col, there[0, -1]))(lambda: hear(1))

        def tell(r, c):
            pltpu.make_async_remote_copy(
                src_ref=moment.at[me], dst_ref=moment.at[me], send_sem=tell_send, recv_sem=mom_recv,
                device_id=(r, c), device_id_type=MESH).start()

        def tell_block(c):
            def body(r, _):
                tell(r, c)
                return 0

            lax.fori_loop(0, n_row, body, 0)

        for c in range(n_col - 1):
            pl.when(c < col)(functools.partial(tell_block, c))
        for_other_rows(lambda r: tell(r, col))
        pl.when(jnp.logical_and(inner_col, jnp.logical_not(upper_half)))(lambda: relay(-1))

    def tell_rest():
        pl.when(first_col)(lambda: hear(-1))
        for c in range(1, n_col):
            pl.when(c > col)(functools.partial(tell_block, c))

    with jax.named_scope("tell_inner"):
        pl.when(inner_col)(tell_rest)

    ends_of = ((0, TOP), (quad - 1, TOP + rows - 4))
    lines_of = [(w, e, q) for w in range(ITERS) for e in range(2) for q in range(tiles // 4)]
    with jax.named_scope("patch"):
        for at, (w, e, q) in enumerate(lines_of):
            for i in range(4):
                four = vec[w, 4 * q + i, pl.ds(ends_of[e][1], 4), :]
                band[i, at:at + 1, :] = jnp.sum(four, axis=0, keepdims=True)
        wide = jnp.concatenate([band[i] for i in range(4)], axis=1)
        patch[row, 0:wide.shape[0], :] = split_dot(wide, pool4)
        odd = lax.rem(row, 2) == 1
        row_lane = lane_of((1, rows))
        for w in range(ITERS):
            flat = vec[w, side_tile, pl.ds(TOP, quad, stride=4), :]
            for line in range(1, 4):
                flat = flat + vec[w, side_tile, pl.ds(TOP + line, quad, stride=4), :]
            even_part, odd_part = jnp.where(odd, 0.0, flat), jnp.where(odd, flat, 0.0)
            turned = jnp.transpose(jnp.concatenate([even_part, odd_part] * 2, axis=0))
            left = jnp.sum(turned[2 * HALO:3 * HALO], axis=0, keepdims=True)
            right = jnp.sum(turned[LANES - HALO:], axis=0, keepdims=True)
            at = len(lines_of) + w
            patch[row, at:at + 1, :] = jnp.where(row_lane < 2 * quad, left, right) * (1.0 / 16)
        for_other_rows(lambda r: pltpu.make_async_remote_copy(
            src_ref=patch.at[row], dst_ref=patch.at[row], send_sem=tell_send,
            recv_sem=patch_recv, device_id=(r, col), device_id_type=MESH).start())

    with jax.named_scope("merge"):
        for w in range(ITERS):
            side = vec[w, side_tile, body_rows]
            vec[w, 0, body_rows, :] = jnp.where(
                wide_lane < HALO, pltpu.roll(side, LANES - 2 * HALO, axis=1), vec[w, 0, body_rows])
            vec[w, tiles - 1, body_rows, :] = jnp.where(
                wide_lane >= LANES - HALO, side, vec[w, tiles - 1, body_rows])

    with jax.named_scope("fines"):
        half = rows // 2
        for w in range(ITERS):
            own = pooled(
                lambda tile, line: jnp.concatenate([
                    vec[w, 2 * q + tile, pl.ds(TOP + line, half, stride=2), :]
                    for q in range(tiles // 2)], axis=0),
                2, pool2)
            for q in range(tiles // 2):
                fines[w, q] = own[q * half:(q + 1) * half]

    with jax.named_scope("tell_first"):
        pl.when(jnp.logical_and(first_col, there[0, 1]))(tell_rest)

    with jax.named_scope("near"):
        for w in range(ITERS):
            wait_bytes(blocks(chips - 1, w), chip_recv.at[w])
            for owner in others:
                to_partner(w, owner)

    with jax.named_scope("wait_patch"):
        patches = patch.at[pl.ds(0, n_row - 1)]
        wait_bytes(patches, patch_recv)
    with jax.named_scope("prepare"):
        for pair in range(n_row // 2):
            for w in range(ITERS):
                at = len(lines_of) + w
                both = patch[2 * pair, at:at + 1, :] + patch[2 * pair + 1, at:at + 1, :]
                turned = jnp.transpose(jnp.broadcast_to(both, (8, LANES)))
                for end in range(2):
                    part_here = turned[2 * quad * end:2 * quad * (end + 1), 0:1]
                    sides[w, end, pl.ds(2 * pair * quad, 2 * quad), :] = jnp.broadcast_to(
                        part_here, (2 * quad, LANES))

    with jax.named_scope("wait_forwards"):
        wait_bytes(blocks(2 * chips - 1), mid_send)
        wait_bytes(blocks(chips), fwd_recv)
    with jax.named_scope("apply"):
        for owner in range(n_row):
            for at, (w, e, q) in enumerate(lines_of):
                mids[w, q, pl.ds(owner * quad + ends_of[e][0], 1), :] = patch[
                    owner, at:at + 1, :]
        all_lane = lane_of((n_row * quad, LANES))
        for w in range(ITERS):
            for end, q, lane in ((0, 0, 0), (1, tiles // 4 - 1, LANES - 1)):
                mids[w, q] = jnp.where(all_lane == lane, sides[w, end], mids[w, q])

    with jax.named_scope("wait_moments"):
        everyone = moment.at[pl.ds(0, n - 1)]
        wait_bytes(everyone, mom_recv)
    with jax.named_scope("coefs"):
        total = jnp.sum(moment[...], axis=0)
        moments = [
            (0.25 ** i * (1.0 if i < 2 * ITERS - 1 else 2.0))
            * jnp.sum(jnp.where(lane1 == i, total, 0.0), axis=1, keepdims=True)
            for i in range(2 * ITERS)
        ]
        for w, c in enumerate(coefficients(moments)):
            coord_ref[w] = jnp.broadcast_to(0.25 ** w * c, (8, LANES))

    with jax.named_scope("wait_sends"):
        wait_rows(send_sem, got_up, got_down)
        wait_columns(send_sem)
        wait_bytes(token.at[pl.ds(0, n - 1 + (n_row - 1) * patch.shape[1])], tell_send)


def finish_kernel(
    rows, cols, vec, fines, mids, coord_ref, blend_out, fine_out, mid_out, coarse_out,
    blend, fine, mid, coarse, out_sem,
):
    tiles = cols // LANES

    def leave(which, source, target, q):
        pltpu.make_async_copy(
            source.at[q], target.at[:, pl.ds(q * LANES, LANES)], out_sem.at[which]).start()

    def combine(load, target, height):
        coords = [coord_ref[w] for w in range(ITERS)]

        def body(g, _):
            start = pl.multiple_of(g * 8, 8)
            strip = None
            for w in range(ITERS):
                term = coords[w] * load(w, start)
                strip = term if strip is None else strip + term
            target[pl.ds(start, 8), :] = strip
            return 0

        lax.fori_loop(0, height // 8, body, 0, unroll=height // 8)

    tall = mid.shape[1]
    with jax.named_scope("mid"):
        for q in range(mid.shape[0]):
            combine(lambda w, start: mids[w, q, pl.ds(start, 8), :], mid.at[q], tall)
            leave(1, mid, mid_out, q)
    with jax.named_scope("coarse"):
        pool2 = pool_matrix(2)
        for q in range(coarse.shape[0]):
            coarse[q] = pooled(
                lambda tile, line: mid[2 * q + tile, pl.ds(line, tall // 2, stride=2), :], 2, pool2)
    with jax.named_scope("blend"):
        for t in range(tiles):
            combine(lambda w, start: vec[w, t, pl.ds(start + TOP, 8), :], blend.at[t], rows)
            leave(0, blend, blend_out, t)
    with jax.named_scope("fine"):
        for q in range(tiles // 2):
            combine(lambda w, start: fines[w, q, pl.ds(start, 8), :], fine.at[q], rows // 2)
            leave(2, fine, fine_out, q)
    with jax.named_scope("coarse_out"):
        for q in range(coarse.shape[0]):
            leave(3, coarse, coarse_out, q)
    with jax.named_scope("wait_out"):
        for which, ref in enumerate((blend, mid, fine, coarse)):
            pltpu.make_async_copy(ref, ref, out_sem.at[which]).wait()


def per_device(n_row, n_col, sources, labels):
    kinds, rows, cols = sources.shape
    n = n_row * n_col
    tiles = cols // LANES
    tall = rows + 2 * TOP
    n_pack = HALO * (kinds + 1)
    f32 = jnp.float32
    vmem = pl.BlockSpec(memory_space=pltpu.VMEM)
    hbm = pl.BlockSpec(memory_space=pltpu.HBM)
    up_lines, down_lines = ((kinds * d + d - 1) * tiles for d in (HALO, HALO - 1))
    token_lines = (kinds + 1) * max(2 * (8 * tiles + rows), (tiles - 2) * rows)
    mid_rows, coarse_rows = n_row * rows // 4, n_row * rows // 8
    chips = n_row // 2
    dma = pltpu.SemaphoreType.DMA
    vec, fines, mids, coords = pl.pallas_call(
        functools.partial(gather_kernel, n_row, n_col, rows, cols, kinds),
        out_shape=(
            jax.ShapeDtypeStruct((ITERS, tiles + 1, tall, LANES), f32),
            jax.ShapeDtypeStruct((ITERS, tiles // 2, rows // 2, LANES), f32),
            jax.ShapeDtypeStruct((ITERS, tiles // 4, mid_rows, LANES), f32),
            jax.ShapeDtypeStruct((ITERS, 8, LANES), f32),
        ),
        in_specs=[hbm] * 2,
        out_specs=(vmem,) * 4,
        scratch_shapes=[
            pltpu.VMEM((kinds, tiles + 1, tall, LANES), f32),
            pltpu.VMEM((tiles + 1, tall, LANES), jnp.int32),
            pltpu.VMEM((kinds, 2, 8, cols), f32),
            pltpu.VMEM((2, 8, cols), jnp.int32),
            pltpu.VMEM((up_lines, LANES), f32),
            pltpu.VMEM((down_lines, LANES), f32),
            pltpu.VMEM((2, n_pack, rows), f32),
            pltpu.VMEM((2, 2, n_pack, LANES), f32),
            pltpu.VMEM((up_lines, LANES), f32),
            pltpu.VMEM((down_lines, LANES), f32),
            pltpu.VMEM((2, n_pack, rows), f32),
            pltpu.VMEM((2, 2, n_pack, LANES), f32),
            pltpu.VMEM((2 * ITERS, 8, LANES), f32),
            pltpu.VMEM((n, 1, LANES), f32),
            pltpu.VMEM((4, ITERS * (tiles // 2), LANES), f32),
            pltpu.VMEM((n_row, ITERS * (tiles // 2) + 4, LANES), f32),
            pltpu.VMEM((ITERS, 2, mid_rows, LANES), f32),
            pltpu.VMEM((token_lines, LANES), f32),
            dma((2,)),
            dma((4,)),
            dma((4,)),
            pltpu.SemaphoreType.REGULAR((2,)),
            dma,
            dma,
            dma,
            dma((ITERS,)),
            dma,
            dma,
        ],
        compiler_params=pltpu.CompilerParams(
            collective_id=0, has_side_effects=True, vmem_limit_bytes=24 * 2**20),
    )(
        pltpu.with_memory_space_constraint(sources, pltpu.HBM),
        pltpu.with_memory_space_constraint(labels, pltpu.HBM),
    )
    return pl.pallas_call(
        functools.partial(finish_kernel, rows, cols),
        out_shape=(
            jax.ShapeDtypeStruct((rows, cols), f32),
            jax.ShapeDtypeStruct((rows // 2, cols // 2), f32),
            jax.ShapeDtypeStruct((mid_rows, cols // 4), f32),
            jax.ShapeDtypeStruct((coarse_rows, cols // 8), f32),
        ),
        in_specs=[vmem] * 4,
        out_specs=(hbm,) * 4,
        scratch_shapes=[
            pltpu.VMEM((tiles, rows, LANES), f32),
            pltpu.VMEM((tiles // 2, rows // 2, LANES), f32),
            pltpu.VMEM((tiles // 4, mid_rows, LANES), f32),
            pltpu.VMEM((tiles // 8, coarse_rows, LANES), f32),
            dma((4,)),
        ],
        compiler_params=pltpu.CompilerParams(vmem_limit_bytes=24 * 2**20),
    )(vec, fines, mids, coords)


def solution(mesh):
    sizes = dict(mesh.shape)
    return jax.shard_map(
        functools.partial(per_device, sizes["row"], sizes["col"]),
        mesh=mesh,
        in_specs=(P(None, "row", "col"), P("row", "col")),
        out_specs=(P("row", "col"), P("row", "col"), P(None, "col"), P(None, "col")),
        check_vma=False,
    )
```

```python
import functools

import jax
import jax.numpy as jnp
from jax import lax
from jax.experimental import pallas as pl
from jax.experimental.pallas import tpu as pltpu
from jax.sharding import PartitionSpec as P

ITERS = 3
MESH = pl.DeviceIdType.MESH
HALO = 4
TOP = 8
LANES = 128
SIDES = ((1, 1), (1, -1), (-1, 1), (-1, -1), (1, 0), (-1, 0), (0, 1), (0, -1))


def lane_of(shape):
    return lax.broadcasted_iota(jnp.int32, shape, len(shape) - 1)


def line_of(shape):
    return lax.broadcasted_iota(jnp.int32, shape, len(shape) - 2)


def lines(ref, index, start):
    return ref[index + (pl.ds(start, 8), slice(None))]


def beside_ring(mid):
    tiles = mid.shape[0]
    lane = lane_of(mid.shape)
    left = pltpu.roll(mid, 1, axis=2)
    right = pltpu.roll(mid, LANES - 1, axis=2)
    from_left = jnp.concatenate([left[tiles - 1:], left[:tiles - 1]], axis=0)
    from_right = jnp.concatenate([right[1:], right[:1]], axis=0)
    return jnp.where(lane == 0, from_left, left) + jnp.where(lane == LANES - 1, from_right, right)


def beside_tile(mid):
    return pltpu.roll(mid, 1, axis=1) + pltpu.roll(mid, LANES - 1, axis=1)


def neighbour_sum(ref, index, start, mid, beside):
    return (lines(ref, index, start - 1) + lines(ref, index, start + 1)) + beside(mid)


def right_side(src, lab, tile, start, beside):
    here = lines(lab, (tile,), start)
    total = None
    for k in reversed(range(src.shape[0])):
        mid = lines(src, (k, tile), start)
        term = 4.0 * mid - neighbour_sum(src, (k, tile), start, mid, beside)
        total = term if total is None else jnp.where(here == k, term, total)
    return total


def from_left(values):
    lane = lane_of(values.shape)
    moved = pltpu.roll(values, 1, axis=2)
    return jnp.where(lane == 0, jnp.concatenate([moved[-1:], moved[:-1]], axis=0), moved)


def from_right(values):
    lane = lane_of(values.shape)
    moved = pltpu.roll(values, LANES - 1, axis=2)
    return jnp.where(lane == LANES - 1, jnp.concatenate([moved[1:], moved[:1]], axis=0), moved)


def chosen(here, values):
    total = values[-1]
    for k in reversed(range(len(values) - 1)):
        total = jnp.where(here == k, values[k], total)
    return total


def beside_chosen(src, lab, tile, start):
    here = lines(lab, (tile,), start)
    mids = [lines(src, (k, tile), start) for k in range(src.shape[0])]
    return chosen(from_right(here), mids), chosen(from_left(here), mids)


def right_side_ring(src, lab, tile, start, left, right):
    here = lines(lab, (tile,), start)
    crosses = [
        4.0 * lines(src, (k, tile), start)
        - (lines(src, (k, tile), start - 1) + lines(src, (k, tile), start + 1))
        for k in range(src.shape[0])
    ]
    return chosen(here, crosses) - (from_left(left) + from_right(right))


def quadratic(left, right, moments, shift):
    total = None
    for i, a in enumerate(left):
        for j, b in enumerate(right):
            term = a * b * moments[i + j + shift]
            total = term if total is None else total + term
    return total


def padded_sum(a, b):
    if len(a) < len(b):
        a, b = b, a
    return [x + b[i] if i < len(b) else x for i, x in enumerate(a)]


def coefficients(moments):
    residual = [jnp.ones_like(moments[0])]
    direction = residual
    solution_coords = [jnp.zeros_like(moments[0])]
    norm_now = moments[0]
    for iteration in range(ITERS):
        applied_dot = 4.0 * (
            quadratic(direction, direction, moments, 0)
            - quadratic(direction, direction, moments, 1)
        )
        step = norm_now / applied_dot
        solution_coords = padded_sum(solution_coords, [step * d for d in direction])
        if iteration + 1 < ITERS:
            moved = [-4.0 * step * d for d in direction]
            residual = padded_sum(residual, moved)
            residual = padded_sum(residual, [jnp.zeros_like(step)] + [-m for m in moved])
            norm_next = quadratic(residual, residual, moments, 0)
            ratio = norm_next / norm_now
            direction = padded_sum(residual, [ratio * d for d in direction])
            norm_now = norm_next
    return solution_coords


def split_dot(values, pool):
    pieces = []
    for _ in range(3):
        pieces.append(values.astype(jnp.bfloat16))
        values = values - pieces[-1].astype(jnp.float32)
    parts = jnp.dot(jnp.concatenate(pieces, axis=0), pool, preferred_element_type=jnp.float32)
    size = values.shape[0]
    return (parts[0:size] + parts[size:2 * size]) + parts[2 * size:]


def pooled(load, stride, pool):
    parts = []
    for tile in range(stride):
        part = load(tile, 0)
        for line in range(1, stride):
            part = part + load(tile, line)
        parts.append(part)
    return split_dot(jnp.concatenate(parts, axis=1), pool)


def pool_matrix(stride):
    shape = (LANES * stride, LANES)
    source, target = (lax.broadcasted_iota(jnp.int32, shape, d) for d in range(2))
    return jnp.where(source // stride == target, 1.0 / (stride * stride), 0.0).astype(jnp.bfloat16)


def gather_kernel(
    n_row, n_col, rows, cols, kinds,
    src_hbm, lab_hbm, vec, fines, mids, coord_ref,
    src, lab, edge, edge_lab, pack_up, pack_down, pack_c, pack_d, got_up, got_down, got_c, got_d,
    part, moment, band, patch, sides, token, load_sem, send_sem, recv_sem, chain,
    mom_recv, chip_recv, fwd_recv, patch_recv,
):
    tell_send, mid_send = load_sem.at[0], load_sem.at[1]
    tiles = cols // LANES
    side_tile = tiles
    main = slice(0, tiles)
    body_rows = pl.ds(TOP, rows)
    n = n_row * n_col
    row, col = lax.axis_index("row"), lax.axis_index("col")
    me = row * n_col + col
    f32 = jnp.float32

    first_row, last_row = row == 0, row == n_row - 1
    first_col, last_col = col == 0, col == n_col - 1
    there = {
        (dr, dc): functools.reduce(jnp.logical_and, [
            jnp.logical_not(edge) for step, edge in (
                (dr < 0, first_row), (dr > 0, last_row), (dc < 0, first_col), (dc > 0, last_col))
            if step])
        for dr, dc in SIDES
    }

    def other_row(step):
        return jnp.where(step >= row, step + 1, step)

    def for_other_rows(act):
        def body(step, _):
            act(other_row(step))
            return 0

        lax.fori_loop(0, n_row - 1, body, 0)

    barrier = pltpu.get_barrier_semaphore()

    def greet(r, c):
        pl.semaphore_signal(barrier, inc=1, device_id=(r, c), device_id_type=MESH)

    greeters = n_row - 1
    for dr, dc in ((-r, -c) for r, c in SIDES):
        if dc:
            pl.when(there[dr, dc])(functools.partial(
                greet, jnp.clip(row + dr, 0, n_row - 1), jnp.clip(col + dc, 0, n_col - 1)))
            greeters = greeters + jnp.where(there[dr, dc], 1, 0)
    def plane_load(k, t, wave):
        lanes = pl.ds(t * LANES, LANES)
        if k < kinds:
            return pltpu.make_async_copy(
                src_hbm.at[k, :, lanes], src.at[k, t, body_rows], load_sem.at[wave])
        return pltpu.make_async_copy(
            lab_hbm.at[:, lanes], lab.at[t, body_rows], load_sem.at[wave])

    def edge_load(k, side):
        here = pl.ds(0 if side == 0 else rows - 8, 8)
        if k < kinds:
            return pltpu.make_async_copy(src_hbm.at[k, here], edge.at[k, side], load_sem.at[0])
        return pltpu.make_async_copy(lab_hbm.at[here], edge_lab.at[side], load_sem.at[0])

    def wait_bytes(ref, sem):
        pltpu.make_async_copy(ref, ref, sem).wait()

    for k in range(kinds + 1):
        for side in range(2):
            edge_load(k, side).start()
    for k in range(kinds + 1):
        for t in (0, tiles - 1):
            plane_load(k, t, 0).start()
    for_other_rows(lambda r: greet(r, col))
    for t in range(1, tiles - 1):
        for k in range(kinds + 1):
            plane_load(k, t, 1).start()

    pad = jnp.zeros((tiles + 1, 8, LANES), f32)
    for start in (0, TOP + rows):
        for k in range(kinds):
            src[k, :, pl.ds(start, 8), :] = pad
        lab[:, pl.ds(start, 8), :] = pad.astype(jnp.int32)
        for w in range(ITERS):
            vec[w, :, pl.ds(start, 8), :] = pad

    def row_part(side, k, t):
        depth = HALO - side
        each = kinds * depth + depth - 1
        return (depth if k < kinds else depth - 1), t * each + k * depth

    n_pack = HALO * (kinds + 1)
    with jax.named_scope("wait_first"):
        wait_bytes(token.at[pl.ds(0, 2 * (kinds + 1) * (8 * tiles + rows))], load_sem.at[0])
    with jax.named_scope("pack"):
        for side in range(2):
            for k in range(kinds + 1):
                for t in range(tiles):
                    lanes = pl.ds(t * LANES, LANES)
                    depth, at = row_part(side, k, t)
                    lines_here = pl.ds(0 if side == 0 else 8 - depth, depth)
                    if k < kinds:
                        value = edge[k, side, lines_here, lanes]
                    else:
                        value = edge_lab[side, lines_here, lanes].astype(f32)
                    (pack_up if side == 0 else pack_down)[pl.ds(at, depth), :] = value
                for end, t in enumerate((0, tiles - 1)):
                    lanes = pl.ds(t * LANES, LANES)
                    lines_here = pl.ds(0 if side == 0 else 8 - HALO, HALO)
                    if k < kinds:
                        value = edge[k, side, lines_here, lanes]
                    else:
                        value = edge_lab[side, lines_here, lanes].astype(f32)
                    pack_d[side, end, pl.ds(HALO * k, HALO), :] = value
        wide_lane = lane_of((rows, LANES))
        for k in range(kinds + 1):
            if k < kinds:
                first, last = src[k, 0, body_rows], src[k, tiles - 1, body_rows]
            else:
                first, last = lab[0, body_rows].astype(f32), lab[tiles - 1, body_rows].astype(f32)
            both = jnp.where(wide_lane < LANES // 2, first, last)
            turned = jnp.transpose(both)
            at = pl.ds(HALO * k, HALO)
            pack_c[0, at, :] = turned[0:HALO]
            pack_c[1, at, :] = turned[LANES - HALO:LANES]

    with jax.named_scope("barrier"):
        pl.semaphore_wait(barrier, greeters)

    def place(dr, dc):
        return (0 if dr < 0 else 1) if dc == 0 else 2 if dr == 0 else 3

    for dr, dc in SIDES:
        mine_r, mine_c = (0 if dr < 0 else 1), (0 if dc < 0 else 1)
        if dc == 0:
            source, target = (pack_up, got_up) if dr < 0 else (pack_down, got_down)
        elif dr == 0:
            source, target = pack_c.at[mine_c], got_c.at[1 - mine_c]
        else:
            source = pack_d.at[mine_r, mine_c]
            target = got_d.at[1 - mine_r, 1 - mine_c]
        device = (
            jnp.clip(row + dr, 0, n_row - 1),
            jnp.clip(col + dc, 0, n_col - 1),
        )
        pl.when(there[dr, dc])(pltpu.make_async_remote_copy(
            src_ref=source, dst_ref=target, send_sem=send_sem.at[place(dr, dc)],
            recv_sem=recv_sem.at[place(-dr, -dc)], device_id=device, device_id_type=MESH,
        ).start)

    beside_rows = jnp.where(there[-1, 0], 1, 0) + jnp.where(there[1, 0], 1, 0)
    beside_cols = jnp.where(there[0, -1], 1, 0) + jnp.where(there[0, 1], 1, 0)
    corners = beside_rows * beside_cols

    def wait_rows(sem, above, below):
        pl.when(there[-1, 0])(lambda: wait_bytes(above, sem.at[0]))
        pl.when(there[1, 0])(lambda: wait_bytes(below, sem.at[1]))
        pl.when(corners == 4)(lambda: wait_bytes(got_d, sem.at[3]))
        pl.when(corners == 2)(lambda: wait_bytes(got_d.at[0], sem.at[3]))
        pl.when(corners == 1)(lambda: wait_bytes(got_d.at[0, 0], sem.at[3]))

    def wait_columns(sem):
        pl.when(beside_cols == 2)(lambda: wait_bytes(got_c, sem.at[2]))
        pl.when(beside_cols == 1)(lambda: wait_bytes(got_c.at[0], sem.at[2]))

    def pass_on(dc):
        pl.semaphore_signal(
            chain.at[0 if dc > 0 else 1], inc=1,
            device_id=(row, jnp.clip(col + dc, 0, n_col - 1)), device_id_type=MESH)

    def hear(dc):
        pl.semaphore_wait(chain.at[0 if dc > 0 else 1], 1)

    def relay(dc):
        hear(dc)
        pass_on(dc)

    inner_col = jnp.logical_and(there[0, 1], there[0, -1])
    upper_half = 2 * col >= n_col
    pl.when(jnp.logical_and(first_col, there[0, 1]))(lambda: pass_on(1))
    pl.when(jnp.logical_and(last_col, there[0, -1]))(lambda: pass_on(-1))

    with jax.named_scope("wait_later"):
        wait_bytes(token.at[pl.ds(0, (kinds + 1) * (tiles - 2) * rows)], load_sem.at[1])
    groups = rows // 8
    lane_r = lane_of((tiles, 8, LANES))
    lane_t = lane_of((8, LANES))
    line_t = line_of((8, LANES))

    def whole_loop(count, act):
        def body(i, _):
            act(i)
            return 0

        lax.fori_loop(0, count, body, 0, unroll=count)

    def save(which, tile, start, value):
        vec[which, tile, pl.ds(start, 8), :] = value

    def applied(which, tile, start, beside):
        mid = lines(vec, (which, tile), start)
        return neighbour_sum(vec, (which, tile), start, mid, beside)

    with jax.named_scope("main_b"):
        def choose(i):
            start = TOP + 8 * i
            left, right = beside_chosen(src, lab, main, start)
            save(1, main, start, left)
            save(2, main, start, right)

        whole_loop(groups, choose)
        whole_loop(groups, lambda i: save(0, main, TOP + 8 * i, right_side_ring(
            src, lab, main, TOP + 8 * i,
            lines(vec, (1, main), TOP + 8 * i), lines(vec, (2, main), TOP + 8 * i))))

    pl.when(jnp.logical_and(inner_col, jnp.logical_not(upper_half)))(lambda: relay(1))

    def inner(which):
        whole_loop(groups, lambda i: save(
            which, main, TOP + 8 * i, applied(which - 1, main, TOP + 8 * i, beside_ring)))


    chips = n_row // 2
    core = lax.rem(row, 2)
    chip = lax.div(row, 2)
    partner = row + 1 - 2 * core
    quad = rows // 4
    pool4, pool2 = pool_matrix(4), pool_matrix(2)

    def blocks(count):
        return mids.at[:, :, pl.ds(0, count * quad)]

    def hand(w, owner, target, send, recv):
        block = mids.at[w, :, pl.ds(pl.multiple_of(owner * quad, 8), quad)]
        pltpu.make_async_remote_copy(
            src_ref=block, dst_ref=block, send_sem=send, recv_sem=recv,
            device_id=(target, col), device_id_type=MESH).start()

    def same_core(q):
        return 2 * q + core

    def to_partner(w, owner):
        hand(w, owner, partner, mid_send, fwd_recv)

    others = [lax.rem(chip + step, chips) for step in range(1, chips)]
    if chips == 4:
        others = [3 - chip, chip + 1 - 2 * lax.rem(chip, 2), chip + 2 - 4 * lax.div(chip, 2)]
    others = [same_core(q) for q in others]

    def send_early(w):
        own = pooled(
            lambda tile, line: jnp.concatenate([
                vec[w, 4 * q + tile, pl.ds(TOP + line, quad, stride=4), :]
                for q in range(tiles // 4)], axis=0),
            4, pool4)
        for q in range(tiles // 4):
            mids[w, q, pl.ds(pl.multiple_of(row * quad, 8), quad), :] = own[
                q * quad:(q + 1) * quad]
        for target in others:
            hand(w, row, target, mid_send, chip_recv)
        to_partner(w, row)

    with jax.named_scope("main_v"):
        for w in range(1, ITERS):
            inner(w)
            send_early(w - 1)
        send_early(ITERS - 1)

    def products(tile, start, right_of, keep):
        powers = [lines(vec, (w, tile), start) for w in range(ITERS)]
        powers.append(lines(vec, (ITERS - 1, tile), start + 1) + right_of(powers[-1]))
        kept = [keep(p) for p in powers[:ITERS]]
        return [kept[i // 2] * powers[(i + 1) // 2] for i in range(2 * ITERS)]

    def right_ring(mid):
        right = pltpu.roll(mid, LANES - 1, axis=2)
        return jnp.where(
            lane_r == LANES - 1, jnp.concatenate([right[1:], right[:1]], axis=0), right)

    def right_tile(mid):
        return pltpu.roll(mid, LANES - 1, axis=1)

    def keep_main(p):
        edge_lane = lane_of((1, 8, LANES))
        return jnp.concatenate([
            jnp.where(edge_lane < HALO, 0.0, p[0:1]), p[1:tiles - 1],
            jnp.where(edge_lane >= LANES - HALO, 0.0, p[tiles - 1:]),
        ], axis=0)

    def fold(value):
        if len(value.shape) == 2:
            return value
        total = value[0]
        for t in range(1, value.shape[0]):
            total = total + value[t]
        return total

    with jax.named_scope("main_m"):
        def main_body(i, sums):
            new = products(main, TOP + HALO + 8 * i, right_ring, keep_main)
            return tuple(s + fold(p) for s, p in zip(sums, new))

        zero8 = jnp.zeros((8, LANES), f32)
        sums = lax.fori_loop(
            0, groups - 1, main_body, tuple(zero8 for _ in range(2 * ITERS)), unroll=groups - 1)
        for i, s in enumerate(sums):
            part[i] = s
    with jax.named_scope("side_fill"):
        for k in range(kinds + 1):
            if k < kinds:
                first, last = src[k, 0, body_rows], src[k, tiles - 1, body_rows]
                src[k, side_tile, body_rows, :] = jnp.where(
                    wide_lane < LANES // 2, pltpu.roll(first, 2 * HALO, axis=1), last)
            else:
                first, last = lab[0, body_rows], lab[tiles - 1, body_rows]
                lab[side_tile, body_rows, :] = jnp.where(
                    wide_lane < LANES // 2, pltpu.roll(first, 2 * HALO, axis=1), last)

    with jax.named_scope("relay"):
        pl.when(jnp.logical_and(inner_col, upper_half))(lambda: relay(1))
        pl.when(jnp.logical_and(inner_col, upper_half))(lambda: relay(-1))

    with jax.named_scope("wait_cols"):
        wait_columns(recv_sem)

    with jax.named_scope("unpack_cols"):
        for k in range(kinds + 1):
            at = pl.ds(HALO * k, HALO)
            right = jnp.where(last_col, 0.0, got_c[1, at, :])
            left = jnp.where(first_col, 0.0, got_c[0, at, :])
            turned = jnp.transpose(jnp.concatenate([right, left], axis=0))
            if k < kinds:
                src[k, side_tile, body_rows, 0:2 * HALO] = turned
            else:
                lab[side_tile, body_rows, 0:2 * HALO] = turned.astype(jnp.int32)
        corner_lane = lane_of((HALO, LANES))

    off_lane = ((lane_t < HALO) & last_col) | ((lane_t >= HALO) & (lane_t < 2 * HALO) & first_col)
    off_top = (line_t < HALO) & first_row
    off_bottom = (line_t >= HALO) & last_row
    ends = ((TOP - HALO, off_top), (TOP + rows - HALO, off_bottom))

    def stage(which, tile, start, beside):
        if which == 0:
            return right_side(src, lab, tile, start, beside)
        return applied(which - 1, tile, start, beside)

    def side_groups(which, begin, end):
        for i in range(begin, end):
            start = TOP - HALO + 8 * i
            off = off_lane
            if i == 0:
                off = off | off_top
            if i == groups:
                off = off | off_bottom
            save(which, side_tile, start, jnp.where(
                off, 0.0, stage(which, side_tile, start, beside_tile)))

    def side_inner(which):
        begin = TOP + HALO + 8 * which
        count = groups - 1 - 2 * which
        whole_loop(count, lambda i: save(
            which, side_tile, begin + 8 * i, jnp.where(
                off_lane, 0.0, stage(which, side_tile, begin + 8 * i, beside_tile))))

    on_side = ((lane_t >= 2 * HALO) & (lane_t < 3 * HALO)) | (lane_t >= LANES - HALO)

    def side_sums(begin, end, sums):
        def body(i, sums):
            new = products(
                side_tile, TOP + 8 * (begin + i), right_tile, lambda p: jnp.where(on_side, p, 0.0))
            return tuple(s + p for s, p in zip(sums, new))

        return list(lax.fori_loop(0, end - begin, body, tuple(sums), unroll=end - begin))

    with jax.named_scope("side_inner"):
        for which in range(ITERS):
            side_inner(which)
        for i, s in enumerate(side_sums(ITERS, groups - ITERS, [part[i] for i in range(2 * ITERS)])):
            part[i] = s

    with jax.named_scope("wait_halo"):
        wait_rows(recv_sem, got_down, got_up)

    with jax.named_scope("unpack"):
        for side in range(2):
            missing = first_row if side == 0 else last_row
            got = got_down if side == 0 else got_up
            for k in range(kinds + 1):
                wide = []
                for t in range(tiles):
                    depth, at = row_part(1 - side, k, t)
                    wide.append(jnp.where(missing, 0.0, got[pl.ds(at, depth), :]))
                shift = HALO - depth if side == 0 else 0
                near_lines = slice(shift, shift + depth)
                at = pl.ds(HALO * k, HALO)
                right = jnp.where(missing | last_col, 0.0, got_d[side, 1, at, :])[near_lines]
                left = jnp.where(missing | first_col, 0.0, got_d[side, 0, at, :])[near_lines]
                corner_lane = lane_of((depth, LANES))
                moved = pltpu.roll(
                    jnp.where(corner_lane >= LANES - HALO, left, wide[0]), 2 * HALO, axis=1)
                own = jnp.where(corner_lane < LANES // 2, moved, wide[-1])
                wide.append(jnp.where(corner_lane < HALO, right, own))
                base = TOP - depth if side == 0 else TOP + rows
                for t, value in enumerate(wide):
                    if k < kinds:
                        src[k, t, pl.ds(base, depth), :] = value
                    else:
                        lab[t, pl.ds(base, depth), :] = value.astype(jnp.int32)

    with jax.named_scope("frames"):
        for which in range(ITERS):
            side_groups(which, 0, 1 + which)
            side_groups(which, groups - which, groups + 1)
            for start, off in ends:
                save(which, main, start, jnp.where(
                    off[None], 0.0, stage(which, main, start, beside_ring)))

    with jax.named_scope("moments"):
        sums = side_sums(0, ITERS, [part[i] for i in range(2 * ITERS)])
        sums = side_sums(groups - ITERS, groups, sums)
        for (start, _), on in zip(ends, (line_t >= HALO, line_t < HALO)):
            new = products(main, start, right_ring, lambda p: jnp.where(on[None], keep_main(p), 0.0))
            sums = [s + fold(p) for s, p in zip(sums, new)]
        lane1 = lane_of((1, LANES))
        mine = jnp.zeros((1, LANES), f32)
        for i, s in enumerate(sums):
            mine = jnp.where(lane1 == i, jnp.sum(s, keepdims=True), mine)
        moment[me] = mine

    with jax.named_scope("send_moments"):
        pl.when(jnp.logical_and(last_col, there[0, -1]))(lambda: hear(1))

        def tell(r, c):
            pltpu.make_async_remote_copy(
                src_ref=moment.at[me], dst_ref=moment.at[me], send_sem=tell_send, recv_sem=mom_recv,
                device_id=(r, c), device_id_type=MESH).start()

        def tell_block(c):
            def body(r, _):
                tell(r, c)
                return 0

            lax.fori_loop(0, n_row, body, 0)

        for c in range(n_col - 1):
            pl.when(c < col)(functools.partial(tell_block, c))
        for_other_rows(lambda r: tell(r, col))
        pl.when(jnp.logical_and(inner_col, jnp.logical_not(upper_half)))(lambda: relay(-1))

    def tell_rest():
        pl.when(first_col)(lambda: hear(-1))
        for c in range(1, n_col):
            pl.when(c > col)(functools.partial(tell_block, c))

    with jax.named_scope("tell_inner"):
        pl.when(inner_col)(tell_rest)

    ends_of = ((0, TOP), (quad - 1, TOP + rows - 4))
    lines_of = [(w, e, q) for w in range(ITERS) for e in range(2) for q in range(tiles // 4)]
    with jax.named_scope("patch"):
        for at, (w, e, q) in enumerate(lines_of):
            for i in range(4):
                four = vec[w, 4 * q + i, pl.ds(ends_of[e][1], 4), :]
                band[i, at:at + 1, :] = jnp.sum(four, axis=0, keepdims=True)
        wide = jnp.concatenate([band[i] for i in range(4)], axis=1)
        patch[row, 0:wide.shape[0], :] = split_dot(wide, pool4)
        odd = lax.rem(row, 2) == 1
        row_lane = lane_of((1, rows))
        for w in range(ITERS):
            flat = vec[w, side_tile, pl.ds(TOP, quad, stride=4), :]
            for line in range(1, 4):
                flat = flat + vec[w, side_tile, pl.ds(TOP + line, quad, stride=4), :]
            even_part, odd_part = jnp.where(odd, 0.0, flat), jnp.where(odd, flat, 0.0)
            turned = jnp.transpose(jnp.concatenate([even_part, odd_part] * 2, axis=0))
            left = jnp.sum(turned[2 * HALO:3 * HALO], axis=0, keepdims=True)
            right = jnp.sum(turned[LANES - HALO:], axis=0, keepdims=True)
            at = len(lines_of) + w
            patch[row, at:at + 1, :] = jnp.where(row_lane < 2 * quad, left, right) * (1.0 / 16)
        for_other_rows(lambda r: pltpu.make_async_remote_copy(
            src_ref=patch.at[row], dst_ref=patch.at[row], send_sem=tell_send,
            recv_sem=patch_recv, device_id=(r, col), device_id_type=MESH).start())

    with jax.named_scope("merge"):
        for w in range(ITERS):
            side = vec[w, side_tile, body_rows]
            vec[w, 0, body_rows, :] = jnp.where(
                wide_lane < HALO, pltpu.roll(side, LANES - 2 * HALO, axis=1), vec[w, 0, body_rows])
            vec[w, tiles - 1, body_rows, :] = jnp.where(
                wide_lane >= LANES - HALO, side, vec[w, tiles - 1, body_rows])

    with jax.named_scope("fines"):
        half = rows // 2
        for w in range(ITERS):
            own = pooled(
                lambda tile, line: jnp.concatenate([
                    vec[w, 2 * q + tile, pl.ds(TOP + line, half, stride=2), :]
                    for q in range(tiles // 2)], axis=0),
                2, pool2)
            for q in range(tiles // 2):
                fines[w, q] = own[q * half:(q + 1) * half]

    with jax.named_scope("tell_first"):
        pl.when(jnp.logical_and(first_col, there[0, 1]))(tell_rest)

    with jax.named_scope("near"):
        wait_bytes(blocks(chips - 1), chip_recv)
        for w in range(ITERS):
            for owner in others:
                to_partner(w, owner)

    with jax.named_scope("wait_patch"):
        patches = patch.at[pl.ds(0, n_row - 1)]
        wait_bytes(patches, patch_recv)
    with jax.named_scope("prepare"):
        for pair in range(n_row // 2):
            for w in range(ITERS):
                at = len(lines_of) + w
                both = patch[2 * pair, at:at + 1, :] + patch[2 * pair + 1, at:at + 1, :]
                turned = jnp.transpose(jnp.broadcast_to(both, (8, LANES)))
                for end in range(2):
                    part_here = turned[2 * quad * end:2 * quad * (end + 1), 0:1]
                    sides[w, end, pl.ds(2 * pair * quad, 2 * quad), :] = jnp.broadcast_to(
                        part_here, (2 * quad, LANES))

    with jax.named_scope("wait_forwards"):
        wait_bytes(blocks(2 * chips - 1), mid_send)
        wait_bytes(blocks(chips), fwd_recv)
    with jax.named_scope("apply"):
        for owner in range(n_row):
            for at, (w, e, q) in enumerate(lines_of):
                mids[w, q, pl.ds(owner * quad + ends_of[e][0], 1), :] = patch[
                    owner, at:at + 1, :]
        all_lane = lane_of((n_row * quad, LANES))
        for w in range(ITERS):
            for end, q, lane in ((0, 0, 0), (1, tiles // 4 - 1, LANES - 1)):
                mids[w, q] = jnp.where(all_lane == lane, sides[w, end], mids[w, q])

    with jax.named_scope("wait_moments"):
        everyone = moment.at[pl.ds(0, n - 1)]
        wait_bytes(everyone, mom_recv)
    with jax.named_scope("coefs"):
        total = jnp.sum(moment[...], axis=0)
        moments = [
            (0.25 ** i * (1.0 if i < 2 * ITERS - 1 else 2.0))
            * jnp.sum(jnp.where(lane1 == i, total, 0.0), axis=1, keepdims=True)
            for i in range(2 * ITERS)
        ]
        for w, c in enumerate(coefficients(moments)):
            coord_ref[w] = jnp.broadcast_to(0.25 ** w * c, (8, LANES))

    with jax.named_scope("wait_sends"):
        wait_rows(send_sem, got_up, got_down)
        wait_columns(send_sem)
        wait_bytes(token.at[pl.ds(0, n - 1 + (n_row - 1) * patch.shape[1])], tell_send)


def finish_kernel(
    rows, cols, vec, fines, mids, coord_ref, blend_out, fine_out, mid_out, coarse_out,
    blend, fine, mid, coarse, out_sem,
):
    tiles = cols // LANES

    def leave(which, source, target, q):
        pltpu.make_async_copy(
            source.at[q], target.at[:, pl.ds(q * LANES, LANES)], out_sem.at[which]).start()

    def combine(load, target, height):
        coords = [coord_ref[w] for w in range(ITERS)]

        def body(g, _):
            start = pl.multiple_of(g * 8, 8)
            strip = None
            for w in range(ITERS):
                term = coords[w] * load(w, start)
                strip = term if strip is None else strip + term
            target[pl.ds(start, 8), :] = strip
            return 0

        lax.fori_loop(0, height // 8, body, 0, unroll=height // 8)

    tall = mid.shape[1]
    with jax.named_scope("mid"):
        for q in range(mid.shape[0]):
            combine(lambda w, start: mids[w, q, pl.ds(start, 8), :], mid.at[q], tall)
            leave(1, mid, mid_out, q)
    with jax.named_scope("coarse"):
        pool2 = pool_matrix(2)
        for q in range(coarse.shape[0]):
            coarse[q] = pooled(
                lambda tile, line: mid[2 * q + tile, pl.ds(line, tall // 2, stride=2), :], 2, pool2)
    with jax.named_scope("blend"):
        for t in range(tiles):
            combine(lambda w, start: vec[w, t, pl.ds(start + TOP, 8), :], blend.at[t], rows)
            leave(0, blend, blend_out, t)
    with jax.named_scope("fine"):
        for q in range(tiles // 2):
            combine(lambda w, start: fines[w, q, pl.ds(start, 8), :], fine.at[q], rows // 2)
            leave(2, fine, fine_out, q)
    with jax.named_scope("coarse_out"):
        for q in range(coarse.shape[0]):
            leave(3, coarse, coarse_out, q)
    with jax.named_scope("wait_out"):
        for which, ref in enumerate((blend, mid, fine, coarse)):
            pltpu.make_async_copy(ref, ref, out_sem.at[which]).wait()


def per_device(n_row, n_col, sources, labels):
    kinds, rows, cols = sources.shape
    n = n_row * n_col
    tiles = cols // LANES
    tall = rows + 2 * TOP
    n_pack = HALO * (kinds + 1)
    f32 = jnp.float32
    vmem = pl.BlockSpec(memory_space=pltpu.VMEM)
    hbm = pl.BlockSpec(memory_space=pltpu.HBM)
    up_lines, down_lines = ((kinds * d + d - 1) * tiles for d in (HALO, HALO - 1))
    token_lines = (kinds + 1) * max(2 * (8 * tiles + rows), (tiles - 2) * rows)
    mid_rows, coarse_rows = n_row * rows // 4, n_row * rows // 8
    chips = n_row // 2
    dma = pltpu.SemaphoreType.DMA
    vec, fines, mids, coords = pl.pallas_call(
        functools.partial(gather_kernel, n_row, n_col, rows, cols, kinds),
        out_shape=(
            jax.ShapeDtypeStruct((ITERS, tiles + 1, tall, LANES), f32),
            jax.ShapeDtypeStruct((ITERS, tiles // 2, rows // 2, LANES), f32),
            jax.ShapeDtypeStruct((ITERS, tiles // 4, mid_rows, LANES), f32),
            jax.ShapeDtypeStruct((ITERS, 8, LANES), f32),
        ),
        in_specs=[hbm] * 2,
        out_specs=(vmem,) * 4,
        scratch_shapes=[
            pltpu.VMEM((kinds, tiles + 1, tall, LANES), f32),
            pltpu.VMEM((tiles + 1, tall, LANES), jnp.int32),
            pltpu.VMEM((kinds, 2, 8, cols), f32),
            pltpu.VMEM((2, 8, cols), jnp.int32),
            pltpu.VMEM((up_lines, LANES), f32),
            pltpu.VMEM((down_lines, LANES), f32),
            pltpu.VMEM((2, n_pack, rows), f32),
            pltpu.VMEM((2, 2, n_pack, LANES), f32),
            pltpu.VMEM((up_lines, LANES), f32),
            pltpu.VMEM((down_lines, LANES), f32),
            pltpu.VMEM((2, n_pack, rows), f32),
            pltpu.VMEM((2, 2, n_pack, LANES), f32),
            pltpu.VMEM((2 * ITERS, 8, LANES), f32),
            pltpu.VMEM((n, 1, LANES), f32),
            pltpu.VMEM((4, ITERS * (tiles // 2), LANES), f32),
            pltpu.VMEM((n_row, ITERS * (tiles // 2) + 4, LANES), f32),
            pltpu.VMEM((ITERS, 2, mid_rows, LANES), f32),
            pltpu.VMEM((token_lines, LANES), f32),
            dma((2,)),
            dma((4,)),
            dma((4,)),
            pltpu.SemaphoreType.REGULAR((2,)),
            dma,
            dma,
            dma,
            dma,
        ],
        compiler_params=pltpu.CompilerParams(
            collective_id=0, has_side_effects=True, vmem_limit_bytes=24 * 2**20),
    )(
        pltpu.with_memory_space_constraint(sources, pltpu.HBM),
        pltpu.with_memory_space_constraint(labels, pltpu.HBM),
    )
    return pl.pallas_call(
        functools.partial(finish_kernel, rows, cols),
        out_shape=(
            jax.ShapeDtypeStruct((rows, cols), f32),
            jax.ShapeDtypeStruct((rows // 2, cols // 2), f32),
            jax.ShapeDtypeStruct((mid_rows, cols // 4), f32),
            jax.ShapeDtypeStruct((coarse_rows, cols // 8), f32),
        ),
        in_specs=[vmem] * 4,
        out_specs=(hbm,) * 4,
        scratch_shapes=[
            pltpu.VMEM((tiles, rows, LANES), f32),
            pltpu.VMEM((tiles // 2, rows // 2, LANES), f32),
            pltpu.VMEM((tiles // 4, mid_rows, LANES), f32),
            pltpu.VMEM((tiles // 8, coarse_rows, LANES), f32),
            dma((4,)),
        ],
        compiler_params=pltpu.CompilerParams(vmem_limit_bytes=24 * 2**20),
    )(vec, fines, mids, coords)


def solution(mesh):
    sizes = dict(mesh.shape)
    return jax.shard_map(
        functools.partial(per_device, sizes["row"], sizes["col"]),
        mesh=mesh,
        in_specs=(P(None, "row", "col"), P("row", "col")),
        out_specs=(P("row", "col"), P("row", "col"), P(None, "col"), P(None, "col")),
        check_vma=False,
    )
```

```python
import functools

import jax
import jax.numpy as jnp
from jax import lax
from jax.experimental import pallas as pl
from jax.experimental.pallas import tpu as pltpu
from jax.sharding import PartitionSpec as P

ITERS = 3
MESH = pl.DeviceIdType.MESH
HALO = 4
TOP = 8
LANES = 128
SIDES = ((1, 1), (1, -1), (-1, 1), (-1, -1), (1, 0), (-1, 0), (0, 1), (0, -1))


def lane_of(shape):
    return lax.broadcasted_iota(jnp.int32, shape, len(shape) - 1)


def line_of(shape):
    return lax.broadcasted_iota(jnp.int32, shape, len(shape) - 2)


def lines(ref, index, start):
    return ref[index + (pl.ds(start, 8), slice(None))]


def beside_ring(mid):
    tiles = mid.shape[0]
    lane = lane_of(mid.shape)
    left = pltpu.roll(mid, 1, axis=2)
    right = pltpu.roll(mid, LANES - 1, axis=2)
    from_left = jnp.concatenate([left[tiles - 1:], left[:tiles - 1]], axis=0)
    from_right = jnp.concatenate([right[1:], right[:1]], axis=0)
    return jnp.where(lane == 0, from_left, left) + jnp.where(lane == LANES - 1, from_right, right)


def beside_tile(mid):
    return pltpu.roll(mid, 1, axis=1) + pltpu.roll(mid, LANES - 1, axis=1)


def neighbour_sum(ref, index, start, mid, beside):
    return (lines(ref, index, start - 1) + lines(ref, index, start + 1)) + beside(mid)


def right_side(src, lab, tile, start, beside):
    here = lines(lab, (tile,), start)
    total = None
    for k in reversed(range(src.shape[0])):
        mid = lines(src, (k, tile), start)
        term = 4.0 * mid - neighbour_sum(src, (k, tile), start, mid, beside)
        total = term if total is None else jnp.where(here == k, term, total)
    return total


def from_left(values):
    lane = lane_of(values.shape)
    moved = pltpu.roll(values, 1, axis=2)
    return jnp.where(lane == 0, jnp.concatenate([moved[-1:], moved[:-1]], axis=0), moved)


def from_right(values):
    lane = lane_of(values.shape)
    moved = pltpu.roll(values, LANES - 1, axis=2)
    return jnp.where(lane == LANES - 1, jnp.concatenate([moved[1:], moved[:1]], axis=0), moved)


def chosen(here, values):
    total = values[-1]
    for k in reversed(range(len(values) - 1)):
        total = jnp.where(here == k, values[k], total)
    return total


def beside_chosen(src, lab, tile, start):
    here = lines(lab, (tile,), start)
    mids = [lines(src, (k, tile), start) for k in range(src.shape[0])]
    return chosen(from_right(here), mids), chosen(from_left(here), mids)


def right_side_ring(src, lab, tile, start, left, right):
    here = lines(lab, (tile,), start)
    crosses = [
        4.0 * lines(src, (k, tile), start)
        - (lines(src, (k, tile), start - 1) + lines(src, (k, tile), start + 1))
        for k in range(src.shape[0])
    ]
    return chosen(here, crosses) - (from_left(left) + from_right(right))


def quadratic(left, right, moments, shift):
    total = None
    for i, a in enumerate(left):
        for j, b in enumerate(right):
            term = a * b * moments[i + j + shift]
            total = term if total is None else total + term
    return total


def padded_sum(a, b):
    if len(a) < len(b):
        a, b = b, a
    return [x + b[i] if i < len(b) else x for i, x in enumerate(a)]


def coefficients(moments):
    residual = [jnp.ones_like(moments[0])]
    direction = residual
    solution_coords = [jnp.zeros_like(moments[0])]
    norm_now = moments[0]
    for iteration in range(ITERS):
        applied_dot = 4.0 * (
            quadratic(direction, direction, moments, 0)
            - quadratic(direction, direction, moments, 1)
        )
        step = norm_now / applied_dot
        solution_coords = padded_sum(solution_coords, [step * d for d in direction])
        if iteration + 1 < ITERS:
            moved = [-4.0 * step * d for d in direction]
            residual = padded_sum(residual, moved)
            residual = padded_sum(residual, [jnp.zeros_like(step)] + [-m for m in moved])
            norm_next = quadratic(residual, residual, moments, 0)
            ratio = norm_next / norm_now
            direction = padded_sum(residual, [ratio * d for d in direction])
            norm_now = norm_next
    return solution_coords


def split_dot(values, pool):
    pieces = []
    for _ in range(3):
        pieces.append(values.astype(jnp.bfloat16))
        values = values - pieces[-1].astype(jnp.float32)
    parts = jnp.dot(jnp.concatenate(pieces, axis=0), pool, preferred_element_type=jnp.float32)
    size = values.shape[0]
    return (parts[0:size] + parts[size:2 * size]) + parts[2 * size:]


def pooled(load, stride, pool):
    parts = []
    for tile in range(stride):
        part = load(tile, 0)
        for line in range(1, stride):
            part = part + load(tile, line)
        parts.append(part)
    return split_dot(jnp.concatenate(parts, axis=1), pool)


def pool_matrix(stride):
    shape = (LANES * stride, LANES)
    source, target = (lax.broadcasted_iota(jnp.int32, shape, d) for d in range(2))
    return jnp.where(source // stride == target, 1.0 / (stride * stride), 0.0).astype(jnp.bfloat16)


def gather_kernel(
    n_row, n_col, rows, cols, kinds,
    src_hbm, lab_hbm, vec, fines, mids, coord_ref,
    src, lab, edge, edge_lab, pack_up, pack_down, pack_c, pack_d, got_up, got_down, got_c, got_d,
    part, moment, band, patch, sides, token, load_sem, send_sem, recv_sem, chain,
    mom_recv, chip_recv, fwd_recv, patch_recv,
):
    tell_send, mid_send = load_sem.at[0], load_sem.at[1]
    tiles = cols // LANES
    side_tile = tiles
    main = slice(0, tiles)
    body_rows = pl.ds(TOP, rows)
    n = n_row * n_col
    row, col = lax.axis_index("row"), lax.axis_index("col")
    me = row * n_col + col
    f32 = jnp.float32

    first_row, last_row = row == 0, row == n_row - 1
    first_col, last_col = col == 0, col == n_col - 1
    there = {
        (dr, dc): functools.reduce(jnp.logical_and, [
            jnp.logical_not(edge) for step, edge in (
                (dr < 0, first_row), (dr > 0, last_row), (dc < 0, first_col), (dc > 0, last_col))
            if step])
        for dr, dc in SIDES
    }

    def other_row(step):
        return jnp.where(step >= row, step + 1, step)

    def for_other_rows(act):
        def body(step, _):
            act(other_row(step))
            return 0

        lax.fori_loop(0, n_row - 1, body, 0)

    barrier = pltpu.get_barrier_semaphore()

    def greet(r, c):
        pl.semaphore_signal(barrier, inc=1, device_id=(r, c), device_id_type=MESH)

    greeters = n_row - 1
    for dr, dc in ((-r, -c) for r, c in SIDES):
        if dc:
            pl.when(there[dr, dc])(functools.partial(
                greet, jnp.clip(row + dr, 0, n_row - 1), jnp.clip(col + dc, 0, n_col - 1)))
            greeters = greeters + jnp.where(there[dr, dc], 1, 0)
    def plane_load(k, t, wave):
        lanes = pl.ds(t * LANES, LANES)
        if k < kinds:
            return pltpu.make_async_copy(
                src_hbm.at[k, :, lanes], src.at[k, t, body_rows], load_sem.at[wave])
        return pltpu.make_async_copy(
            lab_hbm.at[:, lanes], lab.at[t, body_rows], load_sem.at[wave])

    def edge_load(k, side):
        here = pl.ds(0 if side == 0 else rows - 8, 8)
        if k < kinds:
            return pltpu.make_async_copy(src_hbm.at[k, here], edge.at[k, side], load_sem.at[0])
        return pltpu.make_async_copy(lab_hbm.at[here], edge_lab.at[side], load_sem.at[0])

    def wait_bytes(ref, sem):
        pltpu.make_async_copy(ref, ref, sem).wait()

    for k in range(kinds + 1):
        for side in range(2):
            edge_load(k, side).start()
    for k in range(kinds + 1):
        for t in (0, tiles - 1):
            plane_load(k, t, 0).start()
    for_other_rows(lambda r: greet(r, col))
    for t in range(1, tiles - 1):
        for k in range(kinds + 1):
            plane_load(k, t, 1).start()

    pad = jnp.zeros((tiles + 1, 8, LANES), f32)
    for start in (0, TOP + rows):
        for k in range(kinds):
            src[k, :, pl.ds(start, 8), :] = pad
        lab[:, pl.ds(start, 8), :] = pad.astype(jnp.int32)
        for w in range(ITERS):
            vec[w, :, pl.ds(start, 8), :] = pad

    def row_part(side, k, t):
        depth = HALO - side
        each = kinds * depth + depth - 1
        return (depth if k < kinds else depth - 1), t * each + k * depth

    n_pack = HALO * (kinds + 1)
    with jax.named_scope("wait_first"):
        wait_bytes(token.at[pl.ds(0, 2 * (kinds + 1) * (8 * tiles + rows))], load_sem.at[0])
    with jax.named_scope("pack"):
        for side in range(2):
            for k in range(kinds + 1):
                for t in range(tiles):
                    lanes = pl.ds(t * LANES, LANES)
                    depth, at = row_part(side, k, t)
                    lines_here = pl.ds(0 if side == 0 else 8 - depth, depth)
                    if k < kinds:
                        value = edge[k, side, lines_here, lanes]
                    else:
                        value = edge_lab[side, lines_here, lanes].astype(f32)
                    (pack_up if side == 0 else pack_down)[pl.ds(at, depth), :] = value
                for end, t in enumerate((0, tiles - 1)):
                    lanes = pl.ds(t * LANES, LANES)
                    lines_here = pl.ds(0 if side == 0 else 8 - HALO, HALO)
                    if k < kinds:
                        value = edge[k, side, lines_here, lanes]
                    else:
                        value = edge_lab[side, lines_here, lanes].astype(f32)
                    pack_d[side, end, pl.ds(HALO * k, HALO), :] = value
        wide_lane = lane_of((rows, LANES))
        for k in range(kinds + 1):
            if k < kinds:
                first, last = src[k, 0, body_rows], src[k, tiles - 1, body_rows]
            else:
                first, last = lab[0, body_rows].astype(f32), lab[tiles - 1, body_rows].astype(f32)
            both = jnp.where(wide_lane < LANES // 2, first, last)
            turned = jnp.transpose(both)
            at = pl.ds(HALO * k, HALO)
            pack_c[0, at, :] = turned[0:HALO]
            pack_c[1, at, :] = turned[LANES - HALO:LANES]

    with jax.named_scope("barrier"):
        pl.semaphore_wait(barrier, greeters)

    def place(dr, dc):
        return (0 if dr < 0 else 1) if dc == 0 else 2 if dr == 0 else 3

    for dr, dc in SIDES:
        mine_r, mine_c = (0 if dr < 0 else 1), (0 if dc < 0 else 1)
        if dc == 0:
            source, target = (pack_up, got_up) if dr < 0 else (pack_down, got_down)
        elif dr == 0:
            source, target = pack_c.at[mine_c], got_c.at[1 - mine_c]
        else:
            source = pack_d.at[mine_r, mine_c]
            target = got_d.at[1 - mine_r, 1 - mine_c]
        device = (
            jnp.clip(row + dr, 0, n_row - 1),
            jnp.clip(col + dc, 0, n_col - 1),
        )
        pl.when(there[dr, dc])(pltpu.make_async_remote_copy(
            src_ref=source, dst_ref=target, send_sem=send_sem.at[place(dr, dc)],
            recv_sem=recv_sem.at[place(-dr, -dc)], device_id=device, device_id_type=MESH,
        ).start)

    beside_rows = jnp.where(there[-1, 0], 1, 0) + jnp.where(there[1, 0], 1, 0)
    beside_cols = jnp.where(there[0, -1], 1, 0) + jnp.where(there[0, 1], 1, 0)
    corners = beside_rows * beside_cols

    def wait_rows(sem, above, below):
        pl.when(there[-1, 0])(lambda: wait_bytes(above, sem.at[0]))
        pl.when(there[1, 0])(lambda: wait_bytes(below, sem.at[1]))
        pl.when(corners == 4)(lambda: wait_bytes(got_d, sem.at[3]))
        pl.when(corners == 2)(lambda: wait_bytes(got_d.at[0], sem.at[3]))
        pl.when(corners == 1)(lambda: wait_bytes(got_d.at[0, 0], sem.at[3]))

    def wait_columns(sem):
        pl.when(beside_cols == 2)(lambda: wait_bytes(got_c, sem.at[2]))
        pl.when(beside_cols == 1)(lambda: wait_bytes(got_c.at[0], sem.at[2]))

    def pass_on(dc):
        pl.semaphore_signal(
            chain.at[0 if dc > 0 else 1], inc=1,
            device_id=(row, jnp.clip(col + dc, 0, n_col - 1)), device_id_type=MESH)

    def hear(dc):
        pl.semaphore_wait(chain.at[0 if dc > 0 else 1], 1)

    def relay(dc):
        hear(dc)
        pass_on(dc)

    inner_col = jnp.logical_and(there[0, 1], there[0, -1])
    upper_half = 2 * col >= n_col
    pl.when(jnp.logical_and(first_col, there[0, 1]))(lambda: pass_on(1))
    pl.when(jnp.logical_and(last_col, there[0, -1]))(lambda: pass_on(-1))

    with jax.named_scope("wait_later"):
        wait_bytes(token.at[pl.ds(0, (kinds + 1) * (tiles - 2) * rows)], load_sem.at[1])
    groups = rows // 8
    lane_r = lane_of((tiles, 8, LANES))
    lane_t = lane_of((8, LANES))
    line_t = line_of((8, LANES))

    def whole_loop(count, act):
        def body(i, _):
            act(i)
            return 0

        lax.fori_loop(0, count, body, 0, unroll=count)

    def save(which, tile, start, value):
        vec[which, tile, pl.ds(start, 8), :] = value

    def applied(which, tile, start, beside):
        mid = lines(vec, (which, tile), start)
        return neighbour_sum(vec, (which, tile), start, mid, beside)

    with jax.named_scope("main_b"):
        def choose(i):
            start = TOP + 8 * i
            left, right = beside_chosen(src, lab, main, start)
            save(1, main, start, left)
            save(2, main, start, right)

        whole_loop(groups, choose)
        whole_loop(groups, lambda i: save(0, main, TOP + 8 * i, right_side_ring(
            src, lab, main, TOP + 8 * i,
            lines(vec, (1, main), TOP + 8 * i), lines(vec, (2, main), TOP + 8 * i))))

    pl.when(jnp.logical_and(inner_col, jnp.logical_not(upper_half)))(lambda: relay(1))

    def inner(which):
        whole_loop(groups, lambda i: save(
            which, main, TOP + 8 * i, applied(which - 1, main, TOP + 8 * i, beside_ring)))


    chips = n_row // 2
    core = lax.rem(row, 2)
    chip = lax.div(row, 2)
    partner = row + 1 - 2 * core
    quad = rows // 4
    pool4, pool2 = pool_matrix(4), pool_matrix(2)

    def blocks(count):
        return mids.at[:, :, pl.ds(0, count * quad)]

    def hand(w, owner, target, send, recv):
        block = mids.at[w, :, pl.ds(pl.multiple_of(owner * quad, 8), quad)]
        pltpu.make_async_remote_copy(
            src_ref=block, dst_ref=block, send_sem=send, recv_sem=recv,
            device_id=(target, col), device_id_type=MESH).start()

    def same_core(q):
        return 2 * q + core

    def to_partner(w, owner):
        hand(w, owner, partner, mid_send, fwd_recv)

    others = [lax.rem(chip + step, chips) for step in range(1, chips)]
    if chips == 4:
        others = [3 - chip, chip + 1 - 2 * lax.rem(chip, 2), chip + 2 - 4 * lax.div(chip, 2)]
    others = [same_core(q) for q in others]

    def send_early(w):
        own = pooled(
            lambda tile, line: jnp.concatenate([
                vec[w, 4 * q + tile, pl.ds(TOP + line, quad, stride=4), :]
                for q in range(tiles // 4)], axis=0),
            4, pool4)
        for q in range(tiles // 4):
            mids[w, q, pl.ds(pl.multiple_of(row * quad, 8), quad), :] = own[
                q * quad:(q + 1) * quad]
        for target in others:
            hand(w, row, target, mid_send, chip_recv)
        to_partner(w, row)

    with jax.named_scope("main_v"):
        for w in range(1, ITERS):
            inner(w)
            send_early(w - 1)
        send_early(ITERS - 1)

    def products(tile, start, right_of, keep):
        powers = [lines(vec, (w, tile), start) for w in range(ITERS)]
        powers.append(lines(vec, (ITERS - 1, tile), start + 1) + right_of(powers[-1]))
        kept = [keep(p) for p in powers[:ITERS]]
        return [kept[i // 2] * powers[(i + 1) // 2] for i in range(2 * ITERS)]

    def right_ring(mid):
        right = pltpu.roll(mid, LANES - 1, axis=2)
        return jnp.where(
            lane_r == LANES - 1, jnp.concatenate([right[1:], right[:1]], axis=0), right)

    def right_tile(mid):
        return pltpu.roll(mid, LANES - 1, axis=1)

    def keep_main(p):
        edge_lane = lane_of((1, 8, LANES))
        return jnp.concatenate([
            jnp.where(edge_lane < HALO, 0.0, p[0:1]), p[1:tiles - 1],
            jnp.where(edge_lane >= LANES - HALO, 0.0, p[tiles - 1:]),
        ], axis=0)

    def fold(value):
        if len(value.shape) == 2:
            return value
        total = value[0]
        for t in range(1, value.shape[0]):
            total = total + value[t]
        return total

    with jax.named_scope("main_m"):
        def main_body(i, sums):
            new = products(main, TOP + HALO + 8 * i, right_ring, keep_main)
            return tuple(s + fold(p) for s, p in zip(sums, new))

        zero8 = jnp.zeros((8, LANES), f32)
        sums = lax.fori_loop(
            0, groups - 1, main_body, tuple(zero8 for _ in range(2 * ITERS)), unroll=groups - 1)
        for i, s in enumerate(sums):
            part[i] = s
    with jax.named_scope("side_fill"):
        for k in range(kinds + 1):
            if k < kinds:
                first, last = src[k, 0, body_rows], src[k, tiles - 1, body_rows]
                src[k, side_tile, body_rows, :] = jnp.where(
                    wide_lane < LANES // 2, pltpu.roll(first, 2 * HALO, axis=1), last)
            else:
                first, last = lab[0, body_rows], lab[tiles - 1, body_rows]
                lab[side_tile, body_rows, :] = jnp.where(
                    wide_lane < LANES // 2, pltpu.roll(first, 2 * HALO, axis=1), last)

    with jax.named_scope("relay"):
        pl.when(jnp.logical_and(inner_col, upper_half))(lambda: relay(1))
        pl.when(jnp.logical_and(inner_col, upper_half))(lambda: relay(-1))

    with jax.named_scope("wait_cols"):
        wait_columns(recv_sem)

    with jax.named_scope("unpack_cols"):
        for k in range(kinds + 1):
            at = pl.ds(HALO * k, HALO)
            right = jnp.where(last_col, 0.0, got_c[1, at, :])
            left = jnp.where(first_col, 0.0, got_c[0, at, :])
            turned = jnp.transpose(jnp.concatenate([right, left], axis=0))
            if k < kinds:
                src[k, side_tile, body_rows, 0:2 * HALO] = turned
            else:
                lab[side_tile, body_rows, 0:2 * HALO] = turned.astype(jnp.int32)
        corner_lane = lane_of((HALO, LANES))

    off_lane = ((lane_t < HALO) & last_col) | ((lane_t >= HALO) & (lane_t < 2 * HALO) & first_col)
    off_top = (line_t < HALO) & first_row
    off_bottom = (line_t >= HALO) & last_row
    ends = ((TOP - HALO, off_top), (TOP + rows - HALO, off_bottom))

    def stage(which, tile, start, beside):
        if which == 0:
            return right_side(src, lab, tile, start, beside)
        return applied(which - 1, tile, start, beside)

    def side_groups(which, begin, end):
        for i in range(begin, end):
            start = TOP - HALO + 8 * i
            off = off_lane
            if i == 0:
                off = off | off_top
            if i == groups:
                off = off | off_bottom
            save(which, side_tile, start, jnp.where(
                off, 0.0, stage(which, side_tile, start, beside_tile)))

    def side_inner(which):
        begin = TOP + HALO + 8 * which
        count = groups - 1 - 2 * which
        whole_loop(count, lambda i: save(
            which, side_tile, begin + 8 * i, jnp.where(
                off_lane, 0.0, stage(which, side_tile, begin + 8 * i, beside_tile))))

    on_side = ((lane_t >= 2 * HALO) & (lane_t < 3 * HALO)) | (lane_t >= LANES - HALO)

    def side_sums(begin, end, sums):
        def body(i, sums):
            new = products(
                side_tile, TOP + 8 * (begin + i), right_tile, lambda p: jnp.where(on_side, p, 0.0))
            return tuple(s + p for s, p in zip(sums, new))

        return list(lax.fori_loop(0, end - begin, body, tuple(sums), unroll=end - begin))

    with jax.named_scope("side_inner"):
        for which in range(ITERS - 1):
            side_inner(which)

    with jax.named_scope("wait_halo"):
        wait_rows(recv_sem, got_down, got_up)

    with jax.named_scope("unpack"):
        for side in range(2):
            missing = first_row if side == 0 else last_row
            got = got_down if side == 0 else got_up
            for k in range(kinds + 1):
                wide = []
                for t in range(tiles):
                    depth, at = row_part(1 - side, k, t)
                    wide.append(jnp.where(missing, 0.0, got[pl.ds(at, depth), :]))
                shift = HALO - depth if side == 0 else 0
                near_lines = slice(shift, shift + depth)
                at = pl.ds(HALO * k, HALO)
                right = jnp.where(missing | last_col, 0.0, got_d[side, 1, at, :])[near_lines]
                left = jnp.where(missing | first_col, 0.0, got_d[side, 0, at, :])[near_lines]
                corner_lane = lane_of((depth, LANES))
                moved = pltpu.roll(
                    jnp.where(corner_lane >= LANES - HALO, left, wide[0]), 2 * HALO, axis=1)
                own = jnp.where(corner_lane < LANES // 2, moved, wide[-1])
                wide.append(jnp.where(corner_lane < HALO, right, own))
                base = TOP - depth if side == 0 else TOP + rows
                for t, value in enumerate(wide):
                    if k < kinds:
                        src[k, t, pl.ds(base, depth), :] = value
                    else:
                        lab[t, pl.ds(base, depth), :] = value.astype(jnp.int32)

    with jax.named_scope("frames"):
        for which in range(ITERS):
            if which < ITERS - 1:
                side_groups(which, 0, 1 + which)
                side_groups(which, groups - which, groups + 1)
            else:
                side_groups(which, 0, groups + 1)
            for start, off in ends:
                save(which, main, start, jnp.where(
                    off[None], 0.0, stage(which, main, start, beside_ring)))

    with jax.named_scope("moments"):
        sums = side_sums(0, groups, [part[i] for i in range(2 * ITERS)])
        for (start, _), on in zip(ends, (line_t >= HALO, line_t < HALO)):
            new = products(main, start, right_ring, lambda p: jnp.where(on[None], keep_main(p), 0.0))
            sums = [s + fold(p) for s, p in zip(sums, new)]
        lane1 = lane_of((1, LANES))
        mine = jnp.zeros((1, LANES), f32)
        for i, s in enumerate(sums):
            mine = jnp.where(lane1 == i, jnp.sum(s, keepdims=True), mine)
        moment[me] = mine

    with jax.named_scope("send_moments"):
        pl.when(jnp.logical_and(last_col, there[0, -1]))(lambda: hear(1))

        def tell(r, c):
            pltpu.make_async_remote_copy(
                src_ref=moment.at[me], dst_ref=moment.at[me], send_sem=tell_send, recv_sem=mom_recv,
                device_id=(r, c), device_id_type=MESH).start()

        def tell_block(c):
            def body(r, _):
                tell(r, c)
                return 0

            lax.fori_loop(0, n_row, body, 0)

        for c in range(n_col - 1):
            pl.when(c < col)(functools.partial(tell_block, c))
        for_other_rows(lambda r: tell(r, col))
        pl.when(jnp.logical_and(inner_col, jnp.logical_not(upper_half)))(lambda: relay(-1))

    def tell_rest():
        pl.when(first_col)(lambda: hear(-1))
        for c in range(1, n_col):
            pl.when(c > col)(functools.partial(tell_block, c))

    with jax.named_scope("tell_inner"):
        pl.when(inner_col)(tell_rest)

    ends_of = ((0, TOP), (quad - 1, TOP + rows - 4))
    lines_of = [(w, e, q) for w in range(ITERS) for e in range(2) for q in range(tiles // 4)]
    with jax.named_scope("patch"):
        for at, (w, e, q) in enumerate(lines_of):
            for i in range(4):
                four = vec[w, 4 * q + i, pl.ds(ends_of[e][1], 4), :]
                band[i, at:at + 1, :] = jnp.sum(four, axis=0, keepdims=True)
        wide = jnp.concatenate([band[i] for i in range(4)], axis=1)
        patch[row, 0:wide.shape[0], :] = split_dot(wide, pool4)
        odd = lax.rem(row, 2) == 1
        row_lane = lane_of((1, rows))
        for w in range(ITERS):
            flat = vec[w, side_tile, pl.ds(TOP, quad, stride=4), :]
            for line in range(1, 4):
                flat = flat + vec[w, side_tile, pl.ds(TOP + line, quad, stride=4), :]
            even_part, odd_part = jnp.where(odd, 0.0, flat), jnp.where(odd, flat, 0.0)
            turned = jnp.transpose(jnp.concatenate([even_part, odd_part] * 2, axis=0))
            left = jnp.sum(turned[2 * HALO:3 * HALO], axis=0, keepdims=True)
            right = jnp.sum(turned[LANES - HALO:], axis=0, keepdims=True)
            at = len(lines_of) + w
            patch[row, at:at + 1, :] = jnp.where(row_lane < 2 * quad, left, right) * (1.0 / 16)
        for_other_rows(lambda r: pltpu.make_async_remote_copy(
            src_ref=patch.at[row], dst_ref=patch.at[row], send_sem=tell_send,
            recv_sem=patch_recv, device_id=(r, col), device_id_type=MESH).start())

    with jax.named_scope("merge"):
        for w in range(ITERS):
            side = vec[w, side_tile, body_rows]
            vec[w, 0, body_rows, :] = jnp.where(
                wide_lane < HALO, pltpu.roll(side, LANES - 2 * HALO, axis=1), vec[w, 0, body_rows])
            vec[w, tiles - 1, body_rows, :] = jnp.where(
                wide_lane >= LANES - HALO, side, vec[w, tiles - 1, body_rows])

    with jax.named_scope("fines"):
        half = rows // 2
        for w in range(ITERS):
            own = pooled(
                lambda tile, line: jnp.concatenate([
                    vec[w, 2 * q + tile, pl.ds(TOP + line, half, stride=2), :]
                    for q in range(tiles // 2)], axis=0),
                2, pool2)
            for q in range(tiles // 2):
                fines[w, q] = own[q * half:(q + 1) * half]

    with jax.named_scope("tell_first"):
        pl.when(jnp.logical_and(first_col, there[0, 1]))(tell_rest)

    with jax.named_scope("near"):
        wait_bytes(blocks(chips - 1), chip_recv)
        for w in range(ITERS):
            for owner in others:
                to_partner(w, owner)

    with jax.named_scope("wait_patch"):
        patches = patch.at[pl.ds(0, n_row - 1)]
        wait_bytes(patches, patch_recv)
    with jax.named_scope("prepare"):
        for pair in range(n_row // 2):
            for w in range(ITERS):
                at = len(lines_of) + w
                both = patch[2 * pair, at:at + 1, :] + patch[2 * pair + 1, at:at + 1, :]
                turned = jnp.transpose(jnp.broadcast_to(both, (8, LANES)))
                for end in range(2):
                    part_here = turned[2 * quad * end:2 * quad * (end + 1), 0:1]
                    sides[w, end, pl.ds(2 * pair * quad, 2 * quad), :] = jnp.broadcast_to(
                        part_here, (2 * quad, LANES))

    with jax.named_scope("wait_forwards"):
        wait_bytes(blocks(2 * chips - 1), mid_send)
        wait_bytes(blocks(chips), fwd_recv)
    with jax.named_scope("apply"):
        for owner in range(n_row):
            for at, (w, e, q) in enumerate(lines_of):
                mids[w, q, pl.ds(owner * quad + ends_of[e][0], 1), :] = patch[
                    owner, at:at + 1, :]
        all_lane = lane_of((n_row * quad, LANES))
        for w in range(ITERS):
            for end, q, lane in ((0, 0, 0), (1, tiles // 4 - 1, LANES - 1)):
                mids[w, q] = jnp.where(all_lane == lane, sides[w, end], mids[w, q])

    with jax.named_scope("wait_moments"):
        everyone = moment.at[pl.ds(0, n - 1)]
        wait_bytes(everyone, mom_recv)
    with jax.named_scope("coefs"):
        total = jnp.sum(moment[...], axis=0)
        moments = [
            (0.25 ** i * (1.0 if i < 2 * ITERS - 1 else 2.0))
            * jnp.sum(jnp.where(lane1 == i, total, 0.0), axis=1, keepdims=True)
            for i in range(2 * ITERS)
        ]
        for w, c in enumerate(coefficients(moments)):
            coord_ref[w] = jnp.broadcast_to(0.25 ** w * c, (8, LANES))

    with jax.named_scope("wait_sends"):
        wait_rows(send_sem, got_up, got_down)
        wait_columns(send_sem)
        wait_bytes(token.at[pl.ds(0, n - 1 + (n_row - 1) * patch.shape[1])], tell_send)


def finish_kernel(
    rows, cols, vec, fines, mids, coord_ref, blend_out, fine_out, mid_out, coarse_out,
    blend, fine, mid, coarse, out_sem,
):
    tiles = cols // LANES

    def leave(which, source, target, q):
        pltpu.make_async_copy(
            source.at[q], target.at[:, pl.ds(q * LANES, LANES)], out_sem.at[which]).start()

    def combine(load, target, height):
        coords = [coord_ref[w] for w in range(ITERS)]

        def body(g, _):
            start = pl.multiple_of(g * 8, 8)
            strip = None
            for w in range(ITERS):
                term = coords[w] * load(w, start)
                strip = term if strip is None else strip + term
            target[pl.ds(start, 8), :] = strip
            return 0

        lax.fori_loop(0, height // 8, body, 0, unroll=height // 8)

    tall = mid.shape[1]
    with jax.named_scope("mid"):
        for q in range(mid.shape[0]):
            combine(lambda w, start: mids[w, q, pl.ds(start, 8), :], mid.at[q], tall)
            leave(1, mid, mid_out, q)
    with jax.named_scope("coarse"):
        pool2 = pool_matrix(2)
        for q in range(coarse.shape[0]):
            coarse[q] = pooled(
                lambda tile, line: mid[2 * q + tile, pl.ds(line, tall // 2, stride=2), :], 2, pool2)
    with jax.named_scope("blend"):
        for t in range(tiles):
            combine(lambda w, start: vec[w, t, pl.ds(start + TOP, 8), :], blend.at[t], rows)
            leave(0, blend, blend_out, t)
    with jax.named_scope("fine"):
        for q in range(tiles // 2):
            combine(lambda w, start: fines[w, q, pl.ds(start, 8), :], fine.at[q], rows // 2)
            leave(2, fine, fine_out, q)
    with jax.named_scope("coarse_out"):
        for q in range(coarse.shape[0]):
            leave(3, coarse, coarse_out, q)
    with jax.named_scope("wait_out"):
        for which, ref in enumerate((blend, mid, fine, coarse)):
            pltpu.make_async_copy(ref, ref, out_sem.at[which]).wait()


def per_device(n_row, n_col, sources, labels):
    kinds, rows, cols = sources.shape
    n = n_row * n_col
    tiles = cols // LANES
    tall = rows + 2 * TOP
    n_pack = HALO * (kinds + 1)
    f32 = jnp.float32
    vmem = pl.BlockSpec(memory_space=pltpu.VMEM)
    hbm = pl.BlockSpec(memory_space=pltpu.HBM)
    up_lines, down_lines = ((kinds * d + d - 1) * tiles for d in (HALO, HALO - 1))
    token_lines = (kinds + 1) * max(2 * (8 * tiles + rows), (tiles - 2) * rows)
    mid_rows, coarse_rows = n_row * rows // 4, n_row * rows // 8
    chips = n_row // 2
    dma = pltpu.SemaphoreType.DMA
    vec, fines, mids, coords = pl.pallas_call(
        functools.partial(gather_kernel, n_row, n_col, rows, cols, kinds),
        out_shape=(
            jax.ShapeDtypeStruct((ITERS, tiles + 1, tall, LANES), f32),
            jax.ShapeDtypeStruct((ITERS, tiles // 2, rows // 2, LANES), f32),
            jax.ShapeDtypeStruct((ITERS, tiles // 4, mid_rows, LANES), f32),
            jax.ShapeDtypeStruct((ITERS, 8, LANES), f32),
        ),
        in_specs=[hbm] * 2,
        out_specs=(vmem,) * 4,
        scratch_shapes=[
            pltpu.VMEM((kinds, tiles + 1, tall, LANES), f32),
            pltpu.VMEM((tiles + 1, tall, LANES), jnp.int32),
            pltpu.VMEM((kinds, 2, 8, cols), f32),
            pltpu.VMEM((2, 8, cols), jnp.int32),
            pltpu.VMEM((up_lines, LANES), f32),
            pltpu.VMEM((down_lines, LANES), f32),
            pltpu.VMEM((2, n_pack, rows), f32),
            pltpu.VMEM((2, 2, n_pack, LANES), f32),
            pltpu.VMEM((up_lines, LANES), f32),
            pltpu.VMEM((down_lines, LANES), f32),
            pltpu.VMEM((2, n_pack, rows), f32),
            pltpu.VMEM((2, 2, n_pack, LANES), f32),
            pltpu.VMEM((2 * ITERS, 8, LANES), f32),
            pltpu.VMEM((n, 1, LANES), f32),
            pltpu.VMEM((4, ITERS * (tiles // 2), LANES), f32),
            pltpu.VMEM((n_row, ITERS * (tiles // 2) + 4, LANES), f32),
            pltpu.VMEM((ITERS, 2, mid_rows, LANES), f32),
            pltpu.VMEM((token_lines, LANES), f32),
            dma((2,)),
            dma((4,)),
            dma((4,)),
            pltpu.SemaphoreType.REGULAR((2,)),
            dma,
            dma,
            dma,
            dma,
        ],
        compiler_params=pltpu.CompilerParams(
            collective_id=0, has_side_effects=True, vmem_limit_bytes=24 * 2**20),
    )(
        pltpu.with_memory_space_constraint(sources, pltpu.HBM),
        pltpu.with_memory_space_constraint(labels, pltpu.HBM),
    )
    return pl.pallas_call(
        functools.partial(finish_kernel, rows, cols),
        out_shape=(
            jax.ShapeDtypeStruct((rows, cols), f32),
            jax.ShapeDtypeStruct((rows // 2, cols // 2), f32),
            jax.ShapeDtypeStruct((mid_rows, cols // 4), f32),
            jax.ShapeDtypeStruct((coarse_rows, cols // 8), f32),
        ),
        in_specs=[vmem] * 4,
        out_specs=(hbm,) * 4,
        scratch_shapes=[
            pltpu.VMEM((tiles, rows, LANES), f32),
            pltpu.VMEM((tiles // 2, rows // 2, LANES), f32),
            pltpu.VMEM((tiles // 4, mid_rows, LANES), f32),
            pltpu.VMEM((tiles // 8, coarse_rows, LANES), f32),
            dma((4,)),
        ],
        compiler_params=pltpu.CompilerParams(vmem_limit_bytes=24 * 2**20),
    )(vec, fines, mids, coords)


def solution(mesh):
    sizes = dict(mesh.shape)
    return jax.shard_map(
        functools.partial(per_device, sizes["row"], sizes["col"]),
        mesh=mesh,
        in_specs=(P(None, "row", "col"), P("row", "col")),
        out_specs=(P("row", "col"), P("row", "col"), P(None, "col"), P(None, "col")),
        check_vma=False,
    )
```
